128 devices in a mesh: elem: 32 (over x_hi, y, z), comp: 2 (over x_lo), rep: 2 (over core).
Axes of the slice: x: 4 (x_hi: 2, x_lo: 2; x = x_hi * 2 + x_lo), y: 4, z: 4, core: 2. Of those that a mesh axis runs over, the one named last changes fastest.
Arguments:
- velocity: float32 [3, 10, 10, 10, 2, 24576], P(None, 'comp', None, None, None, ('elem', 'rep')), may hold values from -6 to 6
- geometry: float32 [3, 3, 10, 10, 10, 2, 24576], P(None, None, 'comp', None, None, None, ('elem', 'rep')), may hold values from -40 to 40
- element_place: int32 [2, 24576], P('comp', ('elem', 'rep')), may hold values from 0 to 383, as said below
Outputs:
- pressure: float32 [10, 10, 10, 2, 24576], P(None, None, None, 'comp', ('elem', 'rep'))
The draws below stay inside these ranges and needn't reach their ends.
Inputs may be any that keep to these rules, and one draw needn't show every extreme that they name: `element_place`: in each row and each aligned run of 384 entries of it, every value 0 to 383 appears once.
All inputs are finite; a program needn't handle non-finite values.
Results may differ from the reference program's by a relative error of at most 0.000071.
Values sent between devices are 32-bit elements; how exact they have to be, the bound alone decides.
A program may use at most 192 MiB of HBM per device.

```python
import jax
import jax.numpy as jnp
import numpy as np
from jax import lax

NODES = 10
BLOCK_X = 6
BLOCK_Y = 8
BLOCK_Z = 8
GRID_Y = 4
SUB_ELEMS = 384
ROW_ELEMS = 24576
BOX_X = 48
BOX_Y = 32
BOX_Z = 32
N_COMP = 2
N_REP = 2


def draw_geometry(key, part):
    base_key = jax.random.fold_in(key, 31)
    weight_key, mixing_key = jax.random.split(base_key)
    node_shape = (NODES, NODES, NODES, N_COMP, ROW_ELEMS)
    full_shape = (3, 3) + node_shape
    weights = jax.random.uniform(weight_key, node_shape, jnp.float32, 0.5, 2.0)
    mixing = 0.35 * jax.random.truncated_normal(mixing_key, -4.0, 4.0, full_shape, jnp.float32)
    mixing = mixing + jnp.eye(3, dtype=jnp.float32).reshape(3, 3, 1, 1, 1, 1, 1)
    return (weights[None, None] * mixing).astype(jnp.float32)


def draw_element_place(key, part):
    blocks = N_COMP * ROW_ELEMS // SUB_ELEMS
    block_keys = jax.random.split(jax.random.fold_in(key, 7), blocks)

    def one_order(block_key):
        return jax.random.permutation(block_key, SUB_ELEMS)
    orders = jax.vmap(one_order)(block_keys)
    return orders.reshape(N_COMP, ROW_ELEMS).astype(jnp.int32)


def steps_of(key, shape, pieces, smallest, top_value):
    gain, own = 1.0, jax.random.fold_in(key, 6)
    for axis_at, blocks in pieces:
        draws = jnp.exp(jax.random.uniform(jax.random.fold_in(own, axis_at), (blocks,), jnp.float32, smallest / len(pieces), top_value / len(pieces)))
        gain = gain * jnp.repeat(draws, shape[axis_at] // blocks).reshape([-1 if axis == axis_at else 1 for axis in range(len(shape))])
    return gain


def scatter_about(rng, shape, scale, most, cuts=(), held_as=jnp.bfloat16):
    drawn = jax.random.normal(rng, shape, jnp.float32) * scale
    if len(cuts) > 0:
        drawn = steps_of(rng, shape, cuts, -0.22, 0.18) * drawn
    return jnp.clip(drawn, min=-most, max=most).astype(held_as)


def setup_inputs(seed: int = 0) -> dict:
    key_of = jax.random.split(jax.random.key(seed), 4)
    return {
        "velocity": scatter_about(key_of[0], (3, NODES, NODES, NODES, N_COMP, ROW_ELEMS), 1.0, 6.0, ((1, 2), (5, 64)), jnp.float32),
        "geometry": draw_geometry(jax.random.fold_in(key_of[3], 71), 0),
        "element_place": draw_element_place(jax.random.fold_in(key_of[3], 71), 0),
    }


exact_mode = lax.Precision.HIGHEST


def legendre_columns(points, degree):
    columns = [points * 0.0 + 1.0, points]
    for order in range(2, degree + 1):
        columns.append(((2 * order - 1) * points * columns[order - 1] - (order - 1) * columns[order - 2]) / order)
    return columns


def derivative_table(node_count):
    degree = node_count - 1
    points = np.cos(np.pi * np.arange(node_count) / degree)
    for sweep in range(100):
        columns = legendre_columns(points, degree)
        points = points - (points * columns[degree] - columns[degree - 1]) / (node_count * columns[degree])
    points = np.sort(points)
    values = legendre_columns(points, degree)[degree]
    identity = np.eye(node_count)
    spacing = points[:, None] - points[None, :] + identity
    matrix = values[:, None] / (values[None, :] * spacing)
    matrix = np.where(identity > 0.5, 0.0, matrix)
    matrix[0, 0] = -degree * (degree + 1) / 4.0
    matrix[degree, degree] = degree * (degree + 1) / 4.0
    return matrix


def apply_transpose(deriv_table, flux_r, flux_s, flux_t):
    along_r = jnp.einsum("ia,i...->a...", deriv_table, flux_r, precision=exact_mode)
    along_s = jnp.einsum("ib,ai...->ab...", deriv_table, flux_s, precision=exact_mode)
    along_t = jnp.einsum("ic,abi...->abc...", deriv_table, flux_t, precision=exact_mode)
    return along_r + along_s + along_t


def local_pass(field, direction, block_grid):
    last_node = field.shape[0] - 1
    low_key = tuple(0 if dim_index == direction else slice(None) for dim_index in range(3))
    high_key = tuple(last_node if dim_index == direction else slice(None) for dim_index in range(3))
    lower = field[low_key]
    upper = field[high_key]
    leading = lower.shape[:-1]
    lower = lower.reshape(leading + tuple(block_grid))
    upper = upper.reshape(leading + tuple(block_grid))
    element_axis = len(leading) + direction
    extent = block_grid[direction]
    summed = lax.slice_in_dim(upper, 0, extent - 1, axis=element_axis) + lax.slice_in_dim(lower, 1, extent, axis=element_axis)
    upper = jnp.concatenate([summed, lax.slice_in_dim(upper, extent - 1, extent, axis=element_axis)], axis=element_axis)
    lower = jnp.concatenate([lax.slice_in_dim(lower, 0, 1, axis=element_axis), summed], axis=element_axis)
    field = field.at[low_key].set(lower.reshape(leading + (-1,)))
    return field.at[high_key].set(upper.reshape(leading + (-1,)))


def element_cells(element_place):
    row_index = jnp.arange(ROW_ELEMS, dtype=jnp.int32)[None, :]
    half_index = jnp.arange(N_COMP, dtype=jnp.int32)[:, None]
    block_index = row_index // SUB_ELEMS
    layers = N_COMP * N_REP
    sub_block = (block_index // N_REP) * layers + half_index * N_REP + block_index % N_REP
    cell_x = (sub_block // (GRID_Y * layers)) * BLOCK_X + element_place // (BLOCK_Y * BLOCK_Z)
    cell_y = ((sub_block // layers) % GRID_Y) * BLOCK_Y + (element_place // BLOCK_Z) % BLOCK_Y
    cell_z = (sub_block % layers) * BLOCK_Z + element_place % BLOCK_Z
    return ((cell_x * BOX_Y + cell_y) * BOX_Z + cell_z).astype(jnp.int32)


def reference(velocity, geometry, element_place):
    deriv_table = jnp.asarray(derivative_table(NODES), jnp.float32)
    fluxes = []
    for direction in range(3):
        fluxes.append(geometry[0, direction] * velocity[0] + geometry[1, direction] * velocity[1] + geometry[2, direction] * velocity[2])
    local_div = apply_transpose(deriv_table, fluxes[0], fluxes[1], fluxes[2])
    flat_cells = element_cells(element_place).reshape(-1).astype(jnp.int32)
    flat_local = local_div.reshape(NODES, NODES, NODES, N_COMP * ROW_ELEMS)
    box_field = jnp.zeros((NODES, NODES, NODES, BOX_X * BOX_Y * BOX_Z), jnp.float32)
    box_field = box_field.at[:, :, :, flat_cells].set(flat_local)
    for direction in range(3):
        box_field = local_pass(box_field, direction, (BOX_X, BOX_Y, BOX_Z))
    pressure = box_field[:, :, :, flat_cells]
    return pressure.reshape(NODES, NODES, NODES, N_COMP, ROW_ELEMS)
```

```python
import jax
import jax.numpy as jnp
import numpy as np
from jax import lax
from jax.experimental import pallas as pl
from jax.experimental.pallas import tpu as pltpu
from jax.sharding import PartitionSpec as P

BLOCK_X = 6
BLOCK_Y = 8
BLOCK_Z = 8
GRID_Y = 4
NODES = 10
HALF = 5
ELEMS = 384
LANES = 128
TILES = 3
ROWS = 104
MESH = pl.DeviceIdType.MESH


def legendre_columns(points, degree):
    columns = [points * 0.0 + 1.0, points]
    for order in range(2, degree + 1):
        columns.append(
            ((2 * order - 1) * points * columns[order - 1] - (order - 1) * columns[order - 2])
            / order
        )
    return columns


def derivative_table(node_count):
    degree = node_count - 1
    points = np.cos(np.pi * np.arange(node_count) / degree)
    for sweep in range(100):
        columns = legendre_columns(points, degree)
        points = points - (points * columns[degree] - columns[degree - 1]) / (
            node_count * columns[degree]
        )
    points = np.sort(points)
    values = legendre_columns(points, degree)[degree]
    identity = np.eye(node_count)
    spacing = points[:, None] - points[None, :] + identity
    matrix = values[:, None] / (values[None, :] * spacing)
    matrix = np.where(identity > 0.5, 0.0, matrix)
    matrix[0, 0] = -degree * (degree + 1) / 4.0
    matrix[degree, degree] = degree * (degree + 1) / 4.0
    return matrix


TABLE = derivative_table(NODES)
EVEN = [[float(0.5 * (TABLE[i, m] + TABLE[i, 9 - m])) for m in range(HALF)] for i in range(HALF)]
ODD = [[float(0.5 * (TABLE[i, m] - TABLE[i, 9 - m])) for m in range(HALF)] for i in range(HALF)]


def weighted(terms, weights):
    total = terms[0] * weights[0]
    for term, weight in zip(terms[1:], weights[1:]):
        total = total + term * weight
    return total


def along(values):
    minus = [values[i] - values[9 - i] for i in range(HALF)]
    plus = [values[i] + values[9 - i] for i in range(HALF)]
    out = [None] * NODES
    for m in range(HALF):
        even = weighted(minus, [EVEN[i][m] for i in range(HALF)])
        odd = weighted(plus, [ODD[i][m] for i in range(HALF)])
        out[m] = even + odd
        out[9 - m] = even - odd
    return out


def tile(t):
    return slice(t * LANES, (t + 1) * LANES)


def roll_lanes(x, shift):
    return pltpu.roll(x, shift % LANES, 1)


def roll_rows(x, shift):
    return pltpu.roll(x, shift % 8, 0)


def two_parts(x):
    high = x.astype(jnp.bfloat16)
    low = (x - high.astype(jnp.float32)).astype(jnp.bfloat16)
    return jnp.concatenate([high, low], axis=1)


def kernel(
    v_hbm, g_hbm, place_ref, out_ref,
    v, g, coef, f0, fl, lhs, perm, back, place_in, canon, got,
    zs, zr, ys, yr, xs, xr, tops, tops_in,
    v_sem, g_sem, place_sem, z_sem, y_sem, x_sem, inner_send, inner_recv, edge_send, edge_recv,
):
    elem = lax.axis_index("elem")
    c = lax.axis_index("comp")
    r = lax.axis_index("rep")
    o = 1 - c
    elem_count = lax.axis_size("elem")
    grid_x = elem_count // GRID_Y
    sx = elem // GRID_Y
    sy = elem % GRID_Y
    y_up = sx * GRID_Y + (sy + 1) % GRID_Y
    y_down = sx * GRID_Y + (sy + GRID_Y - 1) % GRID_Y
    x_up = (elem + GRID_Y) % elem_count
    x_down = (elem + elem_count - GRID_Y) % elem_count

    for i in range(HALF):
        pltpu.make_async_copy(v_hbm.at[:, i], v.at[:, i], v_sem.at[i]).start()
        pltpu.make_async_copy(g_hbm.at[:, 0, i], g.at[:, 0, i], g_sem.at[0, i]).start()
    for i in range(HALF):
        for j in (1, 2):
            pltpu.make_async_copy(g_hbm.at[:, j, i], g.at[:, j, i], g_sem.at[j, i]).start()

    others = (
        (elem, o, r), (elem, c, 1 - r), (y_up, c, r), (y_down, c, r), (x_up, c, r), (x_down, c, r),
    )
    barrier = pltpu.get_barrier_semaphore()
    for other in others:
        pl.semaphore_signal(barrier, inc=1, device_id=other, device_id_type=MESH)

    for kind in range(2):
        for m in range(HALF):
            for i in range(HALF):
                first = float(TABLE[i, (5 + m) if kind == 0 else m])
                second = float(TABLE[5 + i, m if kind == 0 else (5 + m)])
                coef[(kind * HALF + m) * HALF + i] = jnp.where(c == 0, first, second).astype(jnp.float32)

    pl.semaphore_wait(barrier, len(others))
    place_copy = pltpu.make_async_remote_copy(
        src_ref=place_ref, dst_ref=place_in, send_sem=place_sem.at[0], recv_sem=place_sem.at[1],
        device_id=(elem, o, r), device_id_type=MESH,
    )
    place_copy.start()

    rows_iota = lax.broadcasted_iota(jnp.int32, (ELEMS, ELEMS), 0)
    hit = (rows_iota == place_ref[...]).astype(jnp.float32)
    back_half = hit.astype(jnp.bfloat16)
    back[0:ELEMS, :] = back_half
    back[ELEMS : 2 * ELEMS, :] = back_half
    own_half = hit.T.astype(jnp.bfloat16)
    perm[c, 0:ELEMS, :] = own_half
    perm[c, ELEMS : 2 * ELEMS, :] = own_half
    lhs[...] = jnp.zeros_like(lhs)

    def first_flux(i, carry):
        pltpu.make_async_copy(v_hbm.at[:, i], v.at[:, i], v_sem.at[i]).wait()
        pltpu.make_async_copy(g_hbm.at[:, 0, i], g.at[:, 0, i], g_sem.at[0, i]).wait()

        def at_b(b, carry):
            for k in range(NODES):
                f0[i, b, k] = (
                    g[0, 0, i, b, k] * v[0, i, b, k]
                    + g[1, 0, i, b, k] * v[1, i, b, k]
                    + g[2, 0, i, b, k] * v[2, i, b, k]
                )
            return carry

        return lax.fori_loop(0, NODES, at_b, carry)

    lax.fori_loop(0, HALF, first_flux, 0)

    place_copy.wait()
    hit_in = (rows_iota == place_in[...]).astype(jnp.float32)
    other_half = hit_in.T.astype(jnp.bfloat16)
    perm[o, 0:ELEMS, :] = other_half
    perm[o, ELEMS : 2 * ELEMS, :] = other_half

    def inner_copy(a):
        return pltpu.make_async_remote_copy(
            src_ref=canon.at[o, a, 0:64], dst_ref=got.at[a, 0:64],
            send_sem=inner_send.at[a], recv_sem=inner_recv.at[a],
            device_id=(elem, o, r), device_id_type=MESH,
        )

    def is_inner(a):
        return jnp.logical_and(a > 0, a < NODES - 1)

    def mix_planes(base, b):
        weights = [coef[base + i] for i in range(HALF)]
        for k in range(NODES):
            fl[b, k] = weighted([f0[i, b, k] for i in range(HALF)], weights)

    def gather_rows():
        for q in range(2):
            for t in range(TILES):
                for b in range(8):
                    lhs[q, b * 8 : b * 8 + 8, tile(t)] = fl[b + 1, 1:9, q, tile(t)]
                lhs[q, 64:72, tile(t)] = fl[1:9, 0, q, tile(t)]
                lhs[q, 72:80, tile(t)] = fl[0, 1:9, q, tile(t)]
                lhs[q, 80:88, tile(t)] = fl[1:9, 9, q, tile(t)]
                lhs[q, 88:96, tile(t)] = fl[9, 1:9, q, tile(t)]
            lhs[q, 96:97, :] = fl[0, 0, q : q + 1, :]
            lhs[q, 97:98, :] = fl[0, 9, q : q + 1, :]
            lhs[q, 98:99, :] = fl[9, 0, q : q + 1, :]
            lhs[q, 99:100, :] = fl[9, 9, q : q + 1, :]

    def to_canon(a):
        for q in range(2):
            canon[q, a] = jnp.dot(two_parts(lhs[q]), perm[q], preferred_element_type=jnp.float32)

    def send_if_inner(a):
        @pl.when(is_inner(a))
        def _():
            inner_copy(a).start()

    far = HALF * o
    near = HALF * c

    def far_plane(m, carry):
        def at_b(b, carry):
            mix_planes(m * HALF, b)
            return carry

        lax.fori_loop(0, NODES, at_b, 0)
        gather_rows()

        @pl.when(m > 0)
        def _():
            send_if_inner(far + m - 1)

        to_canon(far + m)
        return carry

    lax.fori_loop(0, HALF, far_plane, 0)

    def near_plane(m, carry):
        for j in (1, 2):
            pltpu.make_async_copy(g_hbm.at[:, j, m], g.at[:, j, m], g_sem.at[j, m]).wait()

        def flux(j, b, k):
            return (
                g[0, j, m, b, k] * v[0, m, b, k]
                + g[1, j, m, b, k] * v[1, m, b, k]
                + g[2, j, m, b, k] * v[2, m, b, k]
            )

        def at_b(b, carry):
            base = (HALF + m) * HALF
            weights = [coef[base + i] for i in range(HALF)]
            out = along([flux(2, b, k) for k in range(NODES)])
            for k in range(NODES):
                fl[b, k] = out[k] + weighted([f0[i, b, k] for i in range(HALF)], weights)
            return carry

        lax.fori_loop(0, NODES, at_b, 0)

        def at_k(k, carry):
            out = along([flux(1, b, k) for b in range(NODES)])
            for b in range(NODES):
                fl[b, k] = fl[b, k] + out[b]
            return carry

        lax.fori_loop(0, NODES, at_k, 0)
        gather_rows()

        @pl.when(m == 0)
        def _():
            send_if_inner(far + HALF - 1)

        @pl.when(m > 0)
        def _():
            send_if_inner(near + m - 1)

        to_canon(near + m)
        return carry

    lax.fori_loop(0, HALF, near_plane, 0)

    lane = lax.broadcasted_iota(jnp.int32, (8, LANES), 1)
    row = lax.broadcasted_iota(jnp.int32, (8, LANES), 0)
    zi = lane % 8
    yi = (lane // 8) % 8
    low_half = lane < 64
    zero = jnp.zeros((8, LANES), jnp.float32)
    c_lo = jnp.logical_or(row == 0, row == 2)
    c_hi = jnp.logical_or(row == 1, row == 3)
    b_lo = row < 2
    b_hi = jnp.logical_or(row == 2, row == 3)

    def yz_pass(a, carry):
        for q in range(2):
            for t in range(TILES):
                lo, hi = canon[q, a, 64:72, tile(t)], canon[q, a, 80:88, tile(t)]
                canon[q, a, 64:72, tile(t)] = lo + jnp.where(zi > 0, roll_lanes(hi, 1), zero)
                canon[q, a, 80:88, tile(t)] = hi + jnp.where(zi < 7, roll_lanes(lo, -1), zero)
                lo, hi = canon[q, a, 72:80, tile(t)], canon[q, a, 88:96, tile(t)]
                canon[q, a, 72:80, tile(t)] = lo + jnp.where(yi > 0, roll_lanes(hi, 8), zero)
                canon[q, a, 88:96, tile(t)] = hi + jnp.where(yi < 7, roll_lanes(lo, -8), zero)
                k = canon[q, a, 96:104, tile(t)]
                to_lo = jnp.where(jnp.logical_and(c_lo, zi > 0), roll_lanes(roll_rows(k, -1), 1), zero)
                to_hi = jnp.where(jnp.logical_and(c_hi, zi < 7), roll_lanes(roll_rows(k, 1), -1), zero)
                k = k + to_lo + to_hi
                to_lo = jnp.where(jnp.logical_and(b_lo, yi > 0), roll_lanes(roll_rows(k, -2), 8), zero)
                to_hi = jnp.where(jnp.logical_and(b_hi, yi < 7), roll_lanes(roll_rows(k, 2), -8), zero)
                canon[q, a, 96:104, tile(t)] = k + to_lo + to_hi
        return carry

    lax.fori_loop(0, NODES, yz_pass, 0)

    @pl.when(is_inner(near + HALF - 1))
    def _():
        inner_copy(near + HALF - 1).start()

    def x_pass(block, carry):
        here = pl.ds(pl.multiple_of(block * 8, 8), 8)
        for q in range(2):
            lo = [canon[q, 0, here, tile(t)] for t in range(TILES)]
            hi = [canon[q, 9, here, tile(t)] for t in range(TILES)]
            lo_rolled = [roll_lanes(x, 64) for x in lo] + [zero]
            hi_rolled = [roll_lanes(x, 64) for x in hi] + [zero]
            for t in range(TILES):
                canon[q, 0, here, tile(t)] = lo[t] + jnp.where(low_half, hi_rolled[t - 1], hi_rolled[t])
                canon[q, 9, here, tile(t)] = hi[t] + jnp.where(low_half, lo_rolled[t], lo_rolled[t + 1])
        return carry

    lax.fori_loop(0, ROWS // 8, x_pass, 0)

    def pack_top(parts, index, step):
        total = parts[0]
        for u in range(1, len(parts)):
            total = jnp.where(index == 7 - u, roll_lanes(parts[u], -step * u), total)
        return total

    def pack_low(parts, index, step):
        total = parts[0]
        for u in range(1, len(parts)):
            total = jnp.where(index == u, roll_lanes(parts[u], step * u), total)
        return total

    def six(a, rows):
        return [canon[q, a, rows, tile(t)] for q in range(2) for t in range(TILES)]

    def on(flag):
        return jnp.where(flag, 1.0, 0.0).astype(jnp.float32)

    def z_pack(a, carry):
        corner = six(a, slice(96, 104))
        zs[0, a, 0:8] = pack_top(six(a, slice(80, 88)), zi, 1)
        zs[0, a, 8:16] = pack_top(corner, zi, 1)
        zs[1, a, 0:8] = pack_low(six(a, slice(64, 72)), zi, 1)
        zs[1, a, 8:16] = pack_low(corner, zi, 1)
        return carry

    lax.fori_loop(0, NODES, z_pack, 0)
    z_copy = pltpu.make_async_remote_copy(
        src_ref=zs, dst_ref=zr, send_sem=z_sem.at[0], recv_sem=z_sem.at[1],
        device_id=(elem, c, 1 - r), device_id_type=MESH,
    )
    z_copy.start()

    def put(a, b_row, value, t, first):
        start = ((a * 10 + b_row) * 10 + 1) * 3 + t
        out_ref[pl.ds(start, 8, stride=3), :] = value[first : first + 8, tile(t)]

    def put_column(a, k_row, value, t, first):
        start = ((a * 10 + 1) * 10 + k_row) * 3 + t
        out_ref[pl.ds(start, 8, stride=30), :] = value[first : first + 8, tile(t)]

    def put_edges(a, value, first):
        for t in range(TILES):
            put_column(a, 0, value, t, first)
            put(a, 0, value, t, first + 8)
            put_column(a, 9, value, t, first + 16)
            put(a, 9, value, t, first + 24)
            for number, (b, k) in enumerate(((0, 0), (0, 9), (9, 0), (9, 9))):
                start = ((a * 10 + b) * 10 + k) * 3 + t
                out_ref[pl.ds(start, 1), :] = value[first + 32 + number : first + 33 + number, tile(t)]

    def inner_done(a, carry):
        @pl.when(is_inner(a))
        def _():
            inner_copy(a).wait_recv()
            total = canon[c, a, 0:64] + got[a, 0:64]
            value = jnp.dot(two_parts(total), back[...], preferred_element_type=jnp.float32)
            for t in range(TILES):
                for b in range(8):
                    put(a, b + 1, value, t, b * 8)

        return carry

    lax.fori_loop(near, near + 2, inner_done, 0)

    z_copy.wait_recv()
    r0, r1 = on(r == 0), on(r == 1)

    def z_unpack(a, carry):
        tops_here = [zr[0, a, 0:8], roll_rows(zr[0, a, 8:16], -1)]
        lows_here = [zr[1, a, 0:8], roll_rows(zr[1, a, 8:16], 1)]
        for t in range(TILES):
            for kind in range(2):
                top_rows = slice(80, 88) if kind == 0 else slice(96, 104)
                low_rows = slice(64, 72) if kind == 0 else slice(96, 104)
                top_mask = zi == 7 if kind == 0 else jnp.logical_and(c_hi, zi == 7)
                low_mask = zi == 0 if kind == 0 else jnp.logical_and(c_lo, zi == 0)
                from_above = [roll_lanes(lows_here[kind], 7 - (3 * q + t)) for q in range(2)]
                from_below = [roll_lanes(tops_here[kind], 3 * q + t - 7) for q in range(2)]
                adds = (
                    (0, top_rows, top_mask, from_above[0] * r0 + from_above[1] * r1),
                    (1, top_rows, top_mask, from_above[1] * r0),
                    (0, low_rows, low_mask, from_below[0] * r1),
                    (1, low_rows, low_mask, from_below[0] * r0 + from_below[1] * r1),
                )
                for q, rows, mask, value in adds:
                    canon[q, a, rows, tile(t)] = canon[q, a, rows, tile(t)] + jnp.where(mask, value, zero)
        return carry

    lax.fori_loop(0, NODES, z_unpack, 0)

    def y_pack(a, carry):
        corner = six(a, slice(96, 104))
        ys[0, a, 0:8] = pack_top(six(a, slice(88, 96)), yi, 8)
        ys[0, a, 8:16] = pack_top(corner, yi, 8)
        ys[1, a, 0:8] = pack_low(six(a, slice(72, 80)), yi, 8)
        ys[1, a, 8:16] = pack_low(corner, yi, 8)
        return carry

    lax.fori_loop(0, NODES, y_pack, 0)
    y_copies = [
        pltpu.make_async_remote_copy(
            src_ref=ys.at[way], dst_ref=yr.at[way], send_sem=y_sem.at[0, way], recv_sem=y_sem.at[1, way],
            device_id=(y_up if way == 0 else y_down, c, r), device_id_type=MESH,
        )
        for way in range(2)
    ]
    for copy in y_copies:
        copy.start()

    lax.fori_loop(near + 2, near + 4, inner_done, 0)

    for copy in y_copies:
        copy.wait_recv()
    y_has_up, y_has_down = on(sy < GRID_Y - 1), on(sy > 0)

    def y_unpack(a, carry):
        below = [yr[0, a, 0:8] * y_has_down, roll_rows(yr[0, a, 8:16], -2) * y_has_down]
        above = [yr[1, a, 0:8] * y_has_up, roll_rows(yr[1, a, 8:16], 2) * y_has_up]
        for q in range(2):
            for t in range(TILES):
                u = 3 * q + t
                for kind in range(2):
                    top_rows = slice(88, 96) if kind == 0 else slice(96, 104)
                    low_rows = slice(72, 80) if kind == 0 else slice(96, 104)
                    top_mask = yi == 7 if kind == 0 else jnp.logical_and(b_hi, yi == 7)
                    low_mask = yi == 0 if kind == 0 else jnp.logical_and(b_lo, yi == 0)
                    up = jnp.where(top_mask, roll_lanes(above[kind], 8 * (7 - u)), zero)
                    down = jnp.where(low_mask, roll_lanes(below[kind], 8 * (u - 7)), zero)
                    canon[q, a, top_rows, tile(t)] = canon[q, a, top_rows, tile(t)] + up
                    canon[q, a, low_rows, tile(t)] = canon[q, a, low_rows, tile(t)] + down
        return carry

    lax.fori_loop(0, NODES, y_unpack, 0)

    def x_pack(block, carry):
        here = pl.ds(pl.multiple_of(block * 8, 8), 8)
        xs[0, here] = jnp.where(low_half, roll_lanes(canon[0, 9, here, tile(2)], 64), canon[1, 9, here, tile(2)])
        xs[1, here] = jnp.where(low_half, canon[0, 0, here, tile(0)], roll_lanes(canon[1, 0, here, tile(0)], 64))
        return carry

    lax.fori_loop(0, ROWS // 8, x_pack, 0)
    x_copies = [
        pltpu.make_async_remote_copy(
            src_ref=xs.at[way], dst_ref=xr.at[way], send_sem=x_sem.at[0, way], recv_sem=x_sem.at[1, way],
            device_id=(x_up if way == 0 else x_down, c, r), device_id_type=MESH,
        )
        for way in range(2)
    ]
    for copy in x_copies:
        copy.start()

    def edge_copy(number, source, target):
        return pltpu.make_async_remote_copy(
            src_ref=source, dst_ref=target, send_sem=edge_send.at[number], recv_sem=edge_recv.at[number],
            device_id=(elem, o, r), device_id_type=MESH,
        )

    edges = [
        edge_copy(0, canon.at[o, 1:9, 64:80], got.at[1:9, 64:80]),
        edge_copy(1, canon.at[o, 1:9, 96:104], got.at[1:9, 96:104]),
        edge_copy(2, tops.at[1:9], tops_in.at[1:9]),
        edge_copy(3, tops.at[0], tops_in.at[0]),
        edge_copy(4, canon.at[o, 0, 0:80], got.at[0, 0:80]),
        edge_copy(5, canon.at[o, 0, 96:104], got.at[0, 96:104]),
        edge_copy(6, canon.at[o, 9, :, 256:384], got.at[9, :, 256:384]),
    ]

    def fill_tops(a, carry):
        tops[a, 0:8] = pack_top([canon[o, a, 80:88, tile(t)] for t in range(TILES)], zi, 1)
        tops[a, 8:16] = pack_top([canon[o, a, 88:96, tile(t)] for t in range(TILES)], yi, 8)
        return carry

    edges[0].start()
    edges[1].start()
    lax.fori_loop(1, NODES - 1, fill_tops, 0)
    lax.fori_loop(near + 4, near + 5, inner_done, 0)
    edges[2].start()

    for copy in x_copies:
        copy.wait_recv()
    x_has_up, x_has_down = on(sx < grid_x - 1), on(sx > 0)

    def x_unpack(block, carry):
        here = pl.ds(pl.multiple_of(block * 8, 8), 8)
        below = xr[0, here] * x_has_down
        above = xr[1, here] * x_has_up
        low = (jnp.where(low_half, below, zero), jnp.where(low_half, roll_lanes(below, 64), zero))
        top = (jnp.where(low_half, zero, roll_lanes(above, 64)), jnp.where(low_half, zero, above))
        for q in range(2):
            canon[q, 0, here, tile(0)] = canon[q, 0, here, tile(0)] + low[q]
            canon[q, 9, here, tile(2)] = canon[q, 9, here, tile(2)] + top[q]
        return carry

    lax.fori_loop(0, ROWS // 8, x_unpack, 0)
    fill_tops(0, 0)
    edges[4].start()
    edges[5].start()
    lax.fori_loop(far, far + 1, inner_done, 0)
    edges[3].start()
    edges[6].start()
    lax.fori_loop(far + 1, far + 5, inner_done, 0)

    def complete(a, carry):
        for t in range(TILES):
            top = tops_in[a, 0:8]
            lo = got[a, 64:72, tile(t)]
            got[a, 80:88, tile(t)] = jnp.where(zi < 7, roll_lanes(lo, -1), roll_lanes(top, t))
            top = tops_in[a, 8:16]
            lo = got[a, 72:80, tile(t)]
            got[a, 88:96, tile(t)] = jnp.where(yi < 7, roll_lanes(lo, -8), roll_lanes(top, 8 * t))
        return carry

    for number in range(3):
        edges[number].wait_recv()
    lax.fori_loop(1, NODES - 1, complete, 0)

    def pair_done(pair, carry):
        start = 1 + pair * 4
        total = canon[c, pl.ds(start, 4), 64:104] + got[pl.ds(start, 4), 64:104]
        value = jnp.dot(
            two_parts(total.reshape(160, ELEMS)), back[...], preferred_element_type=jnp.float32
        )
        for k in range(4):
            put_edges(start + k, value, k * 40)
        return carry

    lax.fori_loop(0, 2, pair_done, 0)

    for number in range(3, 7):
        edges[number].wait_recv()
    complete(0, 0)

    def last_plane(block, carry):
        here = pl.ds(pl.multiple_of(block * 8, 8), 8)
        lo = [roll_lanes(got[0, here, tile(t)], 64) for t in range(TILES)]
        for t in range(TILES):
            after = lo[t + 1] if t < TILES - 1 else got[9, here, tile(2)]
            got[9, here, tile(t)] = jnp.where(low_half, lo[t], after)
        return carry

    lax.fori_loop(0, ROWS // 8, last_plane, 0)

    for a in (0, 9):
        total = canon[c, a] + got[a]
        value = jnp.dot(two_parts(total), back[...], preferred_element_type=jnp.float32)
        for t in range(TILES):
            for b in range(8):
                put(a, b + 1, value, t, b * 8)
        put_edges(a, value, 64)

    z_copy.wait_send()
    for copy in y_copies + x_copies + edges:
        copy.wait_send()

    def sent(a, carry):
        inner_copy(a).wait_send()
        return carry

    lax.fori_loop(1, NODES - 1, sent, 0)


def body(velocity, geometry, element_place):
    vmem = pltpu.VMEM
    dma = pltpu.SemaphoreType.DMA
    f32 = jnp.float32
    out = pl.pallas_call(
        kernel,
        out_shape=jax.ShapeDtypeStruct((NODES * NODES * NODES * TILES, LANES), f32),
        in_specs=[
            pl.BlockSpec(memory_space=pl.ANY),
            pl.BlockSpec(memory_space=pl.ANY),
            pl.BlockSpec(memory_space=pltpu.VMEM),
        ],
        out_specs=pl.BlockSpec(memory_space=pltpu.VMEM),
        scratch_shapes=[
            vmem((3, HALF, NODES, NODES, 2, ELEMS), f32),
            vmem((3, 3, HALF, NODES, NODES, 2, ELEMS), f32),
            pltpu.SMEM((2 * HALF * HALF,), f32),
            vmem((HALF, NODES, NODES, 2, ELEMS), f32),
            vmem((NODES, NODES, 2, ELEMS), f32),
            vmem((2, ROWS, ELEMS), f32),
            vmem((2, 2 * ELEMS, ELEMS), jnp.bfloat16),
            vmem((2 * ELEMS, ELEMS), jnp.bfloat16),
            vmem((1, ELEMS), jnp.int32),
            vmem((2, NODES, ROWS, ELEMS), f32),
            vmem((NODES, ROWS, ELEMS), f32),
            vmem((2, NODES, 16, LANES), f32),
            vmem((2, NODES, 16, LANES), f32),
            vmem((2, NODES, 16, LANES), f32),
            vmem((2, NODES, 16, LANES), f32),
            vmem((2, ROWS, LANES), f32),
            vmem((2, ROWS, LANES), f32),
            vmem((NODES - 1, 16, LANES), f32),
            vmem((NODES - 1, 16, LANES), f32),
            dma((HALF,)), dma((3, HALF)), dma((2,)), dma((2,)), dma((2, 2)), dma((2, 2)),
            dma((NODES,)), dma((NODES,)), dma((7,)), dma((7,)),
        ],
        compiler_params=pltpu.CompilerParams(
            collective_id=0, has_side_effects=True, vmem_limit_bytes=60 * 1024 * 1024
        ),
    )(velocity, geometry, element_place)
    return out.reshape(NODES, NODES, NODES, 1, ELEMS)


def solution(mesh):
    placed = (
        P(None, "comp", None, None, None, ("elem", "rep")),
        P(None, None, "comp", None, None, None, ("elem", "rep")),
        P("comp", ("elem", "rep")),
    )
    return jax.shard_map(
        body,
        mesh=mesh,
        in_specs=placed,
        out_specs=P(None, None, None, "comp", ("elem", "rep")),
        check_vma=False,
    )
```

```python
import jax
import jax.numpy as jnp
import numpy as np
from jax import lax
from jax.experimental import pallas as pl
from jax.experimental.pallas import tpu as pltpu
from jax.sharding import PartitionSpec as P

BLOCK_X = 6
BLOCK_Y = 8
BLOCK_Z = 8
GRID_Y = 4
NODES = 10
HALF = 5
ELEMS = 384
LANES = 128
TILES = 3
ROWS = 104
MESH = pl.DeviceIdType.MESH


def legendre_columns(points, degree):
    columns = [points * 0.0 + 1.0, points]
    for order in range(2, degree + 1):
        columns.append(
            ((2 * order - 1) * points * columns[order - 1] - (order - 1) * columns[order - 2])
            / order
        )
    return columns


def derivative_table(node_count):
    degree = node_count - 1
    points = np.cos(np.pi * np.arange(node_count) / degree)
    for sweep in range(100):
        columns = legendre_columns(points, degree)
        points = points - (points * columns[degree] - columns[degree - 1]) / (
            node_count * columns[degree]
        )
    points = np.sort(points)
    values = legendre_columns(points, degree)[degree]
    identity = np.eye(node_count)
    spacing = points[:, None] - points[None, :] + identity
    matrix = values[:, None] / (values[None, :] * spacing)
    matrix = np.where(identity > 0.5, 0.0, matrix)
    matrix[0, 0] = -degree * (degree + 1) / 4.0
    matrix[degree, degree] = degree * (degree + 1) / 4.0
    return matrix


TABLE = derivative_table(NODES)
EVEN = [[float(0.5 * (TABLE[i, m] + TABLE[i, 9 - m])) for m in range(HALF)] for i in range(HALF)]
ODD = [[float(0.5 * (TABLE[i, m] - TABLE[i, 9 - m])) for m in range(HALF)] for i in range(HALF)]


def weighted(terms, weights):
    total = terms[0] * weights[0]
    for term, weight in zip(terms[1:], weights[1:]):
        total = total + term * weight
    return total


def along(values):
    minus = [values[i] - values[9 - i] for i in range(HALF)]
    plus = [values[i] + values[9 - i] for i in range(HALF)]
    out = [None] * NODES
    for m in range(HALF):
        even = weighted(minus, [EVEN[i][m] for i in range(HALF)])
        odd = weighted(plus, [ODD[i][m] for i in range(HALF)])
        out[m] = even + odd
        out[9 - m] = even - odd
    return out


def tile(t):
    return slice(t * LANES, (t + 1) * LANES)


def roll_lanes(x, shift):
    return pltpu.roll(x, shift % LANES, 1)


def roll_rows(x, shift):
    return pltpu.roll(x, shift % 8, 0)


def two_parts(x):
    high = x.astype(jnp.bfloat16)
    low = (x - high.astype(jnp.float32)).astype(jnp.bfloat16)
    return jnp.concatenate([high, low], axis=1)


def steps(start, count, per, fn):
    if per == count:
        for k in range(count):
            fn(start + k, 0)
        return

    def several(step, carry):
        for k in range(per):
            fn(start + step * per + k, 0)
        return carry

    lax.fori_loop(0, count // per, several, 0)


def kernel(
    v_hbm, g_hbm, place_ref, out_ref,
    v, g, coef, f0, fl, lhs, perm, back, place_in, canon, got,
    zs, zr, ys, yr, xs, xr, tops, tops_in, ends, ends_in,
    v_sem, g_sem, place_sem, z_sem, y_sem, x_sem, inner_send, inner_recv, edge_send, edge_recv,
):
    elem = lax.axis_index("elem")
    c = lax.axis_index("comp")
    r = lax.axis_index("rep")
    o = 1 - c
    elem_count = lax.axis_size("elem")
    grid_x = elem_count // GRID_Y
    sx = elem // GRID_Y
    sy = elem % GRID_Y
    y_up = sx * GRID_Y + (sy + 1) % GRID_Y
    y_down = sx * GRID_Y + (sy + GRID_Y - 1) % GRID_Y
    x_up = (elem + GRID_Y) % elem_count
    x_down = (elem + elem_count - GRID_Y) % elem_count

    for i in range(HALF):
        pltpu.make_async_copy(v_hbm.at[:, i], v.at[:, i], v_sem.at[i]).start()
        pltpu.make_async_copy(g_hbm.at[:, 0, i], g.at[:, 0, i], g_sem.at[0, i]).start()
    others = (
        (elem, o, r), (elem, c, 1 - r), (y_up, c, r), (y_down, c, r), (x_up, c, r), (x_down, c, r),
    )
    barrier = pltpu.get_barrier_semaphore()
    for other in others:
        pl.semaphore_signal(barrier, inc=1, device_id=other, device_id_type=MESH)

    for kind in range(2):
        for m in range(HALF):
            for i in range(HALF):
                first = float(TABLE[i, (5 + m) if kind == 0 else m])
                second = float(TABLE[5 + i, m if kind == 0 else (5 + m)])
                coef[(kind * HALF + m) * HALF + i] = jnp.where(c == 0, first, second).astype(jnp.float32)

    rows_iota = lax.broadcasted_iota(jnp.int32, (ELEMS, ELEMS), 0)
    lanes_iota = lax.broadcasted_iota(jnp.int32, (LANES, ELEMS), 1).astype(jnp.float32)

    def fill_perm(q, places):
        for t in range(TILES):
            place = jnp.broadcast_to(places[:, tile(t)].astype(jnp.float32), (LANES, LANES)).T
            place = jnp.concatenate([place] * TILES, axis=1)
            part = jnp.where(lanes_iota == place, 1.0, 0.0).astype(jnp.bfloat16)
            for copy in range(2):
                perm[q, copy * ELEMS + t * LANES : copy * ELEMS + (t + 1) * LANES, :] = part

    back_half = jnp.where(rows_iota == place_ref[...], 1.0, 0.0).astype(jnp.bfloat16)
    back[0:ELEMS, :] = back_half
    back[ELEMS : 2 * ELEMS, :] = back_half
    fill_perm(c, place_ref[...])
    lhs[...] = jnp.zeros_like(lhs)

    pl.semaphore_wait(barrier, len(others))
    place_copy = pltpu.make_async_remote_copy(
        src_ref=place_ref, dst_ref=place_in, send_sem=place_sem.at[0], recv_sem=place_sem.at[1],
        device_id=(elem, o, r), device_id_type=MESH,
    )
    place_copy.start()

    def first_flux(i, carry):
        pltpu.make_async_copy(v_hbm.at[:, i], v.at[:, i], v_sem.at[i]).wait()
        pltpu.make_async_copy(g_hbm.at[:, 0, i], g.at[:, 0, i], g_sem.at[0, i]).wait()
        for j in (1, 2):
            pltpu.make_async_copy(g_hbm.at[:, j, i], g.at[:, j, i], g_sem.at[j, i]).start()

        def at_b(b, carry):
            for k in range(NODES):
                f0[i, b, k] = (
                    g[0, 0, i, b, k] * v[0, i, b, k]
                    + g[1, 0, i, b, k] * v[1, i, b, k]
                    + g[2, 0, i, b, k] * v[2, i, b, k]
                )
            return carry

        steps(0, NODES, 2, at_b)
        return carry

    lax.fori_loop(0, HALF, first_flux, 0)

    place_copy.wait()
    fill_perm(o, place_in[...])

    def inner_copy(a):
        return pltpu.make_async_remote_copy(
            src_ref=canon.at[o, a, 0:64], dst_ref=got.at[a, 0:64],
            send_sem=inner_send.at[a], recv_sem=inner_recv.at[a],
            device_id=(elem, o, r), device_id_type=MESH,
        )

    def is_inner(a):
        return jnp.logical_and(a > 0, a < NODES - 1)

    def mix_planes(base, b):
        weights = [coef[base + i] for i in range(HALF)]
        for k in range(NODES):
            fl[b, k] = weighted([f0[i, b, k] for i in range(HALF)], weights)

    def gather_rows():
        for q in range(2):
            for t in range(TILES):
                for b in range(8):
                    lhs[q, b * 8 : b * 8 + 8, tile(t)] = fl[b + 1, 1:9, q, tile(t)]
                lhs[q, 64:72, tile(t)] = fl[1:9, 0, q, tile(t)]
                lhs[q, 72:80, tile(t)] = fl[0, 1:9, q, tile(t)]
                lhs[q, 80:88, tile(t)] = fl[1:9, 9, q, tile(t)]
                lhs[q, 88:96, tile(t)] = fl[9, 1:9, q, tile(t)]
            lhs[q, 96:97, :] = fl[0, 0, q : q + 1, :]
            lhs[q, 97:98, :] = fl[0, 9, q : q + 1, :]
            lhs[q, 98:99, :] = fl[9, 0, q : q + 1, :]
            lhs[q, 99:100, :] = fl[9, 9, q : q + 1, :]

    def to_canon(a):
        for q in (o, c):
            canon[q, a] = jnp.dot(two_parts(lhs[q]), perm[q], preferred_element_type=jnp.float32)

    def send_if_inner(a):
        @pl.when(is_inner(a))
        def _():
            inner_copy(a).start()

    far = HALF * o
    near = HALF * c

    def far_plane(m, carry):
        def at_b(b, carry):
            mix_planes(m * HALF, b)
            return carry

        steps(0, NODES, 2, at_b)
        gather_rows()
        to_canon(far + m)
        send_if_inner(far + m)
        return carry

    lax.fori_loop(0, HALF, far_plane, 0)

    def near_plane(m, carry):
        for j in (1, 2):
            pltpu.make_async_copy(g_hbm.at[:, j, m], g.at[:, j, m], g_sem.at[j, m]).wait()

        def flux(j, b, k):
            return (
                g[0, j, m, b, k] * v[0, m, b, k]
                + g[1, j, m, b, k] * v[1, m, b, k]
                + g[2, j, m, b, k] * v[2, m, b, k]
            )

        def at_b(b, carry):
            base = (HALF + m) * HALF
            weights = [coef[base + i] for i in range(HALF)]
            out = along([flux(2, b, k) for k in range(NODES)])
            for k in range(NODES):
                fl[b, k] = out[k] + weighted([f0[i, b, k] for i in range(HALF)], weights)
            return carry

        steps(0, NODES, 2, at_b)

        def at_k(k, carry):
            out = along([flux(1, b, k) for b in range(NODES)])
            for b in range(NODES):
                fl[b, k] = fl[b, k] + out[b]
            return carry

        steps(0, NODES, 2, at_k)
        gather_rows()
        to_canon(near + m)
        send_if_inner(near + m)
        return carry

    lax.fori_loop(0, HALF, near_plane, 0)

    lane = lax.broadcasted_iota(jnp.int32, (8, LANES), 1)
    row = lax.broadcasted_iota(jnp.int32, (8, LANES), 0)
    zi = lane % 8
    yi = (lane // 8) % 8
    low_half = lane < 64
    zero = jnp.zeros((8, LANES), jnp.float32)
    c_lo = jnp.logical_or(row == 0, row == 2)
    c_hi = jnp.logical_or(row == 1, row == 3)
    b_lo = row < 2
    b_hi = jnp.logical_or(row == 2, row == 3)

    def edge_pass(step, carry):
        spots = [
            (q, 2 * step + k, lo_row, hi_row, tile(t))
            for k in range(2) for q in range(2) for t in range(TILES) for lo_row, hi_row in ((64, 80), (72, 88))
        ]
        held = [
            (canon[q, a, lo_row : lo_row + 8, lanes], canon[q, a, hi_row : hi_row + 8, lanes])
            for q, a, lo_row, hi_row, lanes in spots
        ]
        for (q, a, lo_row, hi_row, lanes), (lo, hi) in zip(spots, held):
            index, shift = (zi, 1) if lo_row == 64 else (yi, 8)
            canon[q, a, lo_row : lo_row + 8, lanes] = lo + jnp.where(index > 0, roll_lanes(hi, shift), zero)
            canon[q, a, hi_row : hi_row + 8, lanes] = hi + jnp.where(index < 7, roll_lanes(lo, -shift), zero)
        return carry

    def corner_pass(step, carry):
        spots = [(q, 5 * step + k, tile(t)) for k in range(5) for q in range(2) for t in range(TILES)]
        held = [canon[q, a, 96:104, lanes] for q, a, lanes in spots]
        held = [
            k
            + jnp.where(jnp.logical_and(c_lo, zi > 0), roll_lanes(roll_rows(k, -1), 1), zero)
            + jnp.where(jnp.logical_and(c_hi, zi < 7), roll_lanes(roll_rows(k, 1), -1), zero)
            for k in held
        ]
        held = [
            k
            + jnp.where(jnp.logical_and(b_lo, yi > 0), roll_lanes(roll_rows(k, -2), 8), zero)
            + jnp.where(jnp.logical_and(b_hi, yi < 7), roll_lanes(roll_rows(k, 2), -8), zero)
            for k in held
        ]
        for (q, a, lanes), k in zip(spots, held):
            canon[q, a, 96:104, lanes] = k
        return carry

    lax.fori_loop(0, NODES // 2, edge_pass, 0)
    lax.fori_loop(0, 2, corner_pass, 0)

    def x_pass(block, carry):
        here = pl.ds(block * 8, 8)
        for q in range(2):
            lo = [canon[q, 0, here, tile(t)] for t in range(TILES)]
            hi = [canon[q, 9, here, tile(t)] for t in range(TILES)]
            lo_rolled = [roll_lanes(x, 64) for x in lo] + [zero]
            hi_rolled = [roll_lanes(x, 64) for x in hi] + [zero]
            for t in range(TILES):
                canon[q, 0, here, tile(t)] = lo[t] + jnp.where(low_half, hi_rolled[t - 1], hi_rolled[t])
                canon[q, 9, here, tile(t)] = hi[t] + jnp.where(low_half, lo_rolled[t], lo_rolled[t + 1])
        return carry

    steps(0, ROWS // 8, 13, x_pass)

    def pack_top(parts, index, step):
        total = parts[0]
        for u in range(1, len(parts)):
            total = jnp.where(index == 7 - u, roll_lanes(parts[u], -step * u), total)
        return total

    def pack_low(parts, index, step):
        total = parts[0]
        for u in range(1, len(parts)):
            total = jnp.where(index == u, roll_lanes(parts[u], step * u), total)
        return total

    def six(a, rows):
        return [canon[q, a, rows, tile(t)] for q in range(2) for t in range(TILES)]

    def on(flag):
        return jnp.where(flag, 1.0, 0.0).astype(jnp.float32)

    def z_pack(a, carry):
        corner = six(a, slice(96, 104))
        zs[0, a, 0:8] = pack_top(six(a, slice(80, 88)), zi, 1)
        zs[0, a, 8:16] = pack_top(corner, zi, 1)
        zs[1, a, 0:8] = pack_low(six(a, slice(64, 72)), zi, 1)
        zs[1, a, 8:16] = pack_low(corner, zi, 1)
        return carry

    steps(0, NODES, NODES, z_pack)
    z_copy = pltpu.make_async_remote_copy(
        src_ref=zs, dst_ref=zr, send_sem=z_sem.at[0], recv_sem=z_sem.at[1],
        device_id=(elem, c, 1 - r), device_id_type=MESH,
    )
    z_copy.start()

    def put(a, b_row, value, t, first):
        start = ((a * 10 + b_row) * 10 + 1) * 3 + t
        out_ref[pl.ds(start, 8, stride=3), :] = value[first : first + 8, tile(t)]

    def put_column(a, k_row, value, t, first):
        start = ((a * 10 + 1) * 10 + k_row) * 3 + t
        out_ref[pl.ds(start, 8, stride=30), :] = value[first : first + 8, tile(t)]

    def put_edges(a, value, first):
        for t in range(TILES):
            put_column(a, 0, value, t, first)
            put(a, 0, value, t, first + 8)
            put_column(a, 9, value, t, first + 16)
            put(a, 9, value, t, first + 24)
            for number, (b, k) in enumerate(((0, 0), (0, 9), (9, 0), (9, 9))):
                start = ((a * 10 + b) * 10 + k) * 3 + t
                out_ref[pl.ds(start, 1), :] = value[first + 32 + number : first + 33 + number, tile(t)]

    def inner_done(a, carry):
        @pl.when(is_inner(a))
        def _():
            inner_copy(a).wait_recv()
            total = canon[c, a, 0:64] + got[a, 0:64]
            value = jnp.dot(two_parts(total), back[...], preferred_element_type=jnp.float32)
            for t in range(TILES):
                for b in range(8):
                    put(a, b + 1, value, t, b * 8)

        return carry

    lax.fori_loop(near, near + 2, inner_done, 0)

    z_copy.wait_recv()
    r0, r1 = on(r == 0), on(r == 1)

    def z_unpack(a, carry):
        tops_here = [zr[0, a, 0:8], roll_rows(zr[0, a, 8:16], -1)]
        lows_here = [zr[1, a, 0:8], roll_rows(zr[1, a, 8:16], 1)]
        for t in range(TILES):
            for kind in range(2):
                top_rows = slice(80, 88) if kind == 0 else slice(96, 104)
                low_rows = slice(64, 72) if kind == 0 else slice(96, 104)
                top_mask = zi == 7 if kind == 0 else jnp.logical_and(c_hi, zi == 7)
                low_mask = zi == 0 if kind == 0 else jnp.logical_and(c_lo, zi == 0)
                from_above = [roll_lanes(lows_here[kind], 7 - (3 * q + t)) for q in range(2)]
                from_below = [roll_lanes(tops_here[kind], 3 * q + t - 7) for q in range(2)]
                adds = (
                    (0, top_rows, top_mask, from_above[0] * r0 + from_above[1] * r1),
                    (1, top_rows, top_mask, from_above[1] * r0),
                    (0, low_rows, low_mask, from_below[0] * r1),
                    (1, low_rows, low_mask, from_below[0] * r0 + from_below[1] * r1),
                )
                for q, rows, mask, value in adds:
                    canon[q, a, rows, tile(t)] = canon[q, a, rows, tile(t)] + jnp.where(mask, value, zero)
        return carry

    steps(0, NODES, NODES, z_unpack)

    def y_pack(a, carry):
        corner = six(a, slice(96, 104))
        ys[0, a, 0:8] = pack_top(six(a, slice(88, 96)), yi, 8)
        ys[0, a, 8:16] = pack_top(corner, yi, 8)
        ys[1, a, 0:8] = pack_low(six(a, slice(72, 80)), yi, 8)
        ys[1, a, 8:16] = pack_low(corner, yi, 8)
        return carry

    steps(0, NODES, NODES, y_pack)
    y_copies = [
        pltpu.make_async_remote_copy(
            src_ref=ys.at[way], dst_ref=yr.at[way], send_sem=y_sem.at[0, way], recv_sem=y_sem.at[1, way],
            device_id=(y_up if way == 0 else y_down, c, r), device_id_type=MESH,
        )
        for way in range(2)
    ]
    for copy in y_copies:
        copy.start()

    lax.fori_loop(near + 2, near + 4, inner_done, 0)

    for copy in y_copies:
        copy.wait_recv()
    y_has_up, y_has_down = on(sy < GRID_Y - 1), on(sy > 0)

    def y_unpack(a, carry):
        below = [yr[0, a, 0:8] * y_has_down, roll_rows(yr[0, a, 8:16], -2) * y_has_down]
        above = [yr[1, a, 0:8] * y_has_up, roll_rows(yr[1, a, 8:16], 2) * y_has_up]
        for q in range(2):
            for t in range(TILES):
                u = 3 * q + t
                for kind in range(2):
                    top_rows = slice(88, 96) if kind == 0 else slice(96, 104)
                    low_rows = slice(72, 80) if kind == 0 else slice(96, 104)
                    top_mask = yi == 7 if kind == 0 else jnp.logical_and(b_hi, yi == 7)
                    low_mask = yi == 0 if kind == 0 else jnp.logical_and(b_lo, yi == 0)
                    up = jnp.where(top_mask, roll_lanes(above[kind], 8 * (7 - u)), zero)
                    down = jnp.where(low_mask, roll_lanes(below[kind], 8 * (u - 7)), zero)
                    canon[q, a, top_rows, tile(t)] = canon[q, a, top_rows, tile(t)] + up
                    canon[q, a, low_rows, tile(t)] = canon[q, a, low_rows, tile(t)] + down
        return carry

    steps(0, NODES, NODES, y_unpack)

    def x_pack(block, carry):
        here = pl.ds(block * 8, 8)
        xs[0, here] = jnp.where(low_half, roll_lanes(canon[0, 9, here, tile(2)], 64), canon[1, 9, here, tile(2)])
        xs[1, here] = jnp.where(low_half, canon[0, 0, here, tile(0)], roll_lanes(canon[1, 0, here, tile(0)], 64))
        return carry

    steps(0, ROWS // 8, 13, x_pack)
    x_copies = [
        pltpu.make_async_remote_copy(
            src_ref=xs.at[way], dst_ref=xr.at[way], send_sem=x_sem.at[0, way], recv_sem=x_sem.at[1, way],
            device_id=(x_up if way == 0 else x_down, c, r), device_id_type=MESH,
        )
        for way in range(2)
    ]
    for copy in x_copies:
        copy.start()

    def edge_copy(number, source, target):
        return pltpu.make_async_remote_copy(
            src_ref=source, dst_ref=target, send_sem=edge_send.at[number], recv_sem=edge_recv.at[number],
            device_id=(elem, o, r), device_id_type=MESH,
        )

    edges = [
        edge_copy(0, canon.at[o, 1:9, 64:80], got.at[1:9, 64:80]),
        edge_copy(1, tops.at[1:9], tops_in.at[1:9]),
        edge_copy(2, canon.at[o, 0, 0:80], got.at[0, 0:80]),
        edge_copy(3, tops.at[0], tops_in.at[0]),
        edge_copy(4, ends, ends_in),
    ]

    def fill_tops(a, carry):
        tops[a, 0:8] = pack_top([canon[o, a, 80:88, tile(t)] for t in range(TILES)], zi, 1)
        tops[a, 8:16] = pack_top([canon[o, a, 88:96, tile(t)] for t in range(TILES)], yi, 8)
        corner = [canon[o, a, 96:104, tile(t)] for t in range(TILES)]
        packed = jnp.where(row < 2, pack_top(corner, zi, 1), pack_top(corner, yi, 8))
        for t in range(TILES):
            packed = jnp.where(row == 4 + t, roll_rows(corner[t], 4 + t), packed)
        tops[a, 16:24] = packed
        return carry

    edges[0].start()
    steps(1, NODES - 2, NODES - 2, fill_tops)
    lax.fori_loop(near + 4, near + 5, inner_done, 0)
    edges[1].start()

    for copy in x_copies:
        copy.wait_recv()
    x_has_up, x_has_down = on(sx < grid_x - 1), on(sx > 0)

    def x_unpack(block, carry):
        here = pl.ds(block * 8, 8)
        below = xr[0, here] * x_has_down
        above = xr[1, here] * x_has_up
        low = (jnp.where(low_half, below, zero), jnp.where(low_half, roll_lanes(below, 64), zero))
        top = (jnp.where(low_half, zero, roll_lanes(above, 64)), jnp.where(low_half, zero, above))
        for q in range(2):
            canon[q, 0, here, tile(0)] = canon[q, 0, here, tile(0)] + low[q]
            canon[q, 9, here, tile(2)] = canon[q, 9, here, tile(2)] + top[q]
        return carry

    steps(0, ROWS // 8, 13, x_unpack)
    edges[2].start()
    fill_tops(0, 0)
    blocks = [canon[o, 9, k * 8 : k * 8 + 8, tile(2)] for k in range(ROWS // 8)] + [zero]
    for k in range(7):
        ends[k * 8 : k * 8 + 8] = jnp.where(low_half, roll_lanes(blocks[k], 64), blocks[k + 7])
    lax.fori_loop(far, far + 1, inner_done, 0)
    edges[3].start()
    edges[4].start()
    lax.fori_loop(far + 1, far + 5, inner_done, 0)

    def complete(a, carry):
        for t in range(TILES):
            top = tops_in[a, 0:8]
            lo = got[a, 64:72, tile(t)]
            got[a, 80:88, tile(t)] = jnp.where(zi < 7, roll_lanes(lo, -1), roll_lanes(top, t))
            top = tops_in[a, 8:16]
            lo = got[a, 72:80, tile(t)]
            got[a, 88:96, tile(t)] = jnp.where(yi < 7, roll_lanes(lo, -8), roll_lanes(top, 8 * t))
            top = tops_in[a, 16:24]
            full = roll_rows(top, -4 - t)
            after = jnp.where(zi < 7, roll_rows(roll_lanes(full, -1), 1), roll_lanes(top, t))
            full = jnp.where(row == 0, full, after)
            after = jnp.where(yi < 7, roll_rows(roll_lanes(full, -8), 2), roll_lanes(top, 8 * t))
            got[a, 96:104, tile(t)] = jnp.where(row < 2, full, jnp.where(row < 4, after, zero))
        return carry

    for number in range(2):
        edges[number].wait_recv()
    steps(1, NODES - 2, NODES - 2, complete)

    def pair_done(pair, carry):
        start = 1 + pair * 4
        total = canon[c, pl.ds(start, 4), 64:104] + got[pl.ds(start, 4), 64:104]
        value = jnp.dot(
            two_parts(total.reshape(160, ELEMS)), back[...], preferred_element_type=jnp.float32
        )
        for k in range(4):
            put_edges(start + k, value, k * 40)
        return carry

    lax.fori_loop(0, 2, pair_done, 0)

    for number in range(2, 5):
        edges[number].wait_recv()
    complete(0, 0)

    for k in range(ROWS // 8):
        here = slice(k * 8, k * 8 + 8)
        end = ends_in[(k % 7) * 8 : (k % 7) * 8 + 8]
        lo = [roll_lanes(got[0, here, tile(t)], 64) for t in range(TILES)]
        lo.append(roll_lanes(end, 64) if k < 7 else end)
        for t in range(TILES):
            got[9, here, tile(t)] = jnp.where(low_half, lo[t], lo[t + 1])

    for a in (0, 9):
        total = canon[c, a] + got[a]
        value = jnp.dot(two_parts(total), back[...], preferred_element_type=jnp.float32)
        for t in range(TILES):
            for b in range(8):
                put(a, b + 1, value, t, b * 8)
        put_edges(a, value, 64)

    z_copy.wait_send()
    for copy in y_copies + x_copies + edges:
        copy.wait_send()

    def sent(a, carry):
        inner_copy(a).wait_send()
        return carry

    lax.fori_loop(1, NODES - 1, sent, 0)


def body(velocity, geometry, element_place):
    vmem = pltpu.VMEM
    dma = pltpu.SemaphoreType.DMA
    f32 = jnp.float32
    out = pl.pallas_call(
        kernel,
        out_shape=pltpu.VMEM((NODES * NODES * NODES * TILES, LANES), f32),
        in_specs=[
            pl.BlockSpec(memory_space=pl.ANY),
            pl.BlockSpec(memory_space=pl.ANY),
            pl.BlockSpec(memory_space=pltpu.VMEM),
        ],
        out_specs=pl.BlockSpec(memory_space=pltpu.VMEM),
        scratch_shapes=[
            vmem((3, HALF, NODES, NODES, 2, ELEMS), f32),
            vmem((3, 3, HALF, NODES, NODES, 2, ELEMS), f32),
            pltpu.SMEM((2 * HALF * HALF,), f32),
            vmem((HALF, NODES, NODES, 2, ELEMS), f32),
            vmem((NODES, NODES, 2, ELEMS), f32),
            vmem((2, ROWS, ELEMS), f32),
            vmem((2, 2 * ELEMS, ELEMS), jnp.bfloat16),
            vmem((2 * ELEMS, ELEMS), jnp.bfloat16),
            vmem((1, ELEMS), jnp.int32),
            vmem((2, NODES, ROWS, ELEMS), f32),
            vmem((NODES, ROWS, ELEMS), f32),
            vmem((2, NODES, 16, LANES), f32),
            vmem((2, NODES, 16, LANES), f32),
            vmem((2, NODES, 16, LANES), f32),
            vmem((2, NODES, 16, LANES), f32),
            vmem((2, ROWS, LANES), f32),
            vmem((2, ROWS, LANES), f32),
            vmem((NODES - 1, 24, LANES), f32),
            vmem((NODES - 1, 24, LANES), f32),
            vmem((56, LANES), f32),
            vmem((56, LANES), f32),
            dma((HALF,)), dma((3, HALF)), dma((2,)), dma((2,)), dma((2, 2)), dma((2, 2)),
            dma((NODES,)), dma((NODES,)), dma((5,)), dma((5,)),
        ],
        compiler_params=pltpu.CompilerParams(
            collective_id=0, has_side_effects=True, vmem_limit_bytes=60 * 1024 * 1024
        ),
    )(velocity, geometry, element_place)
    return out.reshape(NODES, NODES, NODES, 1, ELEMS)


def solution(mesh):
    placed = (
        P(None, "comp", None, None, None, ("elem", "rep")),
        P(None, None, "comp", None, None, None, ("elem", "rep")),
        P("comp", ("elem", "rep")),
    )
    return jax.shard_map(
        body,
        mesh=mesh,
        in_specs=placed,
        out_specs=P(None, None, None, "comp", ("elem", "rep")),
        check_vma=False,
    )
```

```python
import jax
import jax.numpy as jnp
import numpy as np
from jax import lax
from jax.experimental import pallas as pl
from jax.experimental.pallas import tpu as pltpu
from jax.sharding import PartitionSpec as P

BLOCK_X = 6
BLOCK_Y = 8
BLOCK_Z = 8
GRID_Y = 4
NODES = 10
HALF = 5
ELEMS = 384
LANES = 128
TILES = 3
ROWS = 104
MESH = pl.DeviceIdType.MESH


def legendre_columns(points, degree):
    columns = [points * 0.0 + 1.0, points]
    for order in range(2, degree + 1):
        columns.append(
            ((2 * order - 1) * points * columns[order - 1] - (order - 1) * columns[order - 2])
            / order
        )
    return columns


def derivative_table(node_count):
    degree = node_count - 1
    points = np.cos(np.pi * np.arange(node_count) / degree)
    for sweep in range(100):
        columns = legendre_columns(points, degree)
        points = points - (points * columns[degree] - columns[degree - 1]) / (
            node_count * columns[degree]
        )
    points = np.sort(points)
    values = legendre_columns(points, degree)[degree]
    identity = np.eye(node_count)
    spacing = points[:, None] - points[None, :] + identity
    matrix = values[:, None] / (values[None, :] * spacing)
    matrix = np.where(identity > 0.5, 0.0, matrix)
    matrix[0, 0] = -degree * (degree + 1) / 4.0
    matrix[degree, degree] = degree * (degree + 1) / 4.0
    return matrix


TABLE = derivative_table(NODES)
EVEN = [[float(0.5 * (TABLE[i, m] + TABLE[i, 9 - m])) for m in range(HALF)] for i in range(HALF)]
ODD = [[float(0.5 * (TABLE[i, m] - TABLE[i, 9 - m])) for m in range(HALF)] for i in range(HALF)]


def weighted(terms, weights):
    total = terms[0] * weights[0]
    for term, weight in zip(terms[1:], weights[1:]):
        total = total + term * weight
    return total


def along(values):
    minus = [values[i] - values[9 - i] for i in range(HALF)]
    plus = [values[i] + values[9 - i] for i in range(HALF)]
    out = [None] * NODES
    for m in range(HALF):
        even = weighted(minus, [EVEN[i][m] for i in range(HALF)])
        odd = weighted(plus, [ODD[i][m] for i in range(HALF)])
        out[m] = even + odd
        out[9 - m] = even - odd
    return out


def tile(t):
    return slice(t * LANES, (t + 1) * LANES)


def roll_lanes(x, shift):
    return pltpu.roll(x, shift % LANES, 1)


def roll_rows(x, shift):
    return pltpu.roll(x, shift % 8, 0)


def two_parts(x):
    high = x.astype(jnp.bfloat16)
    low = (x - high.astype(jnp.float32)).astype(jnp.bfloat16)
    return jnp.concatenate([high, low], axis=1)


def steps(start, count, per, fn):
    if per == count:
        for k in range(count):
            fn(start + k, 0)
        return

    def several(step, carry):
        for k in range(per):
            fn(start + step * per + k, 0)
        return carry

    lax.fori_loop(0, count // per, several, 0)


def kernel(
    v_hbm, g_hbm, place_ref, out_ref,
    v, g, coef, f0, fl, perm, back, place_in, raw, canon, got,
    zs, zr, ys, yr, xs, xr, tops, tops_in, ends, ends_in,
    v_sem, g_sem, place_sem, z_sem, y_sem, x_sem, inner_send, inner_recv, edge_send, edge_recv,
):
    elem = lax.axis_index("elem")
    c = lax.axis_index("comp")
    r = lax.axis_index("rep")
    o = 1 - c
    elem_count = lax.axis_size("elem")
    grid_x = elem_count // GRID_Y
    sx = elem // GRID_Y
    sy = elem % GRID_Y
    y_links = ((elem + 1, sy < GRID_Y - 1), (elem - 1, sy > 0))
    x_links = ((elem + GRID_Y, sx < grid_x - 1), (elem - GRID_Y, sx > 0))

    for i in range(HALF):
        pltpu.make_async_copy(v_hbm.at[:, i], v.at[:, i], v_sem.at[i]).start()
        pltpu.make_async_copy(g_hbm.at[:, 0, i], g.at[:, 0, i], g_sem.at[0, i]).start()
    barrier = pltpu.get_barrier_semaphore()
    expected = 2
    for other in ((elem, o, r), (elem, c, 1 - r)):
        pl.semaphore_signal(barrier, inc=1, device_id=other, device_id_type=MESH)
    for near_elem, exists in y_links + x_links:
        expected = expected + exists.astype(jnp.int32)

        @pl.when(exists)
        def _(near_elem=near_elem):
            pl.semaphore_signal(barrier, inc=1, device_id=(near_elem, c, r), device_id_type=MESH)

    pl.semaphore_wait(barrier, expected)
    place_copy = pltpu.make_async_remote_copy(
        src_ref=place_ref, dst_ref=place_in, send_sem=place_sem.at[0], recv_sem=place_sem.at[1],
        device_id=(elem, o, r), device_id_type=MESH,
    )
    place_copy.start()

    for links, target in ((y_links, yr), (x_links, xr)):
        for way in range(2):
            @pl.when(jnp.logical_not(links[1 - way][1]))
            def _(target=target, way=way):
                target[way] = jnp.zeros(target.shape[1:], jnp.float32)

    for kind in range(2):
        for m in range(HALF):
            for i in range(HALF):
                first = float(TABLE[i, (5 + m) if kind == 0 else m])
                second = float(TABLE[5 + i, m if kind == 0 else (5 + m)])
                coef[(kind * HALF + m) * HALF + i] = jnp.where(c == 0, first, second).astype(jnp.float32)

    rows_iota = lax.broadcasted_iota(jnp.int32, (ELEMS, ELEMS), 0)
    lanes_iota = lax.broadcasted_iota(jnp.int32, (LANES, ELEMS), 1).astype(jnp.float32)

    def fill_perm(q, places):
        for t in range(TILES):
            place = jnp.broadcast_to(places[:, tile(t)].astype(jnp.float32), (LANES, LANES)).T
            place = jnp.concatenate([place] * TILES, axis=1)
            part = jnp.where(lanes_iota == place, 1.0, 0.0).astype(jnp.bfloat16)
            for copy in range(2):
                perm[q, copy * ELEMS + t * LANES : copy * ELEMS + (t + 1) * LANES, :] = part

    back_half = jnp.where(rows_iota == place_ref[...], 1.0, 0.0).astype(jnp.bfloat16)
    back[0:ELEMS, :] = back_half
    back[ELEMS : 2 * ELEMS, :] = back_half
    fill_perm(c, place_ref[...])
    raw[:, :, 96:104] = jnp.zeros((2, NODES, 8, ELEMS), jnp.float32)

    def first_flux(i, carry):
        pltpu.make_async_copy(v_hbm.at[:, i], v.at[:, i], v_sem.at[i]).wait()
        pltpu.make_async_copy(g_hbm.at[:, 0, i], g.at[:, 0, i], g_sem.at[0, i]).wait()
        for j in (1, 2):
            pltpu.make_async_copy(g_hbm.at[:, j, i], g.at[:, j, i], g_sem.at[j, i]).start()

        def at_b(b, carry):
            for k in range(NODES):
                f0[i, b, k] = (
                    g[0, 0, i, b, k] * v[0, i, b, k]
                    + g[1, 0, i, b, k] * v[1, i, b, k]
                    + g[2, 0, i, b, k] * v[2, i, b, k]
                )
            return carry

        steps(0, NODES, 2, at_b)
        return carry

    lax.fori_loop(0, HALF, first_flux, 0)

    place_copy.wait()
    fill_perm(o, place_in[...])

    def inner_copy(a):
        return pltpu.make_async_remote_copy(
            src_ref=canon.at[o, a, 0:64], dst_ref=got.at[a, 0:64],
            send_sem=inner_send.at[a], recv_sem=inner_recv.at[a],
            device_id=(elem, o, r), device_id_type=MESH,
        )

    def is_inner(a):
        return jnp.logical_and(a > 0, a < NODES - 1)

    def mix_planes(base, b):
        weights = [coef[base + i] for i in range(HALF)]
        for k in range(NODES):
            fl[b, k] = weighted([f0[i, b, k] for i in range(HALF)], weights)

    def send_if_inner(a):
        @pl.when(is_inner(a))
        def _():
            inner_copy(a).start()

    def gather_rows(a):
        for q in range(2):
            for t in range(TILES):
                for b in range(8):
                    raw[q, a, b * 8 : b * 8 + 8, tile(t)] = fl[b + 1, 1:9, q, tile(t)]
                raw[q, a, 64:72, tile(t)] = fl[1:9, 0, q, tile(t)]
                raw[q, a, 72:80, tile(t)] = fl[0, 1:9, q, tile(t)]
                raw[q, a, 80:88, tile(t)] = fl[1:9, 9, q, tile(t)]
                raw[q, a, 88:96, tile(t)] = fl[9, 1:9, q, tile(t)]
            raw[q, a, 96:97, :] = fl[0, 0, q : q + 1, :]
            raw[q, a, 97:98, :] = fl[0, 9, q : q + 1, :]
            raw[q, a, 98:99, :] = fl[9, 0, q : q + 1, :]
            raw[q, a, 99:100, :] = fl[9, 9, q : q + 1, :]

    def permuted(x, matrix):
        return jnp.dot(two_parts(x), matrix, preferred_element_type=jnp.float32)

    def to_canon(a, between=None):
        first = two_parts(raw[o, a])
        second = two_parts(raw[c, a, 64:104])
        if between is not None:
            gather_rows(between)
        canon[o, a] = jnp.dot(first, perm[o], preferred_element_type=jnp.float32)
        canon[c, a, 64:104] = jnp.dot(second, perm[c], preferred_element_type=jnp.float32)
        send_if_inner(a)

    far = HALF * o
    near = HALF * c

    def far_plane(m):
        def at_b(b, carry):
            mix_planes(m * HALF, b)
            return carry

        steps(0, NODES, 2, at_b)

    def far_step(m, carry):
        far_plane(m)
        to_canon(far + m - 1, far + m)
        return carry

    far_plane(0)
    gather_rows(far)
    to_canon(far)
    far_plane(1)
    gather_rows(far + 1)
    lax.fori_loop(2, HALF, far_step, 0)

    def near_plane(m, carry):
        for j in (1, 2):
            pltpu.make_async_copy(g_hbm.at[:, j, m], g.at[:, j, m], g_sem.at[j, m]).wait()

        def flux(j, b, k):
            return (
                g[0, j, m, b, k] * v[0, m, b, k]
                + g[1, j, m, b, k] * v[1, m, b, k]
                + g[2, j, m, b, k] * v[2, m, b, k]
            )

        def at_b(b, carry):
            base = (HALF + m) * HALF
            weights = [coef[base + i] for i in range(HALF)]
            out = along([flux(2, b, k) for k in range(NODES)])
            for k in range(NODES):
                fl[b, k] = out[k] + weighted([f0[i, b, k] for i in range(HALF)], weights)
            return carry

        steps(0, NODES, 2, at_b)

        def at_k(k, carry):
            out = along([flux(1, b, k) for b in range(NODES)])
            for b in range(NODES):
                fl[b, k] = fl[b, k] + out[b]
            return carry

        steps(0, NODES, 2, at_k)
        to_canon(jnp.where(m == 0, far + HALF - 1, near + m - 1), near + m)
        return carry

    lax.fori_loop(0, HALF, near_plane, 0)
    to_canon(near + HALF - 1)
    for a in (0, 9):
        canon[c, a, 0:64] = permuted(raw[c, a, 0:64], perm[c])

    lane = lax.broadcasted_iota(jnp.int32, (8, LANES), 1)
    row = lax.broadcasted_iota(jnp.int32, (8, LANES), 0)
    zi = lane % 8
    yi = (lane // 8) % 8
    low_half = lane < 64
    zero = jnp.zeros((8, LANES), jnp.float32)
    c_lo = jnp.logical_or(row == 0, row == 2)
    c_hi = jnp.logical_or(row == 1, row == 3)
    b_lo = row < 2
    b_hi = jnp.logical_or(row == 2, row == 3)

    def edge_pass(step, carry):
        planes = [2 * step, 2 * step + 1]
        spots = [
            (q, a, lo_row, hi_row, tile(t))
            for a in planes for q in range(2) for t in range(TILES) for lo_row, hi_row in ((64, 80), (72, 88))
        ]
        corner_spots = [(q, a, tile(t)) for a in planes for q in range(2) for t in range(TILES)]
        corners = [canon[q, a, 96:104, lanes] for q, a, lanes in corner_spots]
        held = [
            (canon[q, a, lo_row : lo_row + 8, lanes], canon[q, a, hi_row : hi_row + 8, lanes])
            for q, a, lo_row, hi_row, lanes in spots
        ]
        corners = [
            k
            + jnp.where(jnp.logical_and(c_lo, zi > 0), roll_lanes(roll_rows(k, -1), 1), zero)
            + jnp.where(jnp.logical_and(c_hi, zi < 7), roll_lanes(roll_rows(k, 1), -1), zero)
            for k in corners
        ]
        for (q, a, lo_row, hi_row, lanes), (lo, hi) in zip(spots, held):
            index, shift = (zi, 1) if lo_row == 64 else (yi, 8)
            canon[q, a, lo_row : lo_row + 8, lanes] = lo + jnp.where(index > 0, roll_lanes(hi, shift), zero)
            canon[q, a, hi_row : hi_row + 8, lanes] = hi + jnp.where(index < 7, roll_lanes(lo, -shift), zero)
        for (q, a, lanes), k in zip(corner_spots, corners):
            canon[q, a, 96:104, lanes] = (
                k
                + jnp.where(jnp.logical_and(b_lo, yi > 0), roll_lanes(roll_rows(k, -2), 8), zero)
                + jnp.where(jnp.logical_and(b_hi, yi < 7), roll_lanes(roll_rows(k, 2), -8), zero)
            )
        return carry

    lax.fori_loop(0, NODES // 2, edge_pass, 0)

    def x_pass(block, carry):
        here = pl.ds(block * 8, 8)
        for q in range(2):
            lo = [canon[q, 0, here, tile(t)] for t in range(TILES)]
            hi = [canon[q, 9, here, tile(t)] for t in range(TILES)]
            lo_rolled = [roll_lanes(x, 64) for x in lo] + [zero]
            hi_rolled = [roll_lanes(x, 64) for x in hi] + [zero]
            for t in range(TILES):
                canon[q, 0, here, tile(t)] = lo[t] + jnp.where(low_half, hi_rolled[t - 1], hi_rolled[t])
                canon[q, 9, here, tile(t)] = hi[t] + jnp.where(low_half, lo_rolled[t], lo_rolled[t + 1])
        return carry

    steps(0, ROWS // 8, 13, x_pass)

    def pack_top(parts, index, step):
        total = parts[0]
        for u in range(1, len(parts)):
            total = jnp.where(index == 7 - u, roll_lanes(parts[u], -step * u), total)
        return total

    def pack_low(parts, index, step):
        total = parts[0]
        for u in range(1, len(parts)):
            total = jnp.where(index == u, roll_lanes(parts[u], step * u), total)
        return total

    def six(a, rows):
        return [canon[q, a, rows, tile(t)] for q in range(2) for t in range(TILES)]

    def on(flag):
        return jnp.where(flag, 1.0, 0.0).astype(jnp.float32)

    def z_pack(a, carry):
        corner = six(a, slice(96, 104))
        zs[0, a, 0:8] = pack_top(six(a, slice(80, 88)), zi, 1)
        zs[0, a, 8:16] = pack_top(corner, zi, 1)
        zs[1, a, 0:8] = pack_low(six(a, slice(64, 72)), zi, 1)
        zs[1, a, 8:16] = pack_low(corner, zi, 1)
        return carry

    steps(0, NODES, NODES, z_pack)
    z_copy = pltpu.make_async_remote_copy(
        src_ref=zs, dst_ref=zr, send_sem=z_sem.at[0], recv_sem=z_sem.at[1],
        device_id=(elem, c, 1 - r), device_id_type=MESH,
    )
    z_copy.start()

    def put(a, b_row, value, t, first):
        start = ((a * 10 + b_row) * 10 + 1) * 3 + t
        out_ref[pl.ds(start, 8, stride=3), :] = value[first : first + 8, tile(t)]

    def put_column(a, k_row, value, t, first):
        start = ((a * 10 + 1) * 10 + k_row) * 3 + t
        out_ref[pl.ds(start, 8, stride=30), :] = value[first : first + 8, tile(t)]

    def put_edges(a, value, first):
        for t in range(TILES):
            put_column(a, 0, value, t, first)
            put(a, 0, value, t, first + 8)
            put_column(a, 9, value, t, first + 16)
            put(a, 9, value, t, first + 24)
            for number, (b, k) in enumerate(((0, 0), (0, 9), (9, 0), (9, 9))):
                start = ((a * 10 + b) * 10 + k) * 3 + t
                out_ref[pl.ds(start, 1), :] = value[first + 32 + number : first + 33 + number, tile(t)]

    def inner_done(a, carry):
        @pl.when(is_inner(a))
        def _():
            inner_copy(a).wait_recv()
            value = permuted(got[a, 0:64], back[...]) + raw[c, a, 0:64]
            for t in range(TILES):
                for b in range(8):
                    put(a, b + 1, value, t, b * 8)

        return carry

    lax.fori_loop(near, near + 2, inner_done, 0)

    z_copy.wait_recv()
    r0, r1 = on(r == 0), on(r == 1)

    def z_unpack(a, carry):
        tops_here = [zr[0, a, 0:8], roll_rows(zr[0, a, 8:16], -1)]
        lows_here = [zr[1, a, 0:8], roll_rows(zr[1, a, 8:16], 1)]
        for t in range(TILES):
            for kind in range(2):
                top_rows = slice(80, 88) if kind == 0 else slice(96, 104)
                low_rows = slice(64, 72) if kind == 0 else slice(96, 104)
                top_mask = zi == 7 if kind == 0 else jnp.logical_and(c_hi, zi == 7)
                low_mask = zi == 0 if kind == 0 else jnp.logical_and(c_lo, zi == 0)
                from_above = [roll_lanes(lows_here[kind], 7 - (3 * q + t)) for q in range(2)]
                from_below = [roll_lanes(tops_here[kind], 3 * q + t - 7) for q in range(2)]
                adds = (
                    (0, top_rows, top_mask, from_above[0] * r0 + from_above[1] * r1),
                    (1, top_rows, top_mask, from_above[1] * r0),
                    (0, low_rows, low_mask, from_below[0] * r1),
                    (1, low_rows, low_mask, from_below[0] * r0 + from_below[1] * r1),
                )
                for q, rows, mask, value in adds:
                    canon[q, a, rows, tile(t)] = canon[q, a, rows, tile(t)] + jnp.where(mask, value, zero)
        return carry

    steps(0, NODES, NODES, z_unpack)

    def y_pack(a, carry):
        corner = six(a, slice(96, 104))
        ys[0, a, 0:8] = pack_top(six(a, slice(88, 96)), yi, 8)
        ys[0, a, 8:16] = pack_top(corner, yi, 8)
        ys[1, a, 0:8] = pack_low(six(a, slice(72, 80)), yi, 8)
        ys[1, a, 8:16] = pack_low(corner, yi, 8)
        return carry

    steps(0, NODES, NODES, y_pack)
    y_copies = [
        pltpu.make_async_remote_copy(
            src_ref=ys.at[way], dst_ref=yr.at[way], send_sem=y_sem.at[0, way], recv_sem=y_sem.at[1, way],
            device_id=(y_links[way][0], c, r), device_id_type=MESH,
        )
        for way in range(2)
    ]
    for way in range(2):
        @pl.when(y_links[way][1])
        def _(copy=y_copies[way]):
            copy.start()


    lax.fori_loop(near + 2, near + 4, inner_done, 0)

    for way in range(2):
        @pl.when(y_links[1 - way][1])
        def _(copy=y_copies[way]):
            copy.wait_recv()


    def y_unpack(a, carry):
        below = [yr[0, a, 0:8], roll_rows(yr[0, a, 8:16], -2)]
        above = [yr[1, a, 0:8], roll_rows(yr[1, a, 8:16], 2)]
        for q in range(2):
            for t in range(TILES):
                u = 3 * q + t
                for kind in range(2):
                    top_rows = slice(88, 96) if kind == 0 else slice(96, 104)
                    low_rows = slice(72, 80) if kind == 0 else slice(96, 104)
                    top_mask = yi == 7 if kind == 0 else jnp.logical_and(b_hi, yi == 7)
                    low_mask = yi == 0 if kind == 0 else jnp.logical_and(b_lo, yi == 0)
                    up = jnp.where(top_mask, roll_lanes(above[kind], 8 * (7 - u)), zero)
                    down = jnp.where(low_mask, roll_lanes(below[kind], 8 * (u - 7)), zero)
                    canon[q, a, top_rows, tile(t)] = canon[q, a, top_rows, tile(t)] + up
                    canon[q, a, low_rows, tile(t)] = canon[q, a, low_rows, tile(t)] + down
        return carry

    steps(0, NODES, NODES, y_unpack)

    def x_pack(block, carry):
        here = pl.ds(block * 8, 8)
        xs[0, here] = jnp.where(low_half, roll_lanes(canon[0, 9, here, tile(2)], 64), canon[1, 9, here, tile(2)])
        xs[1, here] = jnp.where(low_half, canon[0, 0, here, tile(0)], roll_lanes(canon[1, 0, here, tile(0)], 64))
        return carry

    steps(0, ROWS // 8, 13, x_pack)
    x_copies = [
        pltpu.make_async_remote_copy(
            src_ref=xs.at[way], dst_ref=xr.at[way], send_sem=x_sem.at[0, way], recv_sem=x_sem.at[1, way],
            device_id=(x_links[way][0], c, r), device_id_type=MESH,
        )
        for way in range(2)
    ]
    for way in range(2):
        @pl.when(x_links[way][1])
        def _(copy=x_copies[way]):
            copy.start()


    def edge_copy(number, source, target):
        return pltpu.make_async_remote_copy(
            src_ref=source, dst_ref=target, send_sem=edge_send.at[number], recv_sem=edge_recv.at[number],
            device_id=(elem, o, r), device_id_type=MESH,
        )

    edges = [
        edge_copy(0, canon.at[o, 1:9, 64:80], got.at[1:9, 64:80]),
        edge_copy(1, tops.at[1:9], tops_in.at[1:9]),
        edge_copy(2, canon.at[o, 0, 0:80], got.at[0, 0:80]),
        edge_copy(3, tops.at[0], tops_in.at[0]),
        edge_copy(4, ends, ends_in),
    ]

    def fill_tops(a, carry):
        z_top = pack_top([canon[o, a, 80:88, tile(t)] for t in range(TILES)], zi, 1)
        y_top = pack_top([canon[o, a, 88:96, tile(t)] for t in range(TILES)], yi, 8)
        tops[a, 0:8] = jnp.where(yi > 4, y_top, jnp.where(zi > 4, z_top, roll_lanes(z_top, -27)))
        corner = [canon[o, a, 96:104, tile(t)] for t in range(TILES)]
        packed = jnp.where(row < 2, pack_top(corner, zi, 1), pack_top(corner, yi, 8))
        for t in range(TILES):
            packed = jnp.where(row == 4 + t, roll_rows(corner[t], 4 + t), packed)
        tops[a, 8:16] = packed
        return carry

    edges[0].start()
    steps(1, NODES - 2, NODES - 2, fill_tops)
    lax.fori_loop(near + 4, near + 5, inner_done, 0)
    edges[1].start()

    for way in range(2):
        @pl.when(x_links[1 - way][1])
        def _(copy=x_copies[way]):
            copy.wait_recv()


    def x_unpack(block, carry):
        here = pl.ds(block * 8, 8)
        below = xr[0, here]
        above = xr[1, here]
        low = (jnp.where(low_half, below, zero), jnp.where(low_half, roll_lanes(below, 64), zero))
        top = (jnp.where(low_half, zero, roll_lanes(above, 64)), jnp.where(low_half, zero, above))
        for q in range(2):
            canon[q, 0, here, tile(0)] = canon[q, 0, here, tile(0)] + low[q]
            canon[q, 9, here, tile(2)] = canon[q, 9, here, tile(2)] + top[q]
        return carry

    steps(0, ROWS // 8, 13, x_unpack)
    edges[2].start()
    fill_tops(0, 0)
    blocks = [canon[o, 9, k * 8 : k * 8 + 8, tile(2)] for k in range(ROWS // 8)] + [zero]
    for k in range(7):
        ends[k * 8 : k * 8 + 8] = jnp.where(low_half, roll_lanes(blocks[k], 64), blocks[k + 7])
    lax.fori_loop(far, far + 1, inner_done, 0)
    edges[3].start()
    edges[4].start()
    lax.fori_loop(far + 1, far + 5, inner_done, 0)

    def complete(a, carry):
        for t in range(TILES):
            top = tops_in[a, 0:8]
            lo = got[a, 64:72, tile(t)]
            z_top = jnp.where(yi < 5, roll_lanes(top, t), roll_lanes(top, 27 + t))
            got[a, 80:88, tile(t)] = jnp.where(zi < 7, roll_lanes(lo, -1), z_top)
            lo = got[a, 72:80, tile(t)]
            got[a, 88:96, tile(t)] = jnp.where(yi < 7, roll_lanes(lo, -8), roll_lanes(top, 8 * t))
            top = tops_in[a, 8:16]
            full = roll_rows(top, -4 - t)
            after = jnp.where(zi < 7, roll_rows(roll_lanes(full, -1), 1), roll_lanes(top, t))
            full = jnp.where(row == 0, full, after)
            after = jnp.where(yi < 7, roll_rows(roll_lanes(full, -8), 2), roll_lanes(top, 8 * t))
            got[a, 96:104, tile(t)] = jnp.where(row < 2, full, jnp.where(row < 4, after, zero))
        return carry

    for number in range(2):
        edges[number].wait_recv()
    steps(1, NODES - 2, NODES - 2, complete)

    def pair_done(pair, carry):
        start = 1 + pair * 4
        total = canon[c, pl.ds(start, 4), 64:104] + got[pl.ds(start, 4), 64:104]
        value = permuted(total.reshape(160, ELEMS), back[...])
        for k in range(4):
            put_edges(start + k, value, k * 40)
        return carry

    lax.fori_loop(0, 2, pair_done, 0)

    for number in range(2, 5):
        edges[number].wait_recv()
    complete(0, 0)

    for k in range(ROWS // 8):
        here = slice(k * 8, k * 8 + 8)
        end = ends_in[(k % 7) * 8 : (k % 7) * 8 + 8]
        lo = [roll_lanes(got[0, here, tile(t)], 64) for t in range(TILES)]
        lo.append(roll_lanes(end, 64) if k < 7 else end)
        for t in range(TILES):
            got[9, here, tile(t)] = jnp.where(low_half, lo[t], lo[t + 1])

    for a in (0, 9):
        total = canon[c, a] + got[a]
        value = permuted(total, back[...])
        for t in range(TILES):
            for b in range(8):
                put(a, b + 1, value, t, b * 8)
        put_edges(a, value, 64)

    z_copy.wait_send()
    for copy in edges:
        copy.wait_send()
    for links, copies in ((y_links, y_copies), (x_links, x_copies)):
        for way in range(2):
            @pl.when(links[way][1])
            def _(copy=copies[way]):
                copy.wait_send()

    def sent(a, carry):
        inner_copy(a).wait_send()
        return carry

    lax.fori_loop(1, NODES - 1, sent, 0)


def body(velocity, geometry, element_place):
    vmem = pltpu.VMEM
    dma = pltpu.SemaphoreType.DMA
    f32 = jnp.float32
    out = pl.pallas_call(
        kernel,
        out_shape=pltpu.VMEM((NODES * NODES * NODES * TILES, LANES), f32),
        in_specs=[
            pl.BlockSpec(memory_space=pl.ANY),
            pl.BlockSpec(memory_space=pl.ANY),
            pl.BlockSpec(memory_space=pltpu.VMEM),
        ],
        out_specs=pl.BlockSpec(memory_space=pltpu.VMEM),
        scratch_shapes=[
            vmem((3, HALF, NODES, NODES, 2, ELEMS), f32),
            vmem((3, 3, HALF, NODES, NODES, 2, ELEMS), f32),
            pltpu.SMEM((2 * HALF * HALF,), f32),
            vmem((HALF, NODES, NODES, 2, ELEMS), f32),
            vmem((NODES, NODES, 2, ELEMS), f32),
            vmem((2, 2 * ELEMS, ELEMS), jnp.bfloat16),
            vmem((2 * ELEMS, ELEMS), jnp.bfloat16),
            vmem((1, ELEMS), jnp.int32),
            vmem((2, NODES, ROWS, ELEMS), f32),
            vmem((2, NODES, ROWS, ELEMS), f32),
            vmem((NODES, ROWS, ELEMS), f32),
            vmem((2, NODES, 16, LANES), f32),
            vmem((2, NODES, 16, LANES), f32),
            vmem((2, NODES, 16, LANES), f32),
            vmem((2, NODES, 16, LANES), f32),
            vmem((2, ROWS, LANES), f32),
            vmem((2, ROWS, LANES), f32),
            vmem((NODES - 1, 16, LANES), f32),
            vmem((NODES - 1, 16, LANES), f32),
            vmem((56, LANES), f32),
            vmem((56, LANES), f32),
            dma((HALF,)), dma((3, HALF)), dma((2,)), dma((2,)), dma((2, 2)), dma((2, 2)),
            dma((NODES,)), dma((NODES,)), dma((5,)), dma((5,)),
        ],
        compiler_params=pltpu.CompilerParams(
            collective_id=0, has_side_effects=True, vmem_limit_bytes=60 * 1024 * 1024
        ),
    )(velocity, geometry, element_place)
    return out.reshape(NODES, NODES, NODES, 1, ELEMS)


def solution(mesh):
    placed = (
        P(None, "comp", None, None, None, ("elem", "rep")),
        P(None, None, "comp", None, None, None, ("elem", "rep")),
        P("comp", ("elem", "rep")),
    )
    return jax.shard_map(
        body,
        mesh=mesh,
        in_specs=placed,
        out_specs=P(None, None, None, "comp", ("elem", "rep")),
        check_vma=False,
    )
```

```python
import jax
import jax.numpy as jnp
import numpy as np
from jax import lax
from jax.experimental import pallas as pl
from jax.experimental.pallas import tpu as pltpu
from jax.sharding import PartitionSpec as P

BLOCK_X = 6
BLOCK_Y = 8
BLOCK_Z = 8
GRID_Y = 4
NODES = 10
HALF = 5
ELEMS = 384
LANES = 128
TILES = 3
ROWS = 104
MESH = pl.DeviceIdType.MESH


def legendre_columns(points, degree):
    columns = [points * 0.0 + 1.0, points]
    for order in range(2, degree + 1):
        columns.append(
            ((2 * order - 1) * points * columns[order - 1] - (order - 1) * columns[order - 2])
            / order
        )
    return columns


def derivative_table(node_count):
    degree = node_count - 1
    points = np.cos(np.pi * np.arange(node_count) / degree)
    for sweep in range(100):
        columns = legendre_columns(points, degree)
        points = points - (points * columns[degree] - columns[degree - 1]) / (
            node_count * columns[degree]
        )
    points = np.sort(points)
    values = legendre_columns(points, degree)[degree]
    identity = np.eye(node_count)
    spacing = points[:, None] - points[None, :] + identity
    matrix = values[:, None] / (values[None, :] * spacing)
    matrix = np.where(identity > 0.5, 0.0, matrix)
    matrix[0, 0] = -degree * (degree + 1) / 4.0
    matrix[degree, degree] = degree * (degree + 1) / 4.0
    return matrix


TABLE = derivative_table(NODES)
EVEN = [[float(0.5 * (TABLE[i, m] + TABLE[i, 9 - m])) for m in range(HALF)] for i in range(HALF)]
ODD = [[float(0.5 * (TABLE[i, m] - TABLE[i, 9 - m])) for m in range(HALF)] for i in range(HALF)]


def weighted(terms, weights):
    total = terms[0] * weights[0]
    for term, weight in zip(terms[1:], weights[1:]):
        total = total + term * weight
    return total


def along(values):
    minus = [values[i] - values[9 - i] for i in range(HALF)]
    plus = [values[i] + values[9 - i] for i in range(HALF)]
    out = [None] * NODES
    for m in range(HALF):
        even = weighted(minus, [EVEN[i][m] for i in range(HALF)])
        odd = weighted(plus, [ODD[i][m] for i in range(HALF)])
        out[m] = even + odd
        out[9 - m] = even - odd
    return out


def tile(t):
    return slice(t * LANES, (t + 1) * LANES)


def roll_lanes(x, shift):
    return pltpu.roll(x, shift % LANES, 1)


def roll_rows(x, shift):
    return pltpu.roll(x, shift % 8, 0)


def two_parts(x):
    high = x.astype(jnp.bfloat16)
    low = (x - high.astype(jnp.float32)).astype(jnp.bfloat16)
    return jnp.concatenate([high, low], axis=1)


def steps(start, count, per, fn):
    if per == count:
        for k in range(count):
            fn(start + k, 0)
        return

    def several(step, carry):
        for k in range(per):
            fn(start + step * per + k, 0)
        return carry

    lax.fori_loop(0, count // per, several, 0)


def kernel(
    v_hbm, g_hbm, place_ref, out_ref,
    v, g, coef, f0, fl, fn, perm, back, place_in, raw, canon, got,
    zs, zr, ys, yr, xs, xr, tops, tops_in, ends, ends_in,
    first_sem, later_sem, place_sem, z_sem, y_sem, x_sem, send_sem, inner_sem, edge_sem,
):
    elem = lax.axis_index("elem")
    c = lax.axis_index("comp")
    r = lax.axis_index("rep")
    o = 1 - c
    elem_count = lax.axis_size("elem")
    grid_x = elem_count // GRID_Y
    sx = elem // GRID_Y
    sy = elem % GRID_Y
    y_links = ((elem + 1, sy < GRID_Y - 1), (elem - 1, sy > 0))
    x_links = ((elem + GRID_Y, sx < grid_x - 1), (elem - GRID_Y, sx > 0))

    def first_copies(i, half):
        here = slice(half * HALF, half * HALF + HALF)
        return (
            pltpu.make_async_copy(v_hbm.at[:, i, here], v.at[:, i, here], first_sem.at[half, i]),
            pltpu.make_async_copy(g_hbm.at[:, 0, i, here], g.at[:, 0, i, here], first_sem.at[half, i]),
        )

    def first_arrived(i, half):
        here = slice(half * HALF, half * HALF + HALF)
        pltpu.make_async_copy(g_hbm.at[:, 0:2, i, here], g.at[:, 0:2, i, here], first_sem.at[half, i]).wait()

    def later_copy(i):
        return pltpu.make_async_copy(g_hbm.at[:, 1:3, i], g.at[:, 1:3, i], later_sem.at[i])

    for i in range(HALF):
        for copy in first_copies(i, 0):
            copy.start()

    barrier = pltpu.get_barrier_semaphore()
    expected = 2
    for other in ((elem, o, r), (elem, c, 1 - r)):
        pl.semaphore_signal(barrier, inc=1, device_id=other, device_id_type=MESH)
    for near_elem, exists in y_links + x_links:
        expected = expected + exists.astype(jnp.int32)

        @pl.when(exists)
        def _(near_elem=near_elem):
            pl.semaphore_signal(barrier, inc=1, device_id=(near_elem, c, r), device_id_type=MESH)

    pl.semaphore_wait(barrier, expected)
    place_copy = pltpu.make_async_remote_copy(
        src_ref=place_ref, dst_ref=place_in, send_sem=place_sem.at[0], recv_sem=place_sem.at[1],
        device_id=(elem, o, r), device_id_type=MESH,
    )
    place_copy.start()

    for links, target in ((y_links, yr), (x_links, xr)):
        for way in range(2):
            @pl.when(jnp.logical_not(links[1 - way][1]))
            def _(target=target, way=way):
                target[way] = jnp.zeros(target.shape[1:], jnp.float32)

    for kind in range(2):
        for m in range(HALF):
            for i in range(HALF):
                first = float(TABLE[i, (5 + m) if kind == 0 else m])
                second = float(TABLE[5 + i, m if kind == 0 else (5 + m)])
                coef[(kind * HALF + m) * HALF + i] = jnp.where(c == 0, first, second).astype(jnp.float32)

    rows_iota = lax.broadcasted_iota(jnp.int32, (ELEMS, ELEMS), 0)
    lanes_iota = lax.broadcasted_iota(jnp.int32, (LANES, ELEMS), 1).astype(jnp.float32)

    def fill_perm(q, places):
        for t in range(TILES):
            place = jnp.broadcast_to(places[:, tile(t)].astype(jnp.float32), (LANES, LANES)).T
            place = jnp.concatenate([place] * TILES, axis=1)
            part = jnp.where(lanes_iota == place, 1.0, 0.0).astype(jnp.bfloat16)
            for copy in range(2):
                perm[q, copy * ELEMS + t * LANES : copy * ELEMS + (t + 1) * LANES, :] = part

    back_half = jnp.where(rows_iota == place_ref[...], 1.0, 0.0).astype(jnp.bfloat16)
    back[0:ELEMS, :] = back_half
    back[ELEMS : 2 * ELEMS, :] = back_half
    fill_perm(c, place_ref[...])
    raw[:, :, 96:104] = jnp.zeros((2, NODES, 8, ELEMS), jnp.float32)

    far = HALF * o
    near = HALF * c

    def inner_copy(a, rows):
        return pltpu.make_async_remote_copy(
            src_ref=raw.at[o, a, rows], dst_ref=got.at[a, rows], send_sem=send_sem.at[0], recv_sem=inner_sem.at[a - 1],
            device_id=(elem, o, r), device_id_type=MESH,
        )

    def is_inner(a):
        return jnp.logical_and(a > 0, a < NODES - 1)

    def send_inner(a, halves):
        @pl.when(is_inner(a))
        def _():
            for half in halves:
                inner_copy(a, slice(half * 32, half * 32 + 32)).start()

    def first_flux(half):
        def at_plane(i, carry):
            first_arrived(i, half)
            for copy in first_copies(i, 1) if half == 0 else (later_copy(i),):
                copy.start()

            def at_b(b, carry):
                for k in range(NODES):
                    f0[i, b, k] = (
                        g[0, 0, i, b, k] * v[0, i, b, k]
                        + g[1, 0, i, b, k] * v[1, i, b, k]
                        + g[2, 0, i, b, k] * v[2, i, b, k]
                    )

            for b in range(half * HALF, half * HALF + HALF):
                at_b(b, 0)
            return carry

        return at_plane

    def mix_planes(m, half):
        weights = [coef[m * HALF + i] for i in range(HALF)]
        for b in range(half * HALF, half * HALF + HALF):
            for k in range(NODES):
                fl[m, b, k] = weighted([f0[i, b, k] for i in range(HALF)], weights)

    def gather_inner(m, a, half):
        for q in range(2):
            for t in range(TILES):
                for b in range(half * 4, half * 4 + 4):
                    raw[q, a, b * 8 : b * 8 + 8, tile(t)] = fl[m, b + 1, 1:9, q, tile(t)]

    def gather_edges(m, a):
        for q in range(2):
            for t in range(TILES):
                raw[q, a, 64:72, tile(t)] = fl[m, 1:9, 0, q, tile(t)]
                raw[q, a, 72:80, tile(t)] = fl[m, 0, 1:9, q, tile(t)]
                raw[q, a, 80:88, tile(t)] = fl[m, 1:9, 9, q, tile(t)]
                raw[q, a, 88:96, tile(t)] = fl[m, 9, 1:9, q, tile(t)]
            raw[q, a, 96:97, :] = fl[m, 0, 0, q : q + 1, :]
            raw[q, a, 97:98, :] = fl[m, 0, 9, q : q + 1, :]
            raw[q, a, 98:99, :] = fl[m, 9, 0, q : q + 1, :]
            raw[q, a, 99:100, :] = fl[m, 9, 9, q : q + 1, :]

    def permuted(x, matrix):
        return jnp.dot(two_parts(x), matrix, preferred_element_type=jnp.float32)

    def to_canon(a, between=None):
        parts = [two_parts(raw[q, a, 64:104]) for q in range(2)]
        if between is not None:
            between()
        for q in range(2):
            canon[q, a, 64:104] = jnp.dot(parts[q], perm[q], preferred_element_type=jnp.float32)

    def far_first(m, carry):
        mix_planes(m, 0)
        gather_inner(m, far + m, 0)
        send_inner(far + m, (0,))
        return carry

    def far_second(m, carry):
        mix_planes(m, 1)
        gather_inner(m, far + m, 1)
        send_inner(far + m, (1,))
        gather_edges(m, far + m)
        return carry

    lax.fori_loop(0, HALF, first_flux(0), 0)
    lax.fori_loop(0, HALF, far_first, 0)
    lax.fori_loop(0, HALF, first_flux(1), 0)
    lax.fori_loop(0, HALF, far_second, 0)
    place_copy.wait()
    fill_perm(o, place_in[...])

    def near_plane(m, carry):
        later_copy(m).wait()

        def flux(j, b, k):
            return (
                g[0, j, m, b, k] * v[0, m, b, k]
                + g[1, j, m, b, k] * v[1, m, b, k]
                + g[2, j, m, b, k] * v[2, m, b, k]
            )

        def at_b(b, carry):
            base = (HALF + m) * HALF
            weights = [coef[base + i] for i in range(HALF)]
            out = along([flux(2, b, k) for k in range(NODES)])
            for k in range(NODES):
                fn[b, k] = out[k] + weighted([f0[i, b, k] for i in range(HALF)], weights)
            return carry

        steps(0, NODES, 2, at_b)

        def at_k(k, carry):
            out = along([flux(1, b, k) for b in range(NODES)])
            for b in range(NODES):
                fl[m, b, k] = fn[b, k] + out[b]
            return carry

        steps(0, NODES, 2, at_k)

        def between():
            gather_inner(m, near + m, 0)
            gather_inner(m, near + m, 1)
            gather_edges(m, near + m)

        to_canon(far + m, between)

        @pl.when(m < 3 - c)
        def _():
            send_inner(near + m, (0, 1))

        return carry

    lax.fori_loop(0, HALF, near_plane, 0)

    for q in range(2):
        canon[q, pl.ds(near, HALF), 64:104] = permuted(
            raw[q, pl.ds(near, HALF), 64:104].reshape(HALF * 40, ELEMS), perm[q]
        ).reshape(HALF, 40, ELEMS)

    lane = lax.broadcasted_iota(jnp.int32, (8, LANES), 1)
    row = lax.broadcasted_iota(jnp.int32, (8, LANES), 0)
    zi = lane % 8
    yi = (lane // 8) % 8
    low_half = lane < 64
    zero = jnp.zeros((8, LANES), jnp.float32)
    c_lo = jnp.logical_or(row == 0, row == 2)
    c_hi = jnp.logical_or(row == 1, row == 3)
    b_lo = row < 2
    b_hi = jnp.logical_or(row == 2, row == 3)

    def line_pass(lo_row, index, shift, corner_lo, corner_hi, corner_step):
        def two_planes(step, carry):
            spots = [(q, 2 * step + k, tile(t)) for k in range(2) for q in range(2) for t in range(TILES)]
            corners = [canon[q, a, 96:104, lanes] for q, a, lanes in spots]
            lows = [canon[q, a, lo_row : lo_row + 8, lanes] for q, a, lanes in spots]
            highs = [canon[q, a, lo_row + 16 : lo_row + 24, lanes] for q, a, lanes in spots]
            for (q, a, lanes), k, lo, hi in zip(spots, corners, lows, highs):
                canon[q, a, lo_row : lo_row + 8, lanes] = lo + jnp.where(index > 0, roll_lanes(hi, shift), zero)
                canon[q, a, lo_row + 16 : lo_row + 24, lanes] = hi + jnp.where(
                    index < 7, roll_lanes(lo, -shift), zero
                )
                canon[q, a, 96:104, lanes] = (
                    k
                    + jnp.where(
                        jnp.logical_and(corner_lo, index > 0), roll_lanes(roll_rows(k, -corner_step), shift), zero
                    )
                    + jnp.where(
                        jnp.logical_and(corner_hi, index < 7), roll_lanes(roll_rows(k, corner_step), -shift), zero
                    )
                )
            return carry

        return two_planes

    z_pass = line_pass(64, zi, 1, c_lo, c_hi, 1)
    y_pass = line_pass(72, yi, 8, b_lo, b_hi, 2)

    def x_pass(block, carry):
        here = pl.ds(block * 8, 8)
        for q in range(2):
            lo = [canon[q, 0, here, tile(t)] for t in range(TILES)]
            hi = [canon[q, 9, here, tile(t)] for t in range(TILES)]
            lo_rolled = [roll_lanes(x, 64) for x in lo] + [zero]
            hi_rolled = [roll_lanes(x, 64) for x in hi] + [zero]
            for t in range(TILES):
                canon[q, 0, here, tile(t)] = lo[t] + jnp.where(low_half, hi_rolled[t - 1], hi_rolled[t])
                canon[q, 9, here, tile(t)] = hi[t] + jnp.where(low_half, lo_rolled[t], lo_rolled[t + 1])
        return carry

    def pack_top(parts, index, step):
        total = parts[0]
        for u in range(1, len(parts)):
            total = jnp.where(index == 7 - u, roll_lanes(parts[u], -step * u), total)
        return total

    def pack_low(parts, index, step):
        total = parts[0]
        for u in range(1, len(parts)):
            total = jnp.where(index == u, roll_lanes(parts[u], step * u), total)
        return total

    def six(a, rows):
        return [canon[q, a, rows, tile(t)] for q in range(2) for t in range(TILES)]

    def on(flag):
        return jnp.where(flag, 1.0, 0.0).astype(jnp.float32)

    def z_pack(a, carry):
        corner = six(a, slice(96, 104))
        zs[0, a, 0:8] = pack_top(six(a, slice(80, 88)), zi, 1)
        zs[0, a, 8:16] = pack_top(corner, zi, 1)
        zs[1, a, 0:8] = pack_low(six(a, slice(64, 72)), zi, 1)
        zs[1, a, 8:16] = pack_low(corner, zi, 1)
        return carry

    steps(0, NODES, NODES, z_pack)
    z_copy = pltpu.make_async_remote_copy(
        src_ref=zs, dst_ref=zr, send_sem=z_sem.at[0], recv_sem=z_sem.at[1],
        device_id=(elem, c, 1 - r), device_id_type=MESH,
    )
    z_copy.start()

    def x_pack(block, carry):
        here = pl.ds(block * 8, 8)
        xs[0, here] = jnp.where(low_half, roll_lanes(canon[0, 9, here, tile(2)], 64), canon[1, 9, here, tile(2)])
        xs[1, here] = jnp.where(low_half, canon[0, 0, here, tile(0)], roll_lanes(canon[1, 0, here, tile(0)], 64))
        return carry

    def x_copy(part, way):
        rows = slice(0, 64) if part == 0 else slice(64, ROWS)
        return pltpu.make_async_remote_copy(
            src_ref=xs.at[way, rows], dst_ref=xr.at[way, rows],
            send_sem=x_sem.at[0, part, way], recv_sem=x_sem.at[1, part, way],
            device_id=(x_links[way][0], c, r), device_id_type=MESH,
        )

    def x_send(part):
        for way in range(2):
            @pl.when(x_links[way][1])
            def _(copy=x_copy(part, way)):
                copy.start()

    def x_wait(part):
        for way in range(2):
            @pl.when(x_links[1 - way][1])
            def _(copy=x_copy(part, way)):
                copy.wait_recv()

    def x_unpack(block, carry):
        here = pl.ds(block * 8, 8)
        below = xr[0, here]
        above = xr[1, here]
        low = (jnp.where(low_half, below, zero), jnp.where(low_half, roll_lanes(below, 64), zero))
        top = (jnp.where(low_half, zero, roll_lanes(above, 64)), jnp.where(low_half, zero, above))
        for q in range(2):
            canon[q, 0, here, tile(0)] = canon[q, 0, here, tile(0)] + low[q]
            canon[q, 9, here, tile(2)] = canon[q, 9, here, tile(2)] + top[q]
        return carry

    def put(a, b_row, value, t, first):
        start = ((a * 10 + b_row) * 10 + 1) * 3 + t
        out_ref[pl.ds(start, 8, stride=3), :] = value[first : first + 8, tile(t)]

    def put_column(a, k_row, value, t, first):
        start = ((a * 10 + 1) * 10 + k_row) * 3 + t
        out_ref[pl.ds(start, 8, stride=30), :] = value[first : first + 8, tile(t)]

    def put_edges(a, value, first):
        for t in range(TILES):
            put_column(a, 0, value, t, first)
            put(a, 0, value, t, first + 8)
            put_column(a, 9, value, t, first + 16)
            put(a, 9, value, t, first + 24)
            for number, (b, k) in enumerate(((0, 0), (0, 9), (9, 0), (9, 9))):
                start = ((a * 10 + b) * 10 + k) * 3 + t
                out_ref[pl.ds(start, 1), :] = value[first + 32 + number : first + 33 + number, tile(t)]

    def inner_done(a, carry):
        @pl.when(is_inner(a))
        def _():
            inner_copy(a, slice(0, 64)).wait_recv()
            for t in range(TILES):
                value = got[a, 0:64, tile(t)] + raw[c, a, 0:64, tile(t)]
                for b in range(8):
                    start = ((a * 10 + b + 1) * 10 + 1) * 3 + t
                    out_ref[pl.ds(start, 8, stride=3), :] = value[b * 8 : b * 8 + 8]

        return carry

    for q in range(2):
        both = jnp.concatenate([raw[q, 0, 0:64], raw[q, 9, 0:64]], axis=0)
        both = permuted(both, perm[q])
        canon[q, 0, 0:64] = both[0:64]
        canon[q, 9, 0:64] = both[64:128]
    steps(0, 8, 8, x_pack)
    x_send(0)

    def send_late(a, carry):
        send_inner(a, (0, 1))
        return carry

    lax.fori_loop(near + 3 - c, near + HALF, send_late, 0)
    lax.fori_loop(0, NODES // 2, z_pass, 0)
    def edge_copy(group, source, target):
        return pltpu.make_async_remote_copy(
            src_ref=source, dst_ref=target, send_sem=send_sem.at[group + 1], recv_sem=edge_sem.at[group],
            device_id=(elem, o, r), device_id_type=MESH,
        )

    z_rows = edge_copy(0, canon.at[o, 1:9, 64:72], got.at[1:9, 64:72])
    y_rows = edge_copy(0, canon.at[o, 1:9, 72:80], got.at[1:9, 72:80])
    most_tops = edge_copy(0, tops.at[1:9], tops_in.at[1:9])
    x_inner = edge_copy(1, canon.at[o, 0, 0:64], got.at[0, 0:64])
    x_edges = edge_copy(1, canon.at[o, 0, 64:80], got.at[0, 64:80])
    x_tops = edge_copy(1, tops.at[0], tops_in.at[0])
    x_ends = edge_copy(1, ends, ends_in)
    whole_groups = (
        edge_copy(0, canon.at[o, 1:9, 0:64, 0:LANES], got.at[1:9, 0:64, 0:LANES]),
        edge_copy(1, canon.at[o, 9], got.at[9]),
    )

    z_copy.wait_recv()
    r0, r1 = on(r == 0), on(r == 1)

    def z_unpack(a, carry):
        tops_here = [zr[0, a, 0:8], roll_rows(zr[0, a, 8:16], -1)]
        lows_here = [zr[1, a, 0:8], roll_rows(zr[1, a, 8:16], 1)]
        for t in range(TILES):
            for kind in range(2):
                top_rows = slice(80, 88) if kind == 0 else slice(96, 104)
                low_rows = slice(64, 72) if kind == 0 else slice(96, 104)
                top_mask = zi == 7 if kind == 0 else jnp.logical_and(c_hi, zi == 7)
                low_mask = zi == 0 if kind == 0 else jnp.logical_and(c_lo, zi == 0)
                from_above = [roll_lanes(lows_here[kind], 7 - (3 * q + t)) for q in range(2)]
                from_below = [roll_lanes(tops_here[kind], 3 * q + t - 7) for q in range(2)]
                adds = (
                    (0, top_rows, top_mask, from_above[0] * r0 + from_above[1] * r1),
                    (1, top_rows, top_mask, from_above[1] * r0),
                    (0, low_rows, low_mask, from_below[0] * r1),
                    (1, low_rows, low_mask, from_below[0] * r0 + from_below[1] * r1),
                )
                for q, rows, mask, value in adds:
                    canon[q, a, rows, tile(t)] = canon[q, a, rows, tile(t)] + jnp.where(mask, value, zero)
        return carry

    steps(0, NODES, NODES, z_unpack)

    z_rows.start()

    for a in range(NODES):
        ys[0, a * 8 : a * 8 + 8] = pack_top(six(a, slice(88, 96)), yi, 8)
        ys[1, a * 8 : a * 8 + 8] = pack_low(six(a, slice(72, 80)), yi, 8)
    for group in range(3):
        top_total, low_total = zero, zero
        for k, a in enumerate(range(4 * group, min(4 * group + 4, NODES))):
            corner = six(a, slice(96, 104))
            mine = row // 2 == k
            top_total = jnp.where(mine, roll_rows(pack_top(corner, yi, 8), 2 * k - 2), top_total)
            low_total = jnp.where(mine, roll_rows(pack_low(corner, yi, 8), 2 * k), low_total)
        ys[0, 80 + group * 8 : 88 + group * 8] = top_total
        ys[1, 80 + group * 8 : 88 + group * 8] = low_total
    y_copies = [
        pltpu.make_async_remote_copy(
            src_ref=ys.at[way], dst_ref=yr.at[way], send_sem=y_sem.at[0, way], recv_sem=y_sem.at[1, way],
            device_id=(y_links[way][0], c, r), device_id_type=MESH,
        )
        for way in range(2)
    ]
    for way in range(2):
        @pl.when(y_links[way][1])
        def _(copy=y_copies[way]):
            copy.start()


    lax.fori_loop(0, NODES // 2, y_pass, 0)
    steps(0, 8, 8, x_pass)
    lax.fori_loop(near, near + 2, inner_done, 0)
    for way in range(2):
        @pl.when(y_links[1 - way][1])
        def _(copy=y_copies[way]):
            copy.wait_recv()


    def y_unpack(a, carry):
        group, k = 80 + a // 4 * 8, a % 4
        below = [yr[0, a * 8 : a * 8 + 8], roll_rows(yr[0, group : group + 8], -2 * k)]
        above = [yr[1, a * 8 : a * 8 + 8], roll_rows(yr[1, group : group + 8], 2 - 2 * k)]
        for q in range(2):
            for t in range(TILES):
                u = 3 * q + t
                for kind in range(2):
                    top_rows = slice(88, 96) if kind == 0 else slice(96, 104)
                    low_rows = slice(72, 80) if kind == 0 else slice(96, 104)
                    top_mask = yi == 7 if kind == 0 else jnp.logical_and(b_hi, yi == 7)
                    low_mask = yi == 0 if kind == 0 else jnp.logical_and(b_lo, yi == 0)
                    up = jnp.where(top_mask, roll_lanes(above[kind], 8 * (7 - u)), zero)
                    down = jnp.where(low_mask, roll_lanes(below[kind], 8 * (u - 7)), zero)
                    canon[q, a, top_rows, tile(t)] = canon[q, a, top_rows, tile(t)] + up
                    canon[q, a, low_rows, tile(t)] = canon[q, a, low_rows, tile(t)] + down
        return carry

    steps(0, NODES, NODES, y_unpack)

    def fill_tops(a, carry):
        z_top = pack_top([canon[o, a, 80:88, tile(t)] for t in range(TILES)], zi, 1)
        y_top = pack_top([canon[o, a, 88:96, tile(t)] for t in range(TILES)], yi, 8)
        tops[a, 0:8] = jnp.where(yi > 4, y_top, jnp.where(zi > 4, z_top, roll_lanes(z_top, -27)))
        corner = [canon[o, a, 96:104, tile(t)] for t in range(TILES)]
        packed = jnp.where(row < 2, pack_top(corner, zi, 1), pack_top(corner, yi, 8))
        for t in range(TILES):
            packed = jnp.where(row == 4 + t, roll_rows(corner[t], 4 + t), packed)
        tops[a, 8:16] = packed
        return carry

    steps(8, 5, 5, x_pack)
    x_send(1)
    y_rows.start()
    steps(1, NODES - 2, NODES - 2, fill_tops)
    steps(8, 5, 5, x_pass)
    most_tops.start()
    x_wait(0)
    steps(0, 8, 8, x_unpack)
    x_inner.start()
    lax.fori_loop(near + 2, near + 5, inner_done, 0)
    x_wait(1)
    steps(8, 5, 5, x_unpack)
    x_edges.start()
    fill_tops(0, 0)
    blocks = [canon[o, 9, k * 8 : k * 8 + 8, tile(2)] for k in range(ROWS // 8)] + [zero]
    for k in range(7):
        ends[k * 8 : k * 8 + 8] = jnp.where(low_half, roll_lanes(blocks[k], 64), blocks[k + 7])
    x_tops.start()
    x_ends.start()
    lax.fori_loop(far, far + HALF, inner_done, 0)

    def complete(a, carry):
        for t in range(TILES):
            top = tops_in[a, 0:8]
            lo = got[a, 64:72, tile(t)]
            z_top = jnp.where(yi < 5, roll_lanes(top, t), roll_lanes(top, 27 + t))
            got[a, 80:88, tile(t)] = jnp.where(zi < 7, roll_lanes(lo, -1), z_top)
            lo = got[a, 72:80, tile(t)]
            got[a, 88:96, tile(t)] = jnp.where(yi < 7, roll_lanes(lo, -8), roll_lanes(top, 8 * t))
            top = tops_in[a, 8:16]
            full = roll_rows(top, -4 - t)
            after = jnp.where(zi < 7, roll_rows(roll_lanes(full, -1), 1), roll_lanes(top, t))
            full = jnp.where(row == 0, full, after)
            after = jnp.where(yi < 7, roll_rows(roll_lanes(full, -8), 2), roll_lanes(top, 8 * t))
            got[a, 96:104, tile(t)] = jnp.where(row < 2, full, jnp.where(row < 4, after, zero))
        return carry

    whole_groups[0].wait_recv()
    steps(1, NODES - 2, NODES - 2, complete)

    def pair_done(pair, carry):
        start = 1 + pair * 4
        total = canon[c, pl.ds(start, 4), 64:104] + got[pl.ds(start, 4), 64:104]
        value = permuted(total.reshape(160, ELEMS), back[...])
        for k in range(4):
            put_edges(start + k, value, k * 40)
        return carry

    lax.fori_loop(0, 2, pair_done, 0)

    whole_groups[1].wait_recv()
    complete(0, 0)

    for k in range(ROWS // 8):
        here = slice(k * 8, k * 8 + 8)
        end = ends_in[(k % 7) * 8 : (k % 7) * 8 + 8]
        lo = [roll_lanes(got[0, here, tile(t)], 64) for t in range(TILES)]
        lo.append(roll_lanes(end, 64) if k < 7 else end)
        for t in range(TILES):
            got[9, here, tile(t)] = jnp.where(low_half, lo[t], lo[t + 1])

    for a in (0, 9):
        total = canon[c, a] + got[a]
        value = permuted(total, back[...])
        for t in range(TILES):
            for b in range(8):
                put(a, b + 1, value, t, b * 8)
        put_edges(a, value, 64)

    z_copy.wait_send()
    for way in range(2):
        @pl.when(y_links[way][1])
        def _(copy=y_copies[way]):
            copy.wait_send()

        @pl.when(x_links[way][1])
        def _(way=way):
            for part in range(2):
                x_copy(part, way).wait_send()

    for group in whole_groups:
        group.wait_send()
    pltpu.make_async_remote_copy(
        src_ref=raw.at[o, 1:9, 0:64], dst_ref=got.at[1:9, 0:64], send_sem=send_sem.at[0], recv_sem=inner_sem.at[0],
        device_id=(elem, o, r), device_id_type=MESH,
    ).wait_send()


def body(velocity, geometry, element_place):
    vmem = pltpu.VMEM
    dma = pltpu.SemaphoreType.DMA
    f32 = jnp.float32
    out = pl.pallas_call(
        kernel,
        out_shape=pltpu.VMEM((NODES * NODES * NODES * TILES, LANES), f32),
        in_specs=[
            pl.BlockSpec(memory_space=pl.ANY),
            pl.BlockSpec(memory_space=pl.ANY),
            pl.BlockSpec(memory_space=pltpu.VMEM),
        ],
        out_specs=pl.BlockSpec(memory_space=pltpu.VMEM),
        scratch_shapes=[
            vmem((3, HALF, NODES, NODES, 2, ELEMS), f32),
            vmem((3, 3, HALF, NODES, NODES, 2, ELEMS), f32),
            pltpu.SMEM((2 * HALF * HALF,), f32),
            vmem((HALF, NODES, NODES, 2, ELEMS), f32),
            vmem((HALF, NODES, NODES, 2, ELEMS), f32),
            vmem((NODES, NODES, 2, ELEMS), f32),
            vmem((2, 2 * ELEMS, ELEMS), jnp.bfloat16),
            vmem((2 * ELEMS, ELEMS), jnp.bfloat16),
            vmem((1, ELEMS), jnp.int32),
            vmem((2, NODES, ROWS, ELEMS), f32),
            vmem((2, NODES, ROWS, ELEMS), f32),
            vmem((NODES, ROWS, ELEMS), f32),
            vmem((2, NODES, 16, LANES), f32),
            vmem((2, NODES, 16, LANES), f32),
            vmem((2, ROWS, LANES), f32),
            vmem((2, ROWS, LANES), f32),
            vmem((2, ROWS, LANES), f32),
            vmem((2, ROWS, LANES), f32),
            vmem((NODES - 1, 16, LANES), f32),
            vmem((NODES - 1, 16, LANES), f32),
            vmem((56, LANES), f32),
            vmem((56, LANES), f32),
            dma((2, HALF)), dma((HALF,)), dma((2,)), dma((2,)), dma((2, 2)), dma((2, 2, 2)),
            dma((3,)), dma((8,)), dma((2,)),
        ],
        compiler_params=pltpu.CompilerParams(
            collective_id=0, has_side_effects=True, vmem_limit_bytes=60 * 1024 * 1024
        ),
    )(velocity, geometry, element_place)
    return out.reshape(NODES, NODES, NODES, 1, ELEMS)


def solution(mesh):
    placed = (
        P(None, "comp", None, None, None, ("elem", "rep")),
        P(None, None, "comp", None, None, None, ("elem", "rep")),
        P("comp", ("elem", "rep")),
    )
    return jax.shard_map(
        body,
        mesh=mesh,
        in_specs=placed,
        out_specs=P(None, None, None, "comp", ("elem", "rep")),
        check_vma=False,
    )
```

```python
import jax
import jax.numpy as jnp
import numpy as np
from jax import lax
from jax.experimental import pallas as pl
from jax.experimental.pallas import tpu as pltpu
from jax.sharding import PartitionSpec as P

BLOCK_X = 6
BLOCK_Y = 8
BLOCK_Z = 8
GRID_Y = 4
RING_Y = 4
NODES = 10
HALF = 5
ELEMS = 384
LANES = 128
TILES = 3
ROWS = 104
MESH = pl.DeviceIdType.MESH


def legendre_columns(points, degree):
    columns = [points * 0.0 + 1.0, points]
    for order in range(2, degree + 1):
        columns.append(
            ((2 * order - 1) * points * columns[order - 1] - (order - 1) * columns[order - 2])
            / order
        )
    return columns


def derivative_table(node_count):
    degree = node_count - 1
    points = np.cos(np.pi * np.arange(node_count) / degree)
    for sweep in range(100):
        columns = legendre_columns(points, degree)
        points = points - (points * columns[degree] - columns[degree - 1]) / (
            node_count * columns[degree]
        )
    points = np.sort(points)
    values = legendre_columns(points, degree)[degree]
    identity = np.eye(node_count)
    spacing = points[:, None] - points[None, :] + identity
    matrix = values[:, None] / (values[None, :] * spacing)
    matrix = np.where(identity > 0.5, 0.0, matrix)
    matrix[0, 0] = -degree * (degree + 1) / 4.0
    matrix[degree, degree] = degree * (degree + 1) / 4.0
    return matrix


TABLE = derivative_table(NODES)
EVEN = [[float(0.5 * (TABLE[i, m] + TABLE[i, 9 - m])) for m in range(HALF)] for i in range(HALF)]
ODD = [[float(0.5 * (TABLE[i, m] - TABLE[i, 9 - m])) for m in range(HALF)] for i in range(HALF)]


def weighted(terms, weights):
    total = terms[0] * weights[0]
    for term, weight in zip(terms[1:], weights[1:]):
        total = total + term * weight
    return total


def along(values):
    minus = [values[i] - values[9 - i] for i in range(HALF)]
    plus = [values[i] + values[9 - i] for i in range(HALF)]
    out = [None] * NODES
    for m in range(HALF):
        even = weighted(minus, [EVEN[i][m] for i in range(HALF)])
        odd = weighted(plus, [ODD[i][m] for i in range(HALF)])
        out[m] = even + odd
        out[9 - m] = even - odd
    return out


def tile(t):
    return slice(t * LANES, (t + 1) * LANES)


def roll_lanes(x, shift):
    return pltpu.roll(x, shift % LANES, 1)


def roll_rows(x, shift):
    return pltpu.roll(x, shift % 8, 0)


def two_parts(x):
    high = x.astype(jnp.bfloat16)
    low = (x - high.astype(jnp.float32)).astype(jnp.bfloat16)
    return jnp.concatenate([high, low], axis=1)


def steps(start, count, per, fn):
    if per == count:
        for k in range(count):
            fn(start + k, 0)
        return

    def several(step, carry):
        for k in range(per):
            fn(start + step * per + k, 0)
        return carry

    lax.fori_loop(0, count // per, several, 0)


def kernel(
    v_hbm, g_hbm, place_ref, out_ref,
    v, g, coef, f0, fl, fn, perm, back, place_in, raw, canon, got,
    zs, zr, ys, yr, xs, xr, tops, tops_in, ends, ends_in,
    first_sem, later_sem, place_sem, z_sem, y_sem, x_sem, send_sem, inner_sem, edge_sem,
):
    elem = lax.axis_index("elem")
    c = lax.axis_index("comp")
    r = lax.axis_index("rep")
    o = 1 - c
    elem_count = lax.axis_size("elem")
    grid_x = elem_count // GRID_Y
    sx = elem // GRID_Y
    sy = elem % GRID_Y
    y_links = (((elem + 1, c, r), sy < GRID_Y - 1), ((elem - 1, c, r), sy > 0))
    up_comp = jnp.where(sx % RING_Y == RING_Y - 1, o, c)
    down_comp = jnp.where(sx % RING_Y == 0, o, c)
    x_links = (((elem + GRID_Y, up_comp, r), sx < grid_x - 1), ((elem - GRID_Y, down_comp, r), sx > 0))

    def first_copies(i, half):
        here = slice(half * HALF, half * HALF + HALF)
        return (
            pltpu.make_async_copy(v_hbm.at[:, i, here], v.at[:, i, here], first_sem.at[half, i]),
            pltpu.make_async_copy(g_hbm.at[:, 0, i, here], g.at[:, 0, i, here], first_sem.at[half, i]),
        )

    def first_arrived(i, half):
        here = slice(half * HALF, half * HALF + HALF)
        pltpu.make_async_copy(g_hbm.at[:, 0:2, i, here], g.at[:, 0:2, i, here], first_sem.at[half, i]).wait()

    def later_copy(i):
        return pltpu.make_async_copy(g_hbm.at[:, 1:3, i], g.at[:, 1:3, i], later_sem.at[i])

    for i in range(HALF):
        for copy in first_copies(i, 0):
            copy.start()

    barrier = pltpu.get_barrier_semaphore()
    expected = 2
    for other in ((elem, o, r), (elem, c, 1 - r)):
        pl.semaphore_signal(barrier, inc=1, device_id=other, device_id_type=MESH)
    for neighbour, exists in y_links + x_links:
        expected = expected + exists.astype(jnp.int32)

        @pl.when(exists)
        def _(neighbour=neighbour):
            pl.semaphore_signal(barrier, inc=1, device_id=neighbour, device_id_type=MESH)

    for links, target in ((y_links, yr), (x_links, xr)):
        for way in range(2):
            @pl.when(jnp.logical_not(links[1 - way][1]))
            def _(target=target, way=way):
                target[way] = jnp.zeros(target.shape[1:], jnp.float32)

    for kind in range(2):
        for m in range(HALF):
            for i in range(HALF):
                first = float(TABLE[i, (5 + m) if kind == 0 else m])
                second = float(TABLE[5 + i, m if kind == 0 else (5 + m)])
                coef[(kind * HALF + m) * HALF + i] = jnp.where(c == 0, first, second).astype(jnp.float32)

    rows_iota = lax.broadcasted_iota(jnp.int32, (ELEMS, ELEMS), 0)
    lanes_iota = lax.broadcasted_iota(jnp.int32, (LANES, ELEMS), 1).astype(jnp.float32)

    def fill_perm(q, places):
        for t in range(TILES):
            place = jnp.broadcast_to(places[:, tile(t)].astype(jnp.float32), (LANES, LANES)).T
            place = jnp.concatenate([place] * TILES, axis=1)
            part = jnp.where(lanes_iota == place, 1.0, 0.0).astype(jnp.bfloat16)
            for copy in range(2):
                perm[q, copy * ELEMS + t * LANES : copy * ELEMS + (t + 1) * LANES, :] = part

    back_half = jnp.where(rows_iota == place_ref[...], 1.0, 0.0).astype(jnp.bfloat16)
    back[0:ELEMS, :] = back_half
    back[ELEMS : 2 * ELEMS, :] = back_half
    fill_perm(c, place_ref[...])
    raw[:, :, 96:104] = jnp.zeros((2, NODES, 8, ELEMS), jnp.float32)

    far = HALF * o
    near = HALF * c

    def inner_copy(a, rows):
        return pltpu.make_async_remote_copy(
            src_ref=raw.at[o, a, rows], dst_ref=got.at[a, rows], send_sem=send_sem.at[0], recv_sem=inner_sem.at[a - 1],
            device_id=(elem, o, r), device_id_type=MESH,
        )

    def is_inner(a):
        return jnp.logical_and(a > 0, a < NODES - 1)

    def send_inner(a, halves):
        @pl.when(is_inner(a))
        def _():
            for half in halves:
                inner_copy(a, slice(half * 32, half * 32 + 32)).start()

    def first_flux(half):
        def at_plane(i, carry):
            first_arrived(i, half)
            for copy in first_copies(i, 1) if half == 0 else (later_copy(i),):
                copy.start()

            def at_b(b, carry):
                for k in range(NODES):
                    f0[i, b, k] = (
                        g[0, 0, i, b, k] * v[0, i, b, k]
                        + g[1, 0, i, b, k] * v[1, i, b, k]
                        + g[2, 0, i, b, k] * v[2, i, b, k]
                    )

            for b in range(half * HALF, half * HALF + HALF):
                at_b(b, 0)
            return carry

        return at_plane

    def mix_planes(m, half):
        weights = [coef[m * HALF + i] for i in range(HALF)]
        for b in range(half * HALF, half * HALF + HALF):
            for k in range(NODES):
                fl[m, b, k] = weighted([f0[i, b, k] for i in range(HALF)], weights)

    def gather_inner(m, a, half):
        for q in range(2):
            for t in range(TILES):
                for b in range(half * 4, half * 4 + 4):
                    raw[q, a, b * 8 : b * 8 + 8, tile(t)] = fl[m, b + 1, 1:9, q, tile(t)]

    def gather_edges(m, a):
        for q in range(2):
            for t in range(TILES):
                raw[q, a, 64:72, tile(t)] = fl[m, 1:9, 0, q, tile(t)]
                raw[q, a, 72:80, tile(t)] = fl[m, 0, 1:9, q, tile(t)]
                raw[q, a, 80:88, tile(t)] = fl[m, 1:9, 9, q, tile(t)]
                raw[q, a, 88:96, tile(t)] = fl[m, 9, 1:9, q, tile(t)]
            raw[q, a, 96:97, :] = fl[m, 0, 0, q : q + 1, :]
            raw[q, a, 97:98, :] = fl[m, 0, 9, q : q + 1, :]
            raw[q, a, 98:99, :] = fl[m, 9, 0, q : q + 1, :]
            raw[q, a, 99:100, :] = fl[m, 9, 9, q : q + 1, :]

    def permuted(x, matrix):
        return jnp.dot(two_parts(x), matrix, preferred_element_type=jnp.float32)

    def to_canon(a, between=None):
        parts = [two_parts(raw[q, a, 64:104]) for q in range(2)]
        if between is not None:
            between()
        for q in range(2):
            canon[q, a, 64:104] = jnp.dot(parts[q], perm[q], preferred_element_type=jnp.float32)

    def far_first(m, carry):
        mix_planes(m, 0)
        gather_inner(m, far + m, 0)
        send_inner(far + m, (0,))
        return carry

    def far_second(m, carry):
        mix_planes(m, 1)
        gather_inner(m, far + m, 1)
        send_inner(far + m, (1,))
        gather_edges(m, far + m)
        return carry

    lax.fori_loop(0, HALF, first_flux(0), 0)
    pl.semaphore_wait(barrier, expected)
    place_copy = pltpu.make_async_remote_copy(
        src_ref=place_ref, dst_ref=place_in, send_sem=place_sem.at[0], recv_sem=place_sem.at[1],
        device_id=(elem, o, r), device_id_type=MESH,
    )
    place_copy.start()
    lax.fori_loop(0, HALF, far_first, 0)
    lax.fori_loop(0, HALF, first_flux(1), 0)
    lax.fori_loop(0, HALF, far_second, 0)

    def near_plane(m):
        later_copy(m).wait()

        def flux(j, b, k):
            return (
                g[0, j, m, b, k] * v[0, m, b, k]
                + g[1, j, m, b, k] * v[1, m, b, k]
                + g[2, j, m, b, k] * v[2, m, b, k]
            )

        def at_b(b, carry):
            base = (HALF + m) * HALF
            weights = [coef[base + i] for i in range(HALF)]
            out = along([flux(2, b, k) for k in range(NODES)])
            for k in range(NODES):
                fn[b, k] = out[k] + weighted([f0[i, b, k] for i in range(HALF)], weights)
            return carry

        steps(0, NODES, 2, at_b)

        def at_k(k, carry):
            out = along([flux(1, b, k) for b in range(NODES)])
            for b in range(NODES):
                fl[m, b, k] = fn[b, k] + out[b]
            return carry

        steps(0, NODES, 2, at_k)

    def near_gather(m):
        gather_inner(m, near + m, 0)
        gather_inner(m, near + m, 1)
        gather_edges(m, near + m)

    def near_step(m, carry):
        near_plane(m)
        to_canon(far + m - c, lambda: near_gather(m))
        send_inner(near + m, (0, 1))
        return carry

    near_plane(0)
    near_gather(0)
    send_inner(near, (0, 1))
    place_copy.wait()
    fill_perm(o, place_in[...])
    lax.fori_loop(1, HALF, near_step, 0)
    six_planes = pl.ds(near - c, HALF + 1)
    for q in range(2):
        canon[q, six_planes, 64:104] = permuted(
            raw[q, six_planes, 64:104].reshape((HALF + 1) * 40, ELEMS), perm[q]
        ).reshape(HALF + 1, 40, ELEMS)

    lane = lax.broadcasted_iota(jnp.int32, (8, LANES), 1)
    row = lax.broadcasted_iota(jnp.int32, (8, LANES), 0)
    zi = lane % 8
    yi = (lane // 8) % 8
    low_half = lane < 64
    zero = jnp.zeros((8, LANES), jnp.float32)
    c_lo = jnp.logical_or(row == 0, row == 2)
    c_hi = jnp.logical_or(row == 1, row == 3)
    b_lo = row < 2
    b_hi = jnp.logical_or(row == 2, row == 3)

    def line_pass(lo_row, index, shift, corner_lo, corner_hi, corner_step):
        def two_planes(planes):
            spots = [(q, a, tile(t)) for a in planes for q in range(2) for t in range(TILES)]
            corners = [canon[q, a, 96:104, lanes] for q, a, lanes in spots]
            lows = [canon[q, a, lo_row : lo_row + 8, lanes] for q, a, lanes in spots]
            highs = [canon[q, a, lo_row + 16 : lo_row + 24, lanes] for q, a, lanes in spots]
            for (q, a, lanes), k, lo, hi in zip(spots, corners, lows, highs):
                canon[q, a, lo_row : lo_row + 8, lanes] = lo + jnp.where(index > 0, roll_lanes(hi, shift), zero)
                canon[q, a, lo_row + 16 : lo_row + 24, lanes] = hi + jnp.where(
                    index < 7, roll_lanes(lo, -shift), zero
                )
                canon[q, a, 96:104, lanes] = (
                    k
                    + jnp.where(
                        jnp.logical_and(corner_lo, index > 0), roll_lanes(roll_rows(k, -corner_step), shift), zero
                    )
                    + jnp.where(
                        jnp.logical_and(corner_hi, index < 7), roll_lanes(roll_rows(k, corner_step), -shift), zero
                    )
                )

        return two_planes

    def over_middle(pass_over):
        def at_step(step, carry):
            pass_over([1 + 2 * step, 2 + 2 * step])
            return carry

        lax.fori_loop(0, 4, at_step, 0)

    z_pass = line_pass(64, zi, 1, c_lo, c_hi, 1)
    y_pass = line_pass(72, yi, 8, b_lo, b_hi, 2)

    def x_pass(block, carry):
        here = pl.ds(block * 8, 8)
        for q in range(2):
            lo = [canon[q, 0, here, tile(t)] for t in range(TILES)]
            hi = [canon[q, 9, here, tile(t)] for t in range(TILES)]
            lo_rolled = [roll_lanes(x, 64) for x in lo] + [zero]
            hi_rolled = [roll_lanes(x, 64) for x in hi] + [zero]
            for t in range(TILES):
                canon[q, 0, here, tile(t)] = lo[t] + jnp.where(low_half, hi_rolled[t - 1], hi_rolled[t])
                canon[q, 9, here, tile(t)] = hi[t] + jnp.where(low_half, lo_rolled[t], lo_rolled[t + 1])
        return carry

    def pack_top(parts, index, step):
        total = parts[0]
        for u in range(1, len(parts)):
            total = jnp.where(index == 7 - u, roll_lanes(parts[u], -step * u), total)
        return total

    def pack_low(parts, index, step):
        total = parts[0]
        for u in range(1, len(parts)):
            total = jnp.where(index == u, roll_lanes(parts[u], step * u), total)
        return total

    def six(a, rows):
        return [canon[q, a, rows, tile(t)] for q in range(2) for t in range(TILES)]

    def on(flag):
        return jnp.where(flag, 1.0, 0.0).astype(jnp.float32)

    middle, ends_planes = tuple(range(1, 9)), (0, 9)
    slots = {a: (a - 1 if 0 < a < 9 else 8 + a // 9) for a in range(NODES)}

    def z_pack(planes):
        for a in planes:
            corner = six(a, slice(96, 104))
            zs[0, slots[a], 0:8] = pack_top(six(a, slice(80, 88)), zi, 1)
            zs[0, slots[a], 8:16] = pack_top(corner, zi, 1)
            zs[1, slots[a], 0:8] = pack_low(six(a, slice(64, 72)), zi, 1)
            zs[1, slots[a], 8:16] = pack_low(corner, zi, 1)

    def z_copy(part):
        here = slice(0, 8) if part == 0 else slice(8, 10)
        return pltpu.make_async_remote_copy(
            src_ref=zs.at[:, here], dst_ref=zr.at[:, here], send_sem=z_sem.at[0, part], recv_sem=z_sem.at[1, part],
            device_id=(elem, c, 1 - r), device_id_type=MESH,
        )

    r0, r1 = on(r == 0), on(r == 1)

    def x_pack(block, carry):
        here = pl.ds(block * 8, 8)
        xs[0, here] = jnp.where(low_half, roll_lanes(canon[0, 9, here, tile(2)], 64), canon[1, 9, here, tile(2)])
        xs[1, here] = jnp.where(low_half, canon[0, 0, here, tile(0)], roll_lanes(canon[1, 0, here, tile(0)], 64))
        return carry

    def x_copy(way):
        return pltpu.make_async_remote_copy(
            src_ref=xs.at[way], dst_ref=xr.at[way], send_sem=x_sem.at[0, way], recv_sem=x_sem.at[1, way],
            device_id=x_links[way][0], device_id_type=MESH,
        )

    def y_copy(part, way):
        here = slice(0, 80) if part == 0 else slice(80, 104)
        return pltpu.make_async_remote_copy(
            src_ref=ys.at[way, here], dst_ref=yr.at[way, here],
            send_sem=y_sem.at[0, part, way], recv_sem=y_sem.at[1, part, way],
            device_id=y_links[way][0], device_id_type=MESH,
        )

    def send_both(links, copies):
        for way in range(2):
            @pl.when(links[way][1])
            def _(copy=copies[way]):
                copy.start()

    def wait_both(links, copies):
        for way in range(2):
            @pl.when(links[1 - way][1])
            def _(copy=copies[way]):
                copy.wait_recv()

    def x_unpack(block, carry):
        here = pl.ds(block * 8, 8)
        below = xr[0, here]
        above = xr[1, here]
        low = (jnp.where(low_half, below, zero), jnp.where(low_half, roll_lanes(below, 64), zero))
        top = (jnp.where(low_half, zero, roll_lanes(above, 64)), jnp.where(low_half, zero, above))
        for q in range(2):
            canon[q, 0, here, tile(0)] = canon[q, 0, here, tile(0)] + low[q]
            canon[q, 9, here, tile(2)] = canon[q, 9, here, tile(2)] + top[q]
        return carry

    def put(a, b_row, value, t, first):
        start = ((a * 10 + b_row) * 10 + 1) * 3 + t
        out_ref[pl.ds(start, 8, stride=3), :] = value[first : first + 8, tile(t)]

    def put_column(a, k_row, value, t, first):
        start = ((a * 10 + 1) * 10 + k_row) * 3 + t
        out_ref[pl.ds(start, 8, stride=30), :] = value[first : first + 8, tile(t)]

    def put_edges(a, value, first):
        for t in range(TILES):
            put_column(a, 0, value, t, first)
            put(a, 0, value, t, first + 8)
            put_column(a, 9, value, t, first + 16)
            put(a, 9, value, t, first + 24)
            for number, (b, k) in enumerate(((0, 0), (0, 9), (9, 0), (9, 9))):
                start = ((a * 10 + b) * 10 + k) * 3 + t
                out_ref[pl.ds(start, 1), :] = value[first + 32 + number : first + 33 + number, tile(t)]

    def inner_done(a, carry):
        @pl.when(is_inner(a))
        def _():
            inner_copy(a, slice(0, 64)).wait_recv()
            for t in range(TILES):
                value = got[a, 0:64, tile(t)] + raw[c, a, 0:64, tile(t)]
                for b in range(8):
                    start = ((a * 10 + b + 1) * 10 + 1) * 3 + t
                    out_ref[pl.ds(start, 8, stride=3), :] = value[b * 8 : b * 8 + 8]

        return carry

    for q in range(2):
        both = jnp.concatenate([raw[q, 0, 0:64], raw[q, 9, 0:64]], axis=0)
        both = permuted(both, perm[q])
        canon[q, 0, 0:64] = both[0:64]
        canon[q, 9, 0:64] = both[64:128]
    steps(0, ROWS // 8, 13, x_pack)
    send_both(x_links, [x_copy(way) for way in range(2)])

    z_pack(middle)
    z_copy(0).start()
    over_middle(z_pass)
    steps(0, ROWS // 8, 13, x_pass)

    def edge_copy(group, source, target):
        return pltpu.make_async_remote_copy(
            src_ref=source, dst_ref=target, send_sem=send_sem.at[group + 1], recv_sem=edge_sem.at[group],
            device_id=(elem, o, r), device_id_type=MESH,
        )

    z_rows = edge_copy(0, canon.at[o, 1:9, 64:72], got.at[1:9, 64:72])
    y_rows = edge_copy(0, canon.at[o, 1:9, 72:80], got.at[1:9, 72:80])
    most_tops = edge_copy(0, tops.at[1:9], tops_in.at[1:9])
    x_inner = edge_copy(1, canon.at[o, 0, 0:64], got.at[0, 0:64])
    x_edges = edge_copy(1, canon.at[o, 0, 64:80], got.at[0, 64:80])
    x_tops = edge_copy(1, tops.at[0], tops_in.at[0])
    x_ends = edge_copy(1, ends, ends_in)
    whole_groups = (
        edge_copy(0, canon.at[o, 1:9, 0:64, 0:LANES], got.at[1:9, 0:64, 0:LANES]),
        edge_copy(1, canon.at[o, 9], got.at[9]),
    )

    def z_unpack(a, carry):
        slot = slots[a]
        tops_here = [zr[0, slot, 0:8], roll_rows(zr[0, slot, 8:16], -1)]
        lows_here = [zr[1, slot, 0:8], roll_rows(zr[1, slot, 8:16], 1)]
        for t in range(TILES):
            for kind in range(2):
                top_rows = slice(80, 88) if kind == 0 else slice(96, 104)
                low_rows = slice(64, 72) if kind == 0 else slice(96, 104)
                top_mask = zi == 7 if kind == 0 else jnp.logical_and(c_hi, zi == 7)
                low_mask = zi == 0 if kind == 0 else jnp.logical_and(c_lo, zi == 0)
                from_above = [roll_lanes(lows_here[kind], 7 - (3 * q + t)) for q in range(2)]
                from_below = [roll_lanes(tops_here[kind], 3 * q + t - 7) for q in range(2)]
                adds = (
                    (0, top_rows, top_mask, from_above[0] * r0 + from_above[1] * r1),
                    (1, top_rows, top_mask, from_above[1] * r0),
                    (0, low_rows, low_mask, from_below[0] * r1),
                    (1, low_rows, low_mask, from_below[0] * r0 + from_below[1] * r1),
                )
                for q, rows, mask, value in adds:
                    canon[q, a, rows, tile(t)] = canon[q, a, rows, tile(t)] + jnp.where(mask, value, zero)
        return carry

    def y_pack(planes, first):
        for k, a in enumerate(planes):
            here = slice(first + k * 8, first + k * 8 + 8)
            ys[0, here] = pack_top(six(a, slice(88, 96)), yi, 8)
            ys[1, here] = pack_low(six(a, slice(72, 80)), yi, 8)
        for group in range(0, len(planes), 4):
            top_total, low_total = zero, zero
            for k, a in enumerate(planes[group : group + 4]):
                corner = six(a, slice(96, 104))
                mine = row // 2 == k
                top_total = jnp.where(mine, roll_rows(pack_top(corner, yi, 8), 2 * k - 2), top_total)
                low_total = jnp.where(mine, roll_rows(pack_low(corner, yi, 8), 2 * k), low_total)
            here = slice(first + len(planes) * 8 + group * 2, first + len(planes) * 8 + group * 2 + 8)
            ys[0, here] = top_total
            ys[1, here] = low_total

    def y_unpack(a, carry):
        place, first, count = (a - 1, 0, 8) if 0 < a < 9 else (a // 9, 80, 2)
        here = slice(first + place * 8, first + place * 8 + 8)
        group, k = first + count * 8 + place // 4 * 8, place % 4
        below = [yr[0, here], roll_rows(yr[0, group : group + 8], -2 * k)]
        above = [yr[1, here], roll_rows(yr[1, group : group + 8], 2 - 2 * k)]
        for q in range(2):
            for t in range(TILES):
                u = 3 * q + t
                for kind in range(2):
                    top_rows = slice(88, 96) if kind == 0 else slice(96, 104)
                    low_rows = slice(72, 80) if kind == 0 else slice(96, 104)
                    top_mask = yi == 7 if kind == 0 else jnp.logical_and(b_hi, yi == 7)
                    low_mask = yi == 0 if kind == 0 else jnp.logical_and(b_lo, yi == 0)
                    up = jnp.where(top_mask, roll_lanes(above[kind], 8 * (7 - u)), zero)
                    down = jnp.where(low_mask, roll_lanes(below[kind], 8 * (u - 7)), zero)
                    canon[q, a, top_rows, tile(t)] = canon[q, a, top_rows, tile(t)] + up
                    canon[q, a, low_rows, tile(t)] = canon[q, a, low_rows, tile(t)] + down
        return carry


    def fill_tops(a, carry):
        z_top = pack_top([canon[o, a, 80:88, tile(t)] for t in range(TILES)], zi, 1)
        y_top = pack_top([canon[o, a, 88:96, tile(t)] for t in range(TILES)], yi, 8)
        tops[a, 0:8] = jnp.where(yi > 4, y_top, jnp.where(zi > 4, z_top, roll_lanes(z_top, -27)))
        corner = [canon[o, a, 96:104, tile(t)] for t in range(TILES)]
        packed = jnp.where(row < 2, pack_top(corner, zi, 1), pack_top(corner, yi, 8))
        for t in range(TILES):
            packed = jnp.where(row == 4 + t, roll_rows(corner[t], 4 + t), packed)
        tops[a, 8:16] = packed
        return carry

    z_copy(0).wait_recv()
    for a in middle:
        z_unpack(a, 0)
    z_rows.start()
    y_pack(middle, 0)
    send_both(y_links, [y_copy(0, way) for way in range(2)])
    over_middle(y_pass)
    lax.fori_loop(near, near + 2, inner_done, 0)
    wait_both(y_links, [y_copy(0, way) for way in range(2)])
    for a in middle:
        y_unpack(a, 0)
    y_rows.start()
    steps(1, NODES - 2, NODES - 2, fill_tops)
    most_tops.start()

    wait_both(x_links, [x_copy(way) for way in range(2)])
    steps(0, ROWS // 8, 13, x_unpack)
    x_inner.start()
    z_pack(ends_planes)
    z_copy(1).start()
    z_pass(ends_planes)
    lax.fori_loop(near + 2, near + 4, inner_done, 0)
    z_copy(1).wait_recv()
    for a in ends_planes:
        z_unpack(a, 0)
    y_pack(ends_planes, 80)
    send_both(y_links, [y_copy(1, way) for way in range(2)])
    y_pass(ends_planes)
    lax.fori_loop(near + 4, near + HALF, inner_done, 0)
    wait_both(y_links, [y_copy(1, way) for way in range(2)])
    for a in ends_planes:
        y_unpack(a, 0)
    x_edges.start()
    fill_tops(0, 0)
    blocks = [canon[o, 9, k * 8 : k * 8 + 8, tile(2)] for k in range(ROWS // 8)] + [zero]
    for k in range(7):
        ends[k * 8 : k * 8 + 8] = jnp.where(low_half, roll_lanes(blocks[k], 64), blocks[k + 7])
    x_tops.start()
    x_ends.start()
    lax.fori_loop(far, far + HALF, inner_done, 0)

    def complete(a, carry):
        for t in range(TILES):
            top = tops_in[a, 0:8]
            lo = got[a, 64:72, tile(t)]
            z_top = jnp.where(yi < 5, roll_lanes(top, t), roll_lanes(top, 27 + t))
            got[a, 80:88, tile(t)] = jnp.where(zi < 7, roll_lanes(lo, -1), z_top)
            lo = got[a, 72:80, tile(t)]
            got[a, 88:96, tile(t)] = jnp.where(yi < 7, roll_lanes(lo, -8), roll_lanes(top, 8 * t))
            top = tops_in[a, 8:16]
            full = roll_rows(top, -4 - t)
            after = jnp.where(zi < 7, roll_rows(roll_lanes(full, -1), 1), roll_lanes(top, t))
            full = jnp.where(row == 0, full, after)
            after = jnp.where(yi < 7, roll_rows(roll_lanes(full, -8), 2), roll_lanes(top, 8 * t))
            got[a, 96:104, tile(t)] = jnp.where(row < 2, full, jnp.where(row < 4, after, zero))
        return carry

    whole_groups[0].wait_recv()
    steps(1, NODES - 2, NODES - 2, complete)

    def pair_done(pair, carry):
        start = 1 + pair * 4
        total = canon[c, pl.ds(start, 4), 64:104] + got[pl.ds(start, 4), 64:104]
        value = permuted(total.reshape(160, ELEMS), back[...])
        for k in range(4):
            put_edges(start + k, value, k * 40)
        return carry

    lax.fori_loop(0, 2, pair_done, 0)

    whole_groups[1].wait_recv()
    complete(0, 0)

    for k in range(ROWS // 8):
        here = slice(k * 8, k * 8 + 8)
        end = ends_in[(k % 7) * 8 : (k % 7) * 8 + 8]
        lo = [roll_lanes(got[0, here, tile(t)], 64) for t in range(TILES)]
        lo.append(roll_lanes(end, 64) if k < 7 else end)
        for t in range(TILES):
            got[9, here, tile(t)] = jnp.where(low_half, lo[t], lo[t + 1])

    for a in (0, 9):
        total = canon[c, a] + got[a]
        value = permuted(total, back[...])
        for t in range(TILES):
            for b in range(8):
                put(a, b + 1, value, t, b * 8)
        put_edges(a, value, 64)

    for part in range(2):
        z_copy(part).wait_send()
    for way in range(2):
        @pl.when(y_links[way][1])
        def _(way=way):
            for part in range(2):
                y_copy(part, way).wait_send()

        @pl.when(x_links[way][1])
        def _(way=way):
            x_copy(way).wait_send()

    for group in whole_groups:
        group.wait_send()
    pltpu.make_async_remote_copy(
        src_ref=raw.at[o, 1:9, 0:64], dst_ref=got.at[1:9, 0:64], send_sem=send_sem.at[0], recv_sem=inner_sem.at[0],
        device_id=(elem, o, r), device_id_type=MESH,
    ).wait_send()


def body(velocity, geometry, element_place):
    vmem = pltpu.VMEM
    dma = pltpu.SemaphoreType.DMA
    f32 = jnp.float32
    out = pl.pallas_call(
        kernel,
        out_shape=pltpu.VMEM((NODES * NODES * NODES * TILES, LANES), f32),
        in_specs=[
            pl.BlockSpec(memory_space=pl.ANY),
            pl.BlockSpec(memory_space=pl.ANY),
            pl.BlockSpec(memory_space=pltpu.VMEM),
        ],
        out_specs=pl.BlockSpec(memory_space=pltpu.VMEM),
        scratch_shapes=[
            vmem((3, HALF, NODES, NODES, 2, ELEMS), f32),
            vmem((3, 3, HALF, NODES, NODES, 2, ELEMS), f32),
            pltpu.SMEM((2 * HALF * HALF,), f32),
            vmem((HALF, NODES, NODES, 2, ELEMS), f32),
            vmem((HALF, NODES, NODES, 2, ELEMS), f32),
            vmem((NODES, NODES, 2, ELEMS), f32),
            vmem((2, 2 * ELEMS, ELEMS), jnp.bfloat16),
            vmem((2 * ELEMS, ELEMS), jnp.bfloat16),
            vmem((1, ELEMS), jnp.int32),
            vmem((2, NODES, ROWS, ELEMS), f32),
            vmem((2, NODES, ROWS, ELEMS), f32),
            vmem((NODES, ROWS, ELEMS), f32),
            vmem((2, NODES, 16, LANES), f32),
            vmem((2, NODES, 16, LANES), f32),
            vmem((2, ROWS, LANES), f32),
            vmem((2, ROWS, LANES), f32),
            vmem((2, ROWS, LANES), f32),
            vmem((2, ROWS, LANES), f32),
            vmem((NODES - 1, 16, LANES), f32),
            vmem((NODES - 1, 16, LANES), f32),
            vmem((56, LANES), f32),
            vmem((56, LANES), f32),
            dma((2, HALF)), dma((HALF,)), dma((2,)), dma((2, 2)), dma((2, 2, 2)), dma((2, 2)),
            dma((3,)), dma((8,)), dma((2,)),
        ],
        compiler_params=pltpu.CompilerParams(
            collective_id=0, has_side_effects=True, vmem_limit_bytes=60 * 1024 * 1024
        ),
    )(velocity, geometry, element_place)
    return out.reshape(NODES, NODES, NODES, 1, ELEMS)


def solution(mesh):
    placed = (
        P(None, "comp", None, None, None, ("elem", "rep")),
        P(None, None, "comp", None, None, None, ("elem", "rep")),
        P("comp", ("elem", "rep")),
    )
    return jax.shard_map(
        body,
        mesh=mesh,
        in_specs=placed,
        out_specs=P(None, None, None, "comp", ("elem", "rep")),
        check_vma=False,
    )
```

```python
import jax
import jax.numpy as jnp
import numpy as np
from jax import lax
from jax.experimental import pallas as pl
from jax.experimental.pallas import tpu as pltpu
from jax.sharding import PartitionSpec as P

BLOCK_X = 6
BLOCK_Y = 8
BLOCK_Z = 8
GRID_Y = 4
RING_Y = 4
PART_ROWS = ((1, 2, 3), (4, 5, 6, 7, 8, 9, 0))
PART_INNER = (slice(0, 24), slice(24, 64))
NODES = 10
HALF = 5
ELEMS = 384
LANES = 128
TILES = 3
ROWS = 104
MESH = pl.DeviceIdType.MESH


def legendre_columns(points, degree):
    columns = [points * 0.0 + 1.0, points]
    for order in range(2, degree + 1):
        columns.append(
            ((2 * order - 1) * points * columns[order - 1] - (order - 1) * columns[order - 2])
            / order
        )
    return columns


def derivative_table(node_count):
    degree = node_count - 1
    points = np.cos(np.pi * np.arange(node_count) / degree)
    for sweep in range(100):
        columns = legendre_columns(points, degree)
        points = points - (points * columns[degree] - columns[degree - 1]) / (
            node_count * columns[degree]
        )
    points = np.sort(points)
    values = legendre_columns(points, degree)[degree]
    identity = np.eye(node_count)
    spacing = points[:, None] - points[None, :] + identity
    matrix = values[:, None] / (values[None, :] * spacing)
    matrix = np.where(identity > 0.5, 0.0, matrix)
    matrix[0, 0] = -degree * (degree + 1) / 4.0
    matrix[degree, degree] = degree * (degree + 1) / 4.0
    return matrix


TABLE = derivative_table(NODES)
EVEN = [[float(0.5 * (TABLE[i, m] + TABLE[i, 9 - m])) for m in range(HALF)] for i in range(HALF)]
ODD = [[float(0.5 * (TABLE[i, m] - TABLE[i, 9 - m])) for m in range(HALF)] for i in range(HALF)]


def weighted(terms, weights):
    total = terms[0] * weights[0]
    for term, weight in zip(terms[1:], weights[1:]):
        total = total + term * weight
    return total


def along(values):
    minus = [values[i] - values[9 - i] for i in range(HALF)]
    plus = [values[i] + values[9 - i] for i in range(HALF)]
    out = [None] * NODES
    for m in range(HALF):
        even = weighted(minus, [EVEN[i][m] for i in range(HALF)])
        odd = weighted(plus, [ODD[i][m] for i in range(HALF)])
        out[m] = even + odd
        out[9 - m] = even - odd
    return out


def tile(t):
    return slice(t * LANES, (t + 1) * LANES)


def roll_lanes(x, shift):
    return pltpu.roll(x, shift % LANES, 1)


def roll_rows(x, shift):
    return pltpu.roll(x, shift % 8, 0)


def two_parts(x):
    high = x.astype(jnp.bfloat16)
    low = (x - high.astype(jnp.float32)).astype(jnp.bfloat16)
    return jnp.concatenate([high, low], axis=1)


def steps(start, count, per, fn):
    if per == count:
        for k in range(count):
            fn(start + k, 0)
        return

    def several(step, carry):
        for k in range(per):
            fn(start + step * per + k, 0)
        return carry

    lax.fori_loop(0, count // per, several, 0)


def kernel(
    v_hbm, g_hbm, place_hbm, out_ref,
    v, g, coef, f0, fl, fn, perm, back, place_own, place_in, raw, canon, got,
    zs, zr, ys, yr, xs, xr, tops, tops_in, ends, ends_in,
    first_sem, later_sem, place_sem, z_sem, y_sem, x_sem, send_sem, inner_sem, edge_sem,
):
    elem = lax.axis_index("elem")
    c = lax.axis_index("comp")
    r = lax.axis_index("rep")
    o = 1 - c
    elem_count = lax.axis_size("elem")
    grid_x = elem_count // GRID_Y
    sx = elem // GRID_Y
    sy = elem % GRID_Y
    y_links = (((elem + 1, c, r), sy < GRID_Y - 1), ((elem - 1, c, r), sy > 0))
    up_comp = jnp.where(sx % RING_Y == RING_Y - 1, o, c)
    down_comp = jnp.where(sx % RING_Y == 0, o, c)
    x_links = (((elem + GRID_Y, up_comp, r), sx < grid_x - 1), ((elem - GRID_Y, down_comp, r), sx > 0))

    barrier = pltpu.get_barrier_semaphore()
    expected = 2
    for other in ((elem, o, r), (elem, c, 1 - r)):
        pl.semaphore_signal(barrier, inc=1, device_id=other, device_id_type=MESH)
    for neighbour, exists in y_links + x_links:
        expected = expected + exists.astype(jnp.int32)

        @pl.when(exists)
        def _(neighbour=neighbour):
            pl.semaphore_signal(barrier, inc=1, device_id=neighbour, device_id_type=MESH)

    own_copy = pltpu.make_async_copy(place_hbm, place_own, place_sem.at[2])
    own_copy.start()

    def first_copies(i, part):
        copies = []
        for here in (slice(1, 4),) if part == 0 else (slice(4, 10), slice(0, 1)):
            copies.append(pltpu.make_async_copy(v_hbm.at[:, i, here], v.at[:, i, here], first_sem.at[part, i]))
            copies.append(
                pltpu.make_async_copy(g_hbm.at[:, 0, i, here], g.at[:, 0, i, here], first_sem.at[part, i])
            )
        return copies

    def first_arrived(i, part):
        here = slice(0, len(PART_ROWS[part]))
        pltpu.make_async_copy(g_hbm.at[:, 0:2, i, here], g.at[:, 0:2, i, here], first_sem.at[part, i]).wait()

    def later_copy(i):
        return pltpu.make_async_copy(g_hbm.at[:, 1:3, i], g.at[:, 1:3, i], later_sem.at[i])

    for i in range(HALF):
        for copy in first_copies(i, 0):
            copy.start()

    for links, target in ((y_links, yr), (x_links, xr)):
        for way in range(2):
            @pl.when(jnp.logical_not(links[1 - way][1]))
            def _(target=target, way=way):
                target[way] = jnp.zeros(target.shape[1:], jnp.float32)

    for kind in range(2):
        for m in range(HALF):
            for i in range(HALF):
                first = float(TABLE[i, (5 + m) if kind == 0 else m])
                second = float(TABLE[5 + i, m if kind == 0 else (5 + m)])
                coef[(kind * HALF + m) * HALF + i] = jnp.where(c == 0, first, second).astype(jnp.float32)


    own_copy.wait()
    rows_iota = lax.broadcasted_iota(jnp.int32, (ELEMS, ELEMS), 0)
    lanes_iota = lax.broadcasted_iota(jnp.int32, (LANES, ELEMS), 1).astype(jnp.float32)

    def fill_perm(q, places):
        for t in range(TILES):
            place = jnp.broadcast_to(places[:, tile(t)].astype(jnp.float32), (LANES, LANES)).T
            place = jnp.concatenate([place] * TILES, axis=1)
            part = jnp.where(lanes_iota == place, 1.0, 0.0).astype(jnp.bfloat16)
            for copy in range(2):
                perm[q, copy * ELEMS + t * LANES : copy * ELEMS + (t + 1) * LANES, :] = part

    back_half = jnp.where(rows_iota == place_own[...], 1.0, 0.0).astype(jnp.bfloat16)
    back[0:ELEMS, :] = back_half
    back[ELEMS : 2 * ELEMS, :] = back_half
    fill_perm(c, place_own[...])
    raw[:, :, 96:104] = jnp.zeros((2, NODES, 8, ELEMS), jnp.float32)

    far = HALF * o
    near = HALF * c

    def inner_copy(a, rows, group):
        return pltpu.make_async_remote_copy(
            src_ref=raw.at[o, a, rows], dst_ref=got.at[a, rows], send_sem=send_sem.at[0], recv_sem=inner_sem.at[group],
            device_id=(elem, o, r), device_id_type=MESH,
        )

    def is_inner(a):
        return jnp.logical_and(a > 0, a < NODES - 1)

    def send_inner(a, halves, group):
        @pl.when(is_inner(a))
        def _():
            for half in halves:
                inner_copy(a, PART_INNER[half], group).start()

    def first_flux(half):
        def at_plane(i, carry):
            first_arrived(i, half)
            for copy in first_copies(i, 1) if half == 0 else (later_copy(i),):
                copy.start()

            def at_b(b, carry):
                for k in range(NODES):
                    f0[i, b, k] = (
                        g[0, 0, i, b, k] * v[0, i, b, k]
                        + g[1, 0, i, b, k] * v[1, i, b, k]
                        + g[2, 0, i, b, k] * v[2, i, b, k]
                    )

            for b in PART_ROWS[half]:
                at_b(b, 0)
            return carry

        return at_plane

    def mix_planes(m, half):
        weights = [coef[m * HALF + i] for i in range(HALF)]
        for b in PART_ROWS[half]:
            for k in range(NODES):
                fl[m, b, k] = weighted([f0[i, b, k] for i in range(HALF)], weights)

    def gather_inner(m, a, half):
        for q in range(2):
            for t in range(TILES):
                for b in range(PART_INNER[half].start // 8, PART_INNER[half].stop // 8):
                    raw[q, a, b * 8 : b * 8 + 8, tile(t)] = fl[m, b + 1, 1:9, q, tile(t)]

    def gather_edges(m, a):
        for q in range(2):
            for t in range(TILES):
                raw[q, a, 64:72, tile(t)] = fl[m, 1:9, 0, q, tile(t)]
                raw[q, a, 72:80, tile(t)] = fl[m, 0, 1:9, q, tile(t)]
                raw[q, a, 80:88, tile(t)] = fl[m, 1:9, 9, q, tile(t)]
                raw[q, a, 88:96, tile(t)] = fl[m, 9, 1:9, q, tile(t)]
            raw[q, a, 96:97, :] = fl[m, 0, 0, q : q + 1, :]
            raw[q, a, 97:98, :] = fl[m, 0, 9, q : q + 1, :]
            raw[q, a, 98:99, :] = fl[m, 9, 0, q : q + 1, :]
            raw[q, a, 99:100, :] = fl[m, 9, 9, q : q + 1, :]

    def permuted(x, matrix):
        return jnp.dot(two_parts(x), matrix, preferred_element_type=jnp.float32)

    def to_canon(a, between=None):
        parts = [two_parts(raw[q, a, 64:104]) for q in range(2)]
        if between is not None:
            between()
        for q in range(2):
            canon[q, a, 64:104] = jnp.dot(parts[q], perm[q], preferred_element_type=jnp.float32)

    def far_first(step, carry):
        m = (step + c) % HALF
        mix_planes(m, 0)
        gather_inner(m, far + m, 0)
        send_inner(far + m, (0,), 0)
        return carry

    def far_second(step, carry):
        m = (step + c) % HALF
        mix_planes(m, 1)
        gather_inner(m, far + m, 1)
        send_inner(far + m, (1,), 0)
        gather_edges(m, far + m)
        return carry

    lax.fori_loop(0, HALF, first_flux(0), 0)
    pl.semaphore_wait(barrier, expected)
    place_copy = pltpu.make_async_remote_copy(
        src_ref=place_own, dst_ref=place_in, send_sem=place_sem.at[0], recv_sem=place_sem.at[1],
        device_id=(elem, o, r), device_id_type=MESH,
    )
    place_copy.start()
    lax.fori_loop(0, HALF, far_first, 0)
    lax.fori_loop(0, HALF, first_flux(1), 0)
    lax.fori_loop(0, HALF, far_second, 0)

    def near_plane(m):
        later_copy(m).wait()

        def flux(j, b, k):
            return (
                g[0, j, m, b, k] * v[0, m, b, k]
                + g[1, j, m, b, k] * v[1, m, b, k]
                + g[2, j, m, b, k] * v[2, m, b, k]
            )

        def at_b(b, carry):
            base = (HALF + m) * HALF
            weights = [coef[base + i] for i in range(HALF)]
            out = along([flux(2, b, k) for k in range(NODES)])
            for k in range(NODES):
                fn[b, k] = out[k] + weighted([f0[i, b, k] for i in range(HALF)], weights)
            return carry

        steps(0, NODES, 2, at_b)

        def at_k(k, carry):
            out = along([flux(1, b, k) for b in range(NODES)])
            for b in range(NODES):
                fl[m, b, k] = fn[b, k] + out[b]
            return carry

        steps(0, NODES, 2, at_k)

    def near_gather(m):
        gather_inner(m, near + m, 0)
        gather_inner(m, near + m, 1)
        gather_edges(m, near + m)

    def near_step(m, carry):
        near_plane(m)
        to_canon(far + m - c, lambda: near_gather(m))
        send_inner(near + m, (0, 1), 1)
        return carry

    near_plane(0)
    near_gather(0)
    send_inner(near, (0, 1), 1)
    place_copy.wait()
    fill_perm(o, place_in[...])
    lax.fori_loop(1, HALF, near_step, 0)
    six_planes = pl.ds(near - c, HALF + 1)
    for q in range(2):
        canon[q, six_planes, 64:104] = permuted(
            raw[q, six_planes, 64:104].reshape((HALF + 1) * 40, ELEMS), perm[q]
        ).reshape(HALF + 1, 40, ELEMS)

    lane = lax.broadcasted_iota(jnp.int32, (8, LANES), 1)
    row = lax.broadcasted_iota(jnp.int32, (8, LANES), 0)
    zi = lane % 8
    yi = (lane // 8) % 8
    low_half = lane < 64
    zero = jnp.zeros((8, LANES), jnp.float32)
    c_lo = jnp.logical_or(row == 0, row == 2)
    c_hi = jnp.logical_or(row == 1, row == 3)
    b_lo = row < 2
    b_hi = jnp.logical_or(row == 2, row == 3)

    def line_pass(lo_row, index, shift, corner_lo, corner_hi, corner_step):
        def two_planes(planes):
            spots = [(q, a, tile(t)) for a in planes for q in range(2) for t in range(TILES)]
            corners = [canon[q, a, 96:104, lanes] for q, a, lanes in spots]
            lows = [canon[q, a, lo_row : lo_row + 8, lanes] for q, a, lanes in spots]
            highs = [canon[q, a, lo_row + 16 : lo_row + 24, lanes] for q, a, lanes in spots]
            for (q, a, lanes), k, lo, hi in zip(spots, corners, lows, highs):
                canon[q, a, lo_row : lo_row + 8, lanes] = lo + jnp.where(index > 0, roll_lanes(hi, shift), zero)
                canon[q, a, lo_row + 16 : lo_row + 24, lanes] = hi + jnp.where(
                    index < 7, roll_lanes(lo, -shift), zero
                )
                canon[q, a, 96:104, lanes] = (
                    k
                    + jnp.where(
                        jnp.logical_and(corner_lo, index > 0), roll_lanes(roll_rows(k, -corner_step), shift), zero
                    )
                    + jnp.where(
                        jnp.logical_and(corner_hi, index < 7), roll_lanes(roll_rows(k, corner_step), -shift), zero
                    )
                )

        return two_planes

    def over_middle(pass_over):
        def at_step(step, carry):
            pass_over([1 + 2 * step, 2 + 2 * step])
            return carry

        lax.fori_loop(0, 4, at_step, 0)

    z_pass = line_pass(64, zi, 1, c_lo, c_hi, 1)
    y_pass = line_pass(72, yi, 8, b_lo, b_hi, 2)

    def x_pass(block, carry):
        here = pl.ds(block * 8, 8)
        for q in range(2):
            lo = [canon[q, 0, here, tile(t)] for t in range(TILES)]
            hi = [canon[q, 9, here, tile(t)] for t in range(TILES)]
            lo_rolled = [roll_lanes(x, 64) for x in lo] + [zero]
            hi_rolled = [roll_lanes(x, 64) for x in hi] + [zero]
            for t in range(TILES):
                canon[q, 0, here, tile(t)] = lo[t] + jnp.where(low_half, hi_rolled[t - 1], hi_rolled[t])
                canon[q, 9, here, tile(t)] = hi[t] + jnp.where(low_half, lo_rolled[t], lo_rolled[t + 1])
        return carry

    def pack_top(parts, index, step):
        total = parts[0]
        for u in range(1, len(parts)):
            total = jnp.where(index == 7 - u, roll_lanes(parts[u], -step * u), total)
        return total

    def pack_low(parts, index, step):
        total = parts[0]
        for u in range(1, len(parts)):
            total = jnp.where(index == u, roll_lanes(parts[u], step * u), total)
        return total

    def six(a, rows):
        return [canon[q, a, rows, tile(t)] for q in range(2) for t in range(TILES)]

    def on(flag):
        return jnp.where(flag, 1.0, 0.0).astype(jnp.float32)

    middle, ends_planes = tuple(range(1, 9)), (0, 9)
    slots = {a: (a - 1 if 0 < a < 9 else 8 + a // 9) for a in range(NODES)}

    def z_pack(planes):
        for a in planes:
            corner = six(a, slice(96, 104))
            zs[0, slots[a], 0:8] = pack_top(six(a, slice(80, 88)), zi, 1)
            zs[0, slots[a], 8:16] = pack_top(corner, zi, 1)
            zs[1, slots[a], 0:8] = pack_low(six(a, slice(64, 72)), zi, 1)
            zs[1, slots[a], 8:16] = pack_low(corner, zi, 1)

    def z_copy(part):
        here = (slice(0, 8), slice(8, 10), slice(0, 10))[part]
        return pltpu.make_async_remote_copy(
            src_ref=zs.at[:, here], dst_ref=zr.at[:, here], send_sem=z_sem.at[2], recv_sem=z_sem.at[part % 2],
            device_id=(elem, c, 1 - r), device_id_type=MESH,
        )

    r0, r1 = on(r == 0), on(r == 1)

    def x_pack(block, carry):
        here = pl.ds(block * 8, 8)
        xs[0, here] = jnp.where(low_half, roll_lanes(canon[0, 9, here, tile(2)], 64), canon[1, 9, here, tile(2)])
        xs[1, here] = jnp.where(low_half, canon[0, 0, here, tile(0)], roll_lanes(canon[1, 0, here, tile(0)], 64))
        return carry

    def x_copy(way):
        return pltpu.make_async_remote_copy(
            src_ref=xs.at[way], dst_ref=xr.at[way], send_sem=x_sem.at[0, way], recv_sem=x_sem.at[1, way],
            device_id=x_links[way][0], device_id_type=MESH,
        )

    def y_copy(part, way):
        here = (slice(0, 80), slice(80, ROWS), slice(0, ROWS))[part]
        return pltpu.make_async_remote_copy(
            src_ref=ys.at[way, here], dst_ref=yr.at[way, here],
            send_sem=y_sem.at[2, way], recv_sem=y_sem.at[part % 2, way],
            device_id=y_links[way][0], device_id_type=MESH,
        )

    def send_both(links, copies):
        for way in range(2):
            @pl.when(links[way][1])
            def _(copy=copies[way]):
                copy.start()

    def wait_both(links, copies):
        for way in range(2):
            @pl.when(links[1 - way][1])
            def _(copy=copies[way]):
                copy.wait_recv()

    def x_unpack(block, carry):
        here = pl.ds(block * 8, 8)
        below = xr[0, here]
        above = xr[1, here]
        low = (jnp.where(low_half, below, zero), jnp.where(low_half, roll_lanes(below, 64), zero))
        top = (jnp.where(low_half, zero, roll_lanes(above, 64)), jnp.where(low_half, zero, above))
        for q in range(2):
            canon[q, 0, here, tile(0)] = canon[q, 0, here, tile(0)] + low[q]
            canon[q, 9, here, tile(2)] = canon[q, 9, here, tile(2)] + top[q]
        return carry

    def put(a, b_row, value, t, first):
        start = ((a * 10 + b_row) * 10 + 1) * 3 + t
        out_ref[pl.ds(start, 8, stride=3), :] = value[first : first + 8, tile(t)]

    def put_column(a, k_row, value, t, first):
        start = ((a * 10 + 1) * 10 + k_row) * 3 + t
        out_ref[pl.ds(start, 8, stride=30), :] = value[first : first + 8, tile(t)]

    def put_edges(a, value, first):
        for t in range(TILES):
            put_column(a, 0, value, t, first)
            put(a, 0, value, t, first + 8)
            put_column(a, 9, value, t, first + 16)
            put(a, 9, value, t, first + 24)
            for number, (b, k) in enumerate(((0, 0), (0, 9), (9, 0), (9, 9))):
                start = ((a * 10 + b) * 10 + k) * 3 + t
                out_ref[pl.ds(start, 1), :] = value[first + 32 + number : first + 33 + number, tile(t)]

    def inner_wait(group):
        inner_copy(slice(1, 5), slice(0, 64), group).wait_recv()

    def inner_done(a, carry):
        @pl.when(is_inner(a))
        def _():
            for t in range(TILES):
                value = got[a, 0:64, tile(t)] + raw[c, a, 0:64, tile(t)]
                for b in range(8):
                    start = ((a * 10 + b + 1) * 10 + 1) * 3 + t
                    out_ref[pl.ds(start, 8, stride=3), :] = value[b * 8 : b * 8 + 8]

        return carry

    for q in range(2):
        both = jnp.concatenate([raw[q, 0, 0:64], raw[q, 9, 0:64]], axis=0)
        both = permuted(both, perm[q])
        canon[q, 0, 0:64] = both[0:64]
        canon[q, 9, 0:64] = both[64:128]
    steps(0, ROWS // 8, 13, x_pack)
    send_both(x_links, [x_copy(way) for way in range(2)])

    z_pack(middle)
    z_copy(0).start()
    over_middle(z_pass)
    steps(0, ROWS // 8, 13, x_pass)

    def edge_copy(group, source, target):
        return pltpu.make_async_remote_copy(
            src_ref=source, dst_ref=target, send_sem=send_sem.at[group + 1], recv_sem=edge_sem.at[group],
            device_id=(elem, o, r), device_id_type=MESH,
        )

    z_rows = edge_copy(0, canon.at[o, 1:9, 64:72], got.at[1:9, 64:72])
    y_rows = edge_copy(0, canon.at[o, 1:9, 72:80], got.at[1:9, 72:80])
    most_tops = edge_copy(0, tops.at[1:9], tops_in.at[1:9])
    x_inner = edge_copy(2, canon.at[o, 0, 0:64], got.at[0, 0:64])
    x_edges = edge_copy(1, canon.at[o, 0, 64:80], got.at[0, 64:80])
    x_tops = edge_copy(1, tops.at[0], tops_in.at[0])
    x_ends_inner = edge_copy(2, ends.at[0:32], ends_in.at[0:32])
    x_ends = edge_copy(1, ends.at[32:56], ends_in.at[32:56])
    whole_groups = (
        edge_copy(0, canon.at[o, 1:9, 0:64, 0:LANES], got.at[1:9, 0:64, 0:LANES]),
        edge_copy(1, canon.at[o, 0, 0:88, 0:LANES], got.at[0, 0:88, 0:LANES]),
        edge_copy(2, canon.at[o, 1:5, 0:56, 0:LANES], got.at[1:5, 0:56, 0:LANES]),
    )

    def z_unpack(a, carry):
        slot = slots[a]
        tops_here = [zr[0, slot, 0:8], roll_rows(zr[0, slot, 8:16], -1)]
        lows_here = [zr[1, slot, 0:8], roll_rows(zr[1, slot, 8:16], 1)]
        for t in range(TILES):
            for kind in range(2):
                top_rows = slice(80, 88) if kind == 0 else slice(96, 104)
                low_rows = slice(64, 72) if kind == 0 else slice(96, 104)
                top_mask = zi == 7 if kind == 0 else jnp.logical_and(c_hi, zi == 7)
                low_mask = zi == 0 if kind == 0 else jnp.logical_and(c_lo, zi == 0)
                from_above = [roll_lanes(lows_here[kind], 7 - (3 * q + t)) for q in range(2)]
                from_below = [roll_lanes(tops_here[kind], 3 * q + t - 7) for q in range(2)]
                adds = (
                    (0, top_rows, top_mask, from_above[0] * r0 + from_above[1] * r1),
                    (1, top_rows, top_mask, from_above[1] * r0),
                    (0, low_rows, low_mask, from_below[0] * r1),
                    (1, low_rows, low_mask, from_below[0] * r0 + from_below[1] * r1),
                )
                for q, rows, mask, value in adds:
                    canon[q, a, rows, tile(t)] = canon[q, a, rows, tile(t)] + jnp.where(mask, value, zero)
        return carry

    def y_pack(planes, first):
        for k, a in enumerate(planes):
            here = slice(first + k * 8, first + k * 8 + 8)
            ys[0, here] = pack_top(six(a, slice(88, 96)), yi, 8)
            ys[1, here] = pack_low(six(a, slice(72, 80)), yi, 8)
        for group in range(0, len(planes), 4):
            top_total, low_total = zero, zero
            for k, a in enumerate(planes[group : group + 4]):
                corner = six(a, slice(96, 104))
                mine = row // 2 == k
                top_total = jnp.where(mine, roll_rows(pack_top(corner, yi, 8), 2 * k - 2), top_total)
                low_total = jnp.where(mine, roll_rows(pack_low(corner, yi, 8), 2 * k), low_total)
            here = slice(first + len(planes) * 8 + group * 2, first + len(planes) * 8 + group * 2 + 8)
            ys[0, here] = top_total
            ys[1, here] = low_total

    def y_unpack(a, carry):
        place, first, count = (a - 1, 0, 8) if 0 < a < 9 else (a // 9, 80, 2)
        here = slice(first + place * 8, first + place * 8 + 8)
        group, k = first + count * 8 + place // 4 * 8, place % 4
        below = [yr[0, here], roll_rows(yr[0, group : group + 8], -2 * k)]
        above = [yr[1, here], roll_rows(yr[1, group : group + 8], 2 - 2 * k)]
        for q in range(2):
            for t in range(TILES):
                u = 3 * q + t
                for kind in range(2):
                    top_rows = slice(88, 96) if kind == 0 else slice(96, 104)
                    low_rows = slice(72, 80) if kind == 0 else slice(96, 104)
                    top_mask = yi == 7 if kind == 0 else jnp.logical_and(b_hi, yi == 7)
                    low_mask = yi == 0 if kind == 0 else jnp.logical_and(b_lo, yi == 0)
                    up = jnp.where(top_mask, roll_lanes(above[kind], 8 * (7 - u)), zero)
                    down = jnp.where(low_mask, roll_lanes(below[kind], 8 * (u - 7)), zero)
                    canon[q, a, top_rows, tile(t)] = canon[q, a, top_rows, tile(t)] + up
                    canon[q, a, low_rows, tile(t)] = canon[q, a, low_rows, tile(t)] + down
        return carry


    def fill_tops(a, carry):
        z_top = pack_top([canon[o, a, 80:88, tile(t)] for t in range(TILES)], zi, 1)
        y_top = pack_top([canon[o, a, 88:96, tile(t)] for t in range(TILES)], yi, 8)
        tops[a, 0:8] = jnp.where(yi > 4, y_top, jnp.where(zi > 4, z_top, roll_lanes(z_top, -27)))
        corner = [canon[o, a, 96:104, tile(t)] for t in range(TILES)]
        packed = jnp.where(row < 2, pack_top(corner, zi, 1), pack_top(corner, yi, 8))
        for t in range(TILES):
            packed = jnp.where(row == 4 + t, roll_rows(corner[t], 4 + t), packed)
        tops[a, 8:16] = packed
        return carry

    def fill_ends(block, pairs, first):
        for k in range(pairs):
            low = canon[o, 9, (block + k) * 8 : (block + k) * 8 + 8, tile(2)]
            high_block = block + k + pairs
            high = canon[o, 9, high_block * 8 : high_block * 8 + 8, tile(2)] if high_block < ROWS // 8 else zero
            ends[first + k * 8 : first + k * 8 + 8] = jnp.where(low_half, roll_lanes(low, 64), high)

    z_copy(0).wait_recv()
    for a in middle:
        z_unpack(a, 0)
    z_rows.start()
    y_pack(middle, 0)
    send_both(y_links, [y_copy(0, way) for way in range(2)])
    over_middle(y_pass)
    inner_wait(0)
    lax.fori_loop(near, near + 2, inner_done, 0)
    wait_both(y_links, [y_copy(0, way) for way in range(2)])
    for a in middle:
        y_unpack(a, 0)
    y_rows.start()
    steps(1, NODES - 2, NODES - 2, fill_tops)
    most_tops.start()

    wait_both(x_links, [x_copy(way) for way in range(2)])
    steps(0, ROWS // 8, 13, x_unpack)
    x_inner.start()
    fill_ends(0, 4, 0)
    x_ends_inner.start()
    z_pack(ends_planes)
    z_copy(1).start()
    z_pass(ends_planes)
    lax.fori_loop(near + 2, near + 4, inner_done, 0)
    z_copy(1).wait_recv()
    for a in ends_planes:
        z_unpack(a, 0)
    y_pack(ends_planes, 80)
    send_both(y_links, [y_copy(1, way) for way in range(2)])
    y_pass(ends_planes)
    lax.fori_loop(near + 4, near + HALF, inner_done, 0)
    wait_both(y_links, [y_copy(1, way) for way in range(2)])
    for a in ends_planes:
        y_unpack(a, 0)
    x_edges.start()
    fill_tops(0, 0)
    fill_ends(8, 3, 32)
    x_tops.start()
    x_ends.start()
    inner_wait(1)
    lax.fori_loop(far, far + HALF, inner_done, 0)

    def complete(a, carry):
        for t in range(TILES):
            top = tops_in[a, 0:8]
            lo = got[a, 64:72, tile(t)]
            z_top = jnp.where(yi < 5, roll_lanes(top, t), roll_lanes(top, 27 + t))
            got[a, 80:88, tile(t)] = jnp.where(zi < 7, roll_lanes(lo, -1), z_top)
            lo = got[a, 72:80, tile(t)]
            got[a, 88:96, tile(t)] = jnp.where(yi < 7, roll_lanes(lo, -8), roll_lanes(top, 8 * t))
            top = tops_in[a, 8:16]
            full = roll_rows(top, -4 - t)
            after = jnp.where(zi < 7, roll_rows(roll_lanes(full, -1), 1), roll_lanes(top, t))
            full = jnp.where(row == 0, full, after)
            after = jnp.where(yi < 7, roll_rows(roll_lanes(full, -8), 2), roll_lanes(top, 8 * t))
            got[a, 96:104, tile(t)] = jnp.where(row < 2, full, jnp.where(row < 4, after, zero))
        return carry

    whole_groups[0].wait_recv()
    steps(1, NODES - 2, NODES - 2, complete)

    def pair_done(pair, carry):
        start = 1 + pair * 4
        total = canon[c, pl.ds(start, 4), 64:104] + got[pl.ds(start, 4), 64:104]
        value = permuted(total.reshape(160, ELEMS), back[...])
        for k in range(4):
            put_edges(start + k, value, k * 40)
        return carry

    lax.fori_loop(0, 2, pair_done, 0)

    def last_plane(block, pairs, first):
        for k in range(block, min(block + 2 * pairs, ROWS // 8)):
            here = slice(k * 8, k * 8 + 8)
            start = first + (k - block) % pairs * 8
            end = ends_in[start : start + 8]
            lo = [roll_lanes(got[0, here, tile(t)], 64) for t in range(TILES)]
            lo.append(roll_lanes(end, 64) if k < block + pairs else end)
            for t in range(TILES):
                got[9, here, tile(t)] = jnp.where(low_half, lo[t], lo[t + 1])

    whole_groups[2].wait_recv()
    last_plane(0, 4, 0)
    total = jnp.concatenate([canon[c, a, 0:64] + got[a, 0:64] for a in (0, 9)], axis=0)
    value = permuted(total, back[...])
    for k, a in enumerate((0, 9)):
        for t in range(TILES):
            for b in range(8):
                put(a, b + 1, value, t, k * 64 + b * 8)

    whole_groups[1].wait_recv()
    complete(0, 0)
    last_plane(8, 3, 32)
    total = jnp.concatenate([canon[c, a, 64:104] + got[a, 64:104] for a in (0, 9)], axis=0)
    value = permuted(total, back[...])
    for k, a in enumerate((0, 9)):
        put_edges(a, value, k * 40)

    z_copy(2).wait_send()
    for way in range(2):
        @pl.when(y_links[way][1])
        def _(way=way):
            y_copy(2, way).wait_send()

        @pl.when(x_links[way][1])
        def _(way=way):
            x_copy(way).wait_send()

    for group in whole_groups:
        group.wait_send()
    inner_copy(slice(1, 9), slice(0, 64), 0).wait_send()


def body(velocity, geometry, element_place):
    vmem = pltpu.VMEM
    dma = pltpu.SemaphoreType.DMA
    f32 = jnp.float32
    out = pl.pallas_call(
        kernel,
        out_shape=pltpu.VMEM((NODES * NODES * NODES * TILES, LANES), f32),
        in_specs=[
            pl.BlockSpec(memory_space=pl.ANY),
            pl.BlockSpec(memory_space=pl.ANY),
            pl.BlockSpec(memory_space=pl.ANY),
        ],
        out_specs=pl.BlockSpec(memory_space=pltpu.VMEM),
        scratch_shapes=[
            vmem((3, HALF, NODES, NODES, 2, ELEMS), f32),
            vmem((3, 3, HALF, NODES, NODES, 2, ELEMS), f32),
            pltpu.SMEM((2 * HALF * HALF,), f32),
            vmem((HALF, NODES, NODES, 2, ELEMS), f32),
            vmem((HALF, NODES, NODES, 2, ELEMS), f32),
            vmem((NODES, NODES, 2, ELEMS), f32),
            vmem((2, 2 * ELEMS, ELEMS), jnp.bfloat16),
            vmem((2 * ELEMS, ELEMS), jnp.bfloat16),
            vmem((1, ELEMS), jnp.int32),
            vmem((1, ELEMS), jnp.int32),
            vmem((2, NODES, ROWS, ELEMS), f32),
            vmem((2, NODES, ROWS, ELEMS), f32),
            vmem((NODES, ROWS, ELEMS), f32),
            vmem((2, NODES, 16, LANES), f32),
            vmem((2, NODES, 16, LANES), f32),
            vmem((2, ROWS, LANES), f32),
            vmem((2, ROWS, LANES), f32),
            vmem((2, ROWS, LANES), f32),
            vmem((2, ROWS, LANES), f32),
            vmem((NODES - 1, 16, LANES), f32),
            vmem((NODES - 1, 16, LANES), f32),
            vmem((56, LANES), f32),
            vmem((56, LANES), f32),
            dma((2, HALF)), dma((HALF,)), dma((3,)), dma((3,)), dma((3, 2)), dma((2, 2)),
            dma((4,)), dma((2,)), dma((3,)),
        ],
        compiler_params=pltpu.CompilerParams(
            collective_id=0, has_side_effects=True, vmem_limit_bytes=60 * 1024 * 1024
        ),
    )(velocity, geometry, element_place)
    return out.reshape(NODES, NODES, NODES, 1, ELEMS)


def solution(mesh):
    placed = (
        P(None, "comp", None, None, None, ("elem", "rep")),
        P(None, None, "comp", None, None, None, ("elem", "rep")),
        P("comp", ("elem", "rep")),
    )
    return jax.shard_map(
        body,
        mesh=mesh,
        in_specs=placed,
        out_specs=P(None, None, None, "comp", ("elem", "rep")),
        check_vma=False,
    )
```

```python
import jax
import jax.numpy as jnp
import numpy as np
from jax import lax
from jax.experimental import pallas as pl
from jax.experimental.pallas import tpu as pltpu
from jax.sharding import PartitionSpec as P

BLOCK_X = 6
BLOCK_Y = 8
BLOCK_Z = 8
GRID_Y = 4
RING_Y = 4
HELD = 3
PART_ROWS = ((1, 2, 3), (4, 5, 6, 7, 8, 9, 0))
PART_INNER = (slice(0, 24), slice(24, 64))
NODES = 10
HALF = 5
ELEMS = 384
LANES = 128
TILES = 3
ROWS = 104
MESH = pl.DeviceIdType.MESH


def legendre_columns(points, degree):
    columns = [points * 0.0 + 1.0, points]
    for order in range(2, degree + 1):
        columns.append(
            ((2 * order - 1) * points * columns[order - 1] - (order - 1) * columns[order - 2])
            / order
        )
    return columns


def derivative_table(node_count):
    degree = node_count - 1
    points = np.cos(np.pi * np.arange(node_count) / degree)
    for sweep in range(100):
        columns = legendre_columns(points, degree)
        points = points - (points * columns[degree] - columns[degree - 1]) / (
            node_count * columns[degree]
        )
    points = np.sort(points)
    values = legendre_columns(points, degree)[degree]
    identity = np.eye(node_count)
    spacing = points[:, None] - points[None, :] + identity
    matrix = values[:, None] / (values[None, :] * spacing)
    matrix = np.where(identity > 0.5, 0.0, matrix)
    matrix[0, 0] = -degree * (degree + 1) / 4.0
    matrix[degree, degree] = degree * (degree + 1) / 4.0
    return matrix


TABLE = derivative_table(NODES)
EVEN = [[float(0.5 * (TABLE[i, m] + TABLE[i, 9 - m])) for m in range(HALF)] for i in range(HALF)]
ODD = [[float(0.5 * (TABLE[i, m] - TABLE[i, 9 - m])) for m in range(HALF)] for i in range(HALF)]


def weighted(terms, weights):
    total = terms[0] * weights[0]
    for term, weight in zip(terms[1:], weights[1:]):
        total = total + term * weight
    return total


def along(values):
    minus = [values[i] - values[9 - i] for i in range(HALF)]
    plus = [values[i] + values[9 - i] for i in range(HALF)]
    out = [None] * NODES
    for m in range(HALF):
        even = weighted(minus, [EVEN[i][m] for i in range(HALF)])
        odd = weighted(plus, [ODD[i][m] for i in range(HALF)])
        out[m] = even + odd
        out[9 - m] = even - odd
    return out


def tile(t):
    return slice(t * LANES, (t + 1) * LANES)


def roll_lanes(x, shift):
    return pltpu.roll(x, shift % LANES, 1)


def roll_rows(x, shift):
    return pltpu.roll(x, shift % 8, 0)


def two_parts(x):
    high = x.astype(jnp.bfloat16)
    low = (x - high.astype(jnp.float32)).astype(jnp.bfloat16)
    return jnp.concatenate([high, low], axis=1)


def steps(start, count, per, fn):
    if per == count:
        for k in range(count):
            fn(start + k, 0)
        return

    def several(step, carry):
        for k in range(per):
            fn(start + step * per + k, 0)
        return carry

    lax.fori_loop(0, count // per, several, 0)


def kernel(
    v_hbm, g_hbm, place_hbm, out_ref,
    v, g, coef, f0, fl, fn, perm, back, place_own, place_in, raw, canon, got,
    zs, zr, ys, yr, xs, xr, tops, tops_in, ends, ends_in,
    first_sem, later_sem, place_sem, z_sem, y_sem, x_sem, send_sem, inner_sem, edge_sem,
):
    elem = lax.axis_index("elem")
    c = lax.axis_index("comp")
    r = lax.axis_index("rep")
    o = 1 - c
    elem_count = lax.axis_size("elem")
    grid_x = elem_count // GRID_Y
    sx = elem // GRID_Y
    sy = elem % GRID_Y
    y_links = (((elem + 1, c, r), sy < GRID_Y - 1), ((elem - 1, c, r), sy > 0))
    up_comp = jnp.where(sx % RING_Y == RING_Y - 1, o, c)
    down_comp = jnp.where(sx % RING_Y == 0, o, c)
    x_links = (((elem + GRID_Y, up_comp, r), sx < grid_x - 1), ((elem - GRID_Y, down_comp, r), sx > 0))

    barrier = pltpu.get_barrier_semaphore()
    expected = 2
    for neighbour, exists in x_links + y_links:
        expected = expected + exists.astype(jnp.int32)

        @pl.when(exists)
        def _(neighbour=neighbour):
            pl.semaphore_signal(barrier, inc=1, device_id=neighbour, device_id_type=MESH)

    for other in ((elem, o, r), (elem, c, 1 - r)):
        pl.semaphore_signal(barrier, inc=1, device_id=other, device_id_type=MESH)

    own_copy = pltpu.make_async_copy(place_hbm, place_own, place_sem.at[2])
    own_copy.start()

    def first_copies(i, part):
        copies = []
        for here in (slice(1, 4),) if part == 0 else (slice(4, 10), slice(0, 1)):
            copies.append(pltpu.make_async_copy(v_hbm.at[:, i, here], v.at[:, i, here], first_sem.at[part, i]))
            copies.append(
                pltpu.make_async_copy(g_hbm.at[:, 0, i, here], g.at[:, 0, i, here], first_sem.at[part, i])
            )
        return copies

    def first_arrived(i, part):
        here = slice(0, len(PART_ROWS[part]))
        pltpu.make_async_copy(g_hbm.at[:, 0:2, i, here], g.at[:, 0:2, i, here], first_sem.at[part, i]).wait()

    def later_copy(i):
        return pltpu.make_async_copy(g_hbm.at[:, 1:3, i], g.at[:, 1:3, i], later_sem.at[i])

    for i in range(HALF):
        for copy in first_copies(i, 0):
            copy.start()

    for links, target in ((y_links, yr), (x_links, xr)):
        for way in range(2):
            @pl.when(jnp.logical_not(links[1 - way][1]))
            def _(target=target, way=way):
                target[way] = jnp.zeros(target.shape[1:], jnp.float32)

    for kind in range(2):
        for m in range(HALF):
            for i in range(HALF):
                first = float(TABLE[i, (5 + m) if kind == 0 else m])
                second = float(TABLE[5 + i, m if kind == 0 else (5 + m)])
                coef[(kind * HALF + m) * HALF + i] = jnp.where(c == 0, first, second).astype(jnp.float32)


    own_copy.wait()
    rows_iota = lax.broadcasted_iota(jnp.int32, (ELEMS, ELEMS), 0)
    lanes_iota = lax.broadcasted_iota(jnp.int32, (LANES, ELEMS), 1).astype(jnp.float32)

    def fill_perm(q, places):
        for t in range(TILES):
            place = jnp.broadcast_to(places[:, tile(t)].astype(jnp.float32), (LANES, LANES)).T
            place = jnp.concatenate([place] * TILES, axis=1)
            part = jnp.where(lanes_iota == place, 1.0, 0.0).astype(jnp.bfloat16)
            for copy in range(2):
                perm[q, copy * ELEMS + t * LANES : copy * ELEMS + (t + 1) * LANES, :] = part

    back_half = jnp.where(rows_iota == place_own[...], 1.0, 0.0).astype(jnp.bfloat16)
    back[0:ELEMS, :] = back_half
    back[ELEMS : 2 * ELEMS, :] = back_half
    fill_perm(c, place_own[...])
    raw[:, :, 96:104] = jnp.zeros((2, NODES, 8, ELEMS), jnp.float32)

    far = HALF * o
    near = HALF * c

    def inner_copy(a, rows, group):
        return pltpu.make_async_remote_copy(
            src_ref=raw.at[o, a, rows], dst_ref=got.at[a, rows], send_sem=send_sem.at[0], recv_sem=inner_sem.at[group],
            device_id=(elem, o, r), device_id_type=MESH,
        )

    def is_inner(a):
        return jnp.logical_and(a > 0, a < NODES - 1)

    def send_inner(a, halves, group):
        @pl.when(is_inner(a))
        def _():
            for half in halves:
                inner_copy(a, PART_INNER[half], group).start()

    def first_flux(half):
        def at_plane(i, carry):
            first_arrived(i, half)
            for copy in first_copies(i, 1) if half == 0 else (later_copy(i),):
                copy.start()

            def at_b(b, carry):
                for k in range(NODES):
                    f0[i, b, k] = (
                        g[0, 0, i, b, k] * v[0, i, b, k]
                        + g[1, 0, i, b, k] * v[1, i, b, k]
                        + g[2, 0, i, b, k] * v[2, i, b, k]
                    )

            for b in PART_ROWS[half]:
                at_b(b, 0)
            return carry

        return at_plane

    def mix_planes(m, half):
        weights = [coef[m * HALF + i] for i in range(HALF)]
        for b in PART_ROWS[half]:
            for k in range(NODES):
                fl[m, b, k] = weighted([f0[i, b, k] for i in range(HALF)], weights)

    def gather_inner(m, a, half):
        for q in range(2):
            for t in range(TILES):
                for b in range(PART_INNER[half].start // 8, PART_INNER[half].stop // 8):
                    raw[q, a, b * 8 : b * 8 + 8, tile(t)] = fl[m, b + 1, 1:9, q, tile(t)]

    def gather_edges(m, a):
        for q in range(2):
            for t in range(TILES):
                raw[q, a, 64:72, tile(t)] = fl[m, 1:9, 0, q, tile(t)]
                raw[q, a, 72:80, tile(t)] = fl[m, 0, 1:9, q, tile(t)]
                raw[q, a, 80:88, tile(t)] = fl[m, 1:9, 9, q, tile(t)]
                raw[q, a, 88:96, tile(t)] = fl[m, 9, 1:9, q, tile(t)]
            raw[q, a, 96:97, :] = fl[m, 0, 0, q : q + 1, :]
            raw[q, a, 97:98, :] = fl[m, 0, 9, q : q + 1, :]
            raw[q, a, 98:99, :] = fl[m, 9, 0, q : q + 1, :]
            raw[q, a, 99:100, :] = fl[m, 9, 9, q : q + 1, :]

    def permuted(x, matrix):
        return jnp.dot(two_parts(x), matrix, preferred_element_type=jnp.float32)

    def to_canon(a, between=None):
        parts = [two_parts(raw[q, a, 64:104]) for q in range(2)]
        if between is not None:
            between()
        for q in range(2):
            canon[q, a, 64:104] = jnp.dot(parts[q], perm[q], preferred_element_type=jnp.float32)

    def far_rows(step):
        m = (step + c) % HALF
        mix_planes(m, 0)
        gather_inner(m, far + m, 0)

    def far_first(step, carry):
        far_rows(step)
        send_inner(far + (step + c) % HALF, (0,), 0)
        return carry

    def far_second(step, carry):
        m = (step + c) % HALF
        mix_planes(m, 1)
        gather_inner(m, far + m, 1)
        send_inner(far + m, (1,), 0)
        gather_edges(m, far + m)
        return carry

    lax.fori_loop(0, HALF, first_flux(0), 0)
    far_rows(0)
    pl.semaphore_wait(barrier, expected)
    send_inner(far + c, (0,), 0)
    place_copy = pltpu.make_async_remote_copy(
        src_ref=place_own, dst_ref=place_in, send_sem=place_sem.at[0], recv_sem=place_sem.at[1],
        device_id=(elem, o, r), device_id_type=MESH,
    )
    place_copy.start()
    lax.fori_loop(1, HALF, far_first, 0)
    lax.fori_loop(0, HALF, first_flux(1), 0)
    lax.fori_loop(0, HALF, far_second, 0)

    def near_plane(m):
        later_copy(m).wait()

        def flux(j, b, k):
            return (
                g[0, j, m, b, k] * v[0, m, b, k]
                + g[1, j, m, b, k] * v[1, m, b, k]
                + g[2, j, m, b, k] * v[2, m, b, k]
            )

        def at_b(b, carry):
            base = (HALF + m) * HALF
            weights = [coef[base + i] for i in range(HALF)]
            out = along([flux(2, b, k) for k in range(NODES)])
            for k in range(NODES):
                fn[b, k] = out[k] + weighted([f0[i, b, k] for i in range(HALF)], weights)
            return carry

        steps(0, NODES, 2, at_b)

        def at_k(k, carry):
            out = along([flux(1, b, k) for b in range(NODES)])
            for b in range(NODES):
                fl[m, b, k] = fn[b, k] + out[b]
            return carry

        steps(0, NODES, 2, at_k)

    def near_gather(m):
        gather_inner(m, near + m, 0)
        gather_inner(m, near + m, 1)
        gather_edges(m, near + m)

    def near_step(m, carry):
        near_plane(m)
        to_canon(far + m - c, lambda: near_gather(m))

        @pl.when(m != HELD)
        def _():
            send_inner(near + m, (0, 1), 1)

        @pl.when(m == HELD)
        def _():
            send_inner(near + m, (1,), 2)

        return carry

    near_plane(0)
    near_gather(0)
    send_inner(near, (0, 1), 1)
    place_copy.wait()
    fill_perm(o, place_in[...])
    lax.fori_loop(1, HALF, near_step, 0)
    six_planes = pl.ds(near - c, HALF + 1)
    for q in range(2):
        canon[q, six_planes, 64:104] = permuted(
            raw[q, six_planes, 64:104].reshape((HALF + 1) * 40, ELEMS), perm[q]
        ).reshape(HALF + 1, 40, ELEMS)

    lane = lax.broadcasted_iota(jnp.int32, (8, LANES), 1)
    row = lax.broadcasted_iota(jnp.int32, (8, LANES), 0)
    zi = lane % 8
    yi = (lane // 8) % 8
    low_half = lane < 64
    zero = jnp.zeros((8, LANES), jnp.float32)
    c_lo = jnp.logical_or(row == 0, row == 2)
    c_hi = jnp.logical_or(row == 1, row == 3)
    b_lo = row < 2
    b_hi = jnp.logical_or(row == 2, row == 3)

    def line_pass(lo_row, index, shift, corner_lo, corner_hi, corner_step):
        def two_planes(planes):
            spots = [(q, a, tile(t)) for a in planes for q in range(2) for t in range(TILES)]
            corners = [canon[q, a, 96:104, lanes] for q, a, lanes in spots]
            lows = [canon[q, a, lo_row : lo_row + 8, lanes] for q, a, lanes in spots]
            highs = [canon[q, a, lo_row + 16 : lo_row + 24, lanes] for q, a, lanes in spots]
            for (q, a, lanes), k, lo, hi in zip(spots, corners, lows, highs):
                canon[q, a, lo_row : lo_row + 8, lanes] = lo + jnp.where(index > 0, roll_lanes(hi, shift), zero)
                canon[q, a, lo_row + 16 : lo_row + 24, lanes] = hi + jnp.where(
                    index < 7, roll_lanes(lo, -shift), zero
                )
                canon[q, a, 96:104, lanes] = (
                    k
                    + jnp.where(
                        jnp.logical_and(corner_lo, index > 0), roll_lanes(roll_rows(k, -corner_step), shift), zero
                    )
                    + jnp.where(
                        jnp.logical_and(corner_hi, index < 7), roll_lanes(roll_rows(k, corner_step), -shift), zero
                    )
                )

        return two_planes

    def over_middle(pass_over):
        def at_step(step, carry):
            pass_over([1 + 2 * step, 2 + 2 * step])
            return carry

        lax.fori_loop(0, 4, at_step, 0)

    z_pass = line_pass(64, zi, 1, c_lo, c_hi, 1)
    y_pass = line_pass(72, yi, 8, b_lo, b_hi, 2)

    def x_pass(block, carry):
        here = pl.ds(block * 8, 8)
        for q in range(2):
            lo = [canon[q, 0, here, tile(t)] for t in range(TILES)]
            hi = [canon[q, 9, here, tile(t)] for t in range(TILES)]
            lo_rolled = [roll_lanes(x, 64) for x in lo] + [zero]
            hi_rolled = [roll_lanes(x, 64) for x in hi] + [zero]
            for t in range(TILES):
                canon[q, 0, here, tile(t)] = lo[t] + jnp.where(low_half, hi_rolled[t - 1], hi_rolled[t])
                canon[q, 9, here, tile(t)] = hi[t] + jnp.where(low_half, lo_rolled[t], lo_rolled[t + 1])
        return carry

    def pack_top(parts, index, step):
        total = parts[0]
        for u in range(1, len(parts)):
            total = jnp.where(index == 7 - u, roll_lanes(parts[u], -step * u), total)
        return total

    def pack_low(parts, index, step):
        total = parts[0]
        for u in range(1, len(parts)):
            total = jnp.where(index == u, roll_lanes(parts[u], step * u), total)
        return total

    def six(a, rows):
        return [canon[q, a, rows, tile(t)] for q in range(2) for t in range(TILES)]

    def on(flag):
        return jnp.where(flag, 1.0, 0.0).astype(jnp.float32)

    middle, ends_planes = tuple(range(1, 9)), (0, 9)
    slots = {a: (a - 1 if 0 < a < 9 else 8 + a // 9) for a in range(NODES)}

    def z_pack(planes):
        for a in planes:
            corner = six(a, slice(96, 104))
            zs[0, slots[a], 0:8] = pack_top(six(a, slice(80, 88)), zi, 1)
            zs[0, slots[a], 8:16] = pack_top(corner, zi, 1)
            zs[1, slots[a], 0:8] = pack_low(six(a, slice(64, 72)), zi, 1)
            zs[1, slots[a], 8:16] = pack_low(corner, zi, 1)

    def z_copy(part):
        here = (slice(0, 8), slice(8, 10), slice(0, 10))[part]
        return pltpu.make_async_remote_copy(
            src_ref=zs.at[:, here], dst_ref=zr.at[:, here], send_sem=z_sem.at[2], recv_sem=z_sem.at[part % 2],
            device_id=(elem, c, 1 - r), device_id_type=MESH,
        )

    r0, r1 = on(r == 0), on(r == 1)

    def x_pack(block, carry):
        here = pl.ds(block * 8, 8)
        xs[0, here] = jnp.where(low_half, roll_lanes(canon[0, 9, here, tile(2)], 64), canon[1, 9, here, tile(2)])
        xs[1, here] = jnp.where(low_half, canon[0, 0, here, tile(0)], roll_lanes(canon[1, 0, here, tile(0)], 64))
        return carry

    def x_copy(way):
        return pltpu.make_async_remote_copy(
            src_ref=xs.at[way], dst_ref=xr.at[way], send_sem=x_sem.at[0, way], recv_sem=x_sem.at[1, way],
            device_id=x_links[way][0], device_id_type=MESH,
        )

    def y_copy(part, way):
        here = (slice(0, 80), slice(80, ROWS), slice(0, ROWS))[part]
        return pltpu.make_async_remote_copy(
            src_ref=ys.at[way, here], dst_ref=yr.at[way, here],
            send_sem=y_sem.at[2, way], recv_sem=y_sem.at[part % 2, way],
            device_id=y_links[way][0], device_id_type=MESH,
        )

    def send_both(links, copies):
        for way in range(2):
            @pl.when(links[way][1])
            def _(copy=copies[way]):
                copy.start()

    def wait_both(links, copies):
        for way in range(2):
            @pl.when(links[1 - way][1])
            def _(copy=copies[way]):
                copy.wait_recv()

    def x_unpack(block, carry):
        here = pl.ds(block * 8, 8)
        below = xr[0, here]
        above = xr[1, here]
        low = (jnp.where(low_half, below, zero), jnp.where(low_half, roll_lanes(below, 64), zero))
        top = (jnp.where(low_half, zero, roll_lanes(above, 64)), jnp.where(low_half, zero, above))
        for q in range(2):
            canon[q, 0, here, tile(0)] = canon[q, 0, here, tile(0)] + low[q]
            canon[q, 9, here, tile(2)] = canon[q, 9, here, tile(2)] + top[q]
        return carry

    def put(a, b_row, value, t, first):
        start = ((a * 10 + b_row) * 10 + 1) * 3 + t
        out_ref[pl.ds(start, 8, stride=3), :] = value[first : first + 8, tile(t)]

    def put_column(a, k_row, value, t, first):
        start = ((a * 10 + 1) * 10 + k_row) * 3 + t
        out_ref[pl.ds(start, 8, stride=30), :] = value[first : first + 8, tile(t)]

    def put_edges(a, value, first):
        for t in range(TILES):
            put_column(a, 0, value, t, first)
            put(a, 0, value, t, first + 8)
            put_column(a, 9, value, t, first + 16)
            put(a, 9, value, t, first + 24)
            for number, (b, k) in enumerate(((0, 0), (0, 9), (9, 0), (9, 9))):
                start = ((a * 10 + b) * 10 + k) * 3 + t
                out_ref[pl.ds(start, 1), :] = value[first + 32 + number : first + 33 + number, tile(t)]

    def inner_wait(group):
        inner_copy(slice(1, 5 - group), slice(0, 64), group).wait_recv()

    def inner_rows(a, blocks):
        for t in range(TILES):
            for b in blocks:
                rows = slice(b * 8, b * 8 + 8)
                start = ((a * 10 + b + 1) * 10 + 1) * 3 + t
                out_ref[pl.ds(start, 8, stride=3), :] = got[a, rows, tile(t)] + raw[c, a, rows, tile(t)]

    def inner_done(a, carry):
        @pl.when(jnp.logical_and(is_inner(a), a != far + HELD))
        def _():
            inner_rows(a, range(8))

        return carry

    for q in range(2):
        both = jnp.concatenate([raw[q, 0, 0:64], raw[q, 9, 0:64]], axis=0)
        both = permuted(both, perm[q])
        canon[q, 0, 0:64] = both[0:64]
        canon[q, 9, 0:64] = both[64:128]
    steps(0, ROWS // 8, 13, x_pack)
    send_both(x_links, [x_copy(way) for way in range(2)])

    z_pack(middle)
    z_copy(0).start()
    over_middle(z_pass)
    steps(0, ROWS // 8, 13, x_pass)

    def edge_copy(group, source, target):
        return pltpu.make_async_remote_copy(
            src_ref=source, dst_ref=target, send_sem=send_sem.at[group + 1], recv_sem=edge_sem.at[group],
            device_id=(elem, o, r), device_id_type=MESH,
        )

    z_rows = edge_copy(0, canon.at[o, 1:9, 64:72], got.at[1:9, 64:72])
    y_rows = edge_copy(0, canon.at[o, 1:9, 72:80], got.at[1:9, 72:80])
    most_tops = edge_copy(0, tops.at[1:9], tops_in.at[1:9])
    x_inner = edge_copy(2, canon.at[o, 0, 0:64], got.at[0, 0:64])
    x_edges = edge_copy(1, canon.at[o, 0, 64:80], got.at[0, 64:80])
    x_tops = edge_copy(1, tops.at[0], tops_in.at[0])
    x_ends_inner = edge_copy(2, ends.at[0:32], ends_in.at[0:32])
    x_ends = edge_copy(1, ends.at[32:56], ends_in.at[32:56])
    whole_groups = (
        edge_copy(0, canon.at[o, 1:9, 0:64, 0:LANES], got.at[1:9, 0:64, 0:LANES]),
        edge_copy(1, canon.at[o, 0, 0:88, 0:LANES], got.at[0, 0:88, 0:LANES]),
        edge_copy(2, canon.at[o, 1:5, 0:56, 0:LANES], got.at[1:5, 0:56, 0:LANES]),
    )

    def z_unpack(a, carry):
        slot = slots[a]
        tops_here = [zr[0, slot, 0:8], roll_rows(zr[0, slot, 8:16], -1)]
        lows_here = [zr[1, slot, 0:8], roll_rows(zr[1, slot, 8:16], 1)]
        for t in range(TILES):
            for kind in range(2):
                top_rows = slice(80, 88) if kind == 0 else slice(96, 104)
                low_rows = slice(64, 72) if kind == 0 else slice(96, 104)
                top_mask = zi == 7 if kind == 0 else jnp.logical_and(c_hi, zi == 7)
                low_mask = zi == 0 if kind == 0 else jnp.logical_and(c_lo, zi == 0)
                from_above = [roll_lanes(lows_here[kind], 7 - (3 * q + t)) for q in range(2)]
                from_below = [roll_lanes(tops_here[kind], 3 * q + t - 7) for q in range(2)]
                adds = (
                    (0, top_rows, top_mask, from_above[0] * r0 + from_above[1] * r1),
                    (1, top_rows, top_mask, from_above[1] * r0),
                    (0, low_rows, low_mask, from_below[0] * r1),
                    (1, low_rows, low_mask, from_below[0] * r0 + from_below[1] * r1),
                )
                for q, rows, mask, value in adds:
                    canon[q, a, rows, tile(t)] = canon[q, a, rows, tile(t)] + jnp.where(mask, value, zero)
        return carry

    def y_pack(planes, first):
        for k, a in enumerate(planes):
            here = slice(first + k * 8, first + k * 8 + 8)
            ys[0, here] = pack_top(six(a, slice(88, 96)), yi, 8)
            ys[1, here] = pack_low(six(a, slice(72, 80)), yi, 8)
        for group in range(0, len(planes), 4):
            top_total, low_total = zero, zero
            for k, a in enumerate(planes[group : group + 4]):
                corner = six(a, slice(96, 104))
                mine = row // 2 == k
                top_total = jnp.where(mine, roll_rows(pack_top(corner, yi, 8), 2 * k - 2), top_total)
                low_total = jnp.where(mine, roll_rows(pack_low(corner, yi, 8), 2 * k), low_total)
            here = slice(first + len(planes) * 8 + group * 2, first + len(planes) * 8 + group * 2 + 8)
            ys[0, here] = top_total
            ys[1, here] = low_total

    def y_unpack(a, carry):
        place, first, count = (a - 1, 0, 8) if 0 < a < 9 else (a // 9, 80, 2)
        here = slice(first + place * 8, first + place * 8 + 8)
        group, k = first + count * 8 + place // 4 * 8, place % 4
        below = [yr[0, here], roll_rows(yr[0, group : group + 8], -2 * k)]
        above = [yr[1, here], roll_rows(yr[1, group : group + 8], 2 - 2 * k)]
        for q in range(2):
            for t in range(TILES):
                u = 3 * q + t
                for kind in range(2):
                    top_rows = slice(88, 96) if kind == 0 else slice(96, 104)
                    low_rows = slice(72, 80) if kind == 0 else slice(96, 104)
                    top_mask = yi == 7 if kind == 0 else jnp.logical_and(b_hi, yi == 7)
                    low_mask = yi == 0 if kind == 0 else jnp.logical_and(b_lo, yi == 0)
                    up = jnp.where(top_mask, roll_lanes(above[kind], 8 * (7 - u)), zero)
                    down = jnp.where(low_mask, roll_lanes(below[kind], 8 * (u - 7)), zero)
                    canon[q, a, top_rows, tile(t)] = canon[q, a, top_rows, tile(t)] + up
                    canon[q, a, low_rows, tile(t)] = canon[q, a, low_rows, tile(t)] + down
        return carry


    def fill_tops(a, carry):
        z_top = pack_top([canon[o, a, 80:88, tile(t)] for t in range(TILES)], zi, 1)
        y_top = pack_top([canon[o, a, 88:96, tile(t)] for t in range(TILES)], yi, 8)
        tops[a, 0:8] = jnp.where(yi > 4, y_top, jnp.where(zi > 4, z_top, roll_lanes(z_top, -27)))
        corner = [canon[o, a, 96:104, tile(t)] for t in range(TILES)]
        packed = jnp.where(row < 2, pack_top(corner, zi, 1), pack_top(corner, yi, 8))
        for t in range(TILES):
            packed = jnp.where(row == 4 + t, roll_rows(corner[t], 4 + t), packed)
        tops[a, 8:16] = packed
        return carry

    def fill_ends(block, pairs, first):
        for k in range(pairs):
            low = canon[o, 9, (block + k) * 8 : (block + k) * 8 + 8, tile(2)]
            high_block = block + k + pairs
            high = canon[o, 9, high_block * 8 : high_block * 8 + 8, tile(2)] if high_block < ROWS // 8 else zero
            ends[first + k * 8 : first + k * 8 + 8] = jnp.where(low_half, roll_lanes(low, 64), high)

    z_copy(0).wait_recv()
    for a in middle:
        z_unpack(a, 0)
    z_rows.start()
    y_pack(middle, 0)
    send_both(y_links, [y_copy(0, way) for way in range(2)])
    over_middle(y_pass)
    inner_wait(0)
    lax.fori_loop(near, near + 2, inner_done, 0)
    wait_both(y_links, [y_copy(0, way) for way in range(2)])
    for a in middle:
        y_unpack(a, 0)
    y_rows.start()
    steps(1, NODES - 2, NODES - 2, fill_tops)
    most_tops.start()

    wait_both(x_links, [x_copy(way) for way in range(2)])
    steps(0, ROWS // 8, 13, x_unpack)
    x_inner.start()
    fill_ends(0, 4, 0)
    x_ends_inner.start()
    z_pack(ends_planes)
    z_copy(1).start()
    z_pass(ends_planes)
    lax.fori_loop(near + 2, near + 4, inner_done, 0)
    z_copy(1).wait_recv()
    for a in ends_planes:
        z_unpack(a, 0)
    y_pack(ends_planes, 80)
    send_both(y_links, [y_copy(1, way) for way in range(2)])
    y_pass(ends_planes)
    lax.fori_loop(near + 4, near + HALF, inner_done, 0)
    wait_both(y_links, [y_copy(1, way) for way in range(2)])
    for a in ends_planes:
        y_unpack(a, 0)
    x_edges.start()
    fill_tops(0, 0)
    fill_ends(8, 3, 32)
    x_tops.start()
    x_ends.start()
    inner_copy(near + HELD, PART_INNER[0], 3).start()
    inner_wait(1)
    lax.fori_loop(far, far + HALF, inner_done, 0)
    inner_copy(far + HELD, PART_INNER[1], 2).wait_recv()
    inner_rows(far + HELD, range(3, 8))

    def complete(a, carry):
        for t in range(TILES):
            top = tops_in[a, 0:8]
            lo = got[a, 64:72, tile(t)]
            z_top = jnp.where(yi < 5, roll_lanes(top, t), roll_lanes(top, 27 + t))
            got[a, 80:88, tile(t)] = jnp.where(zi < 7, roll_lanes(lo, -1), z_top)
            lo = got[a, 72:80, tile(t)]
            got[a, 88:96, tile(t)] = jnp.where(yi < 7, roll_lanes(lo, -8), roll_lanes(top, 8 * t))
            top = tops_in[a, 8:16]
            full = roll_rows(top, -4 - t)
            after = jnp.where(zi < 7, roll_rows(roll_lanes(full, -1), 1), roll_lanes(top, t))
            full = jnp.where(row == 0, full, after)
            after = jnp.where(yi < 7, roll_rows(roll_lanes(full, -8), 2), roll_lanes(top, 8 * t))
            got[a, 96:104, tile(t)] = jnp.where(row < 2, full, jnp.where(row < 4, after, zero))
        return carry

    whole_groups[0].wait_recv()
    steps(1, NODES - 2, NODES - 2, complete)

    def pair_done(pair, carry):
        start = 1 + pair * 4
        total = canon[c, pl.ds(start, 4), 64:104] + got[pl.ds(start, 4), 64:104]
        value = permuted(total.reshape(160, ELEMS), back[...])
        for k in range(4):
            put_edges(start + k, value, k * 40)
        return carry

    lax.fori_loop(0, 2, pair_done, 0)

    def last_plane(block, pairs, first):
        for k in range(block, min(block + 2 * pairs, ROWS // 8)):
            here = slice(k * 8, k * 8 + 8)
            start = first + (k - block) % pairs * 8
            end = ends_in[start : start + 8]
            lo = [roll_lanes(got[0, here, tile(t)], 64) for t in range(TILES)]
            lo.append(roll_lanes(end, 64) if k < block + pairs else end)
            for t in range(TILES):
                got[9, here, tile(t)] = jnp.where(low_half, lo[t], lo[t + 1])

    whole_groups[2].wait_recv()
    last_plane(0, 4, 0)
    total = jnp.concatenate([canon[c, a, 0:64] + got[a, 0:64] for a in (0, 9)], axis=0)
    value = permuted(total, back[...])
    for k, a in enumerate((0, 9)):
        for t in range(TILES):
            for b in range(8):
                put(a, b + 1, value, t, k * 64 + b * 8)

    whole_groups[1].wait_recv()
    complete(0, 0)
    last_plane(8, 3, 32)
    total = jnp.concatenate([canon[c, a, 64:104] + got[a, 64:104] for a in (0, 9)], axis=0)
    value = permuted(total, back[...])
    for k, a in enumerate((0, 9)):
        put_edges(a, value, k * 40)

    inner_copy(far + HELD, PART_INNER[0], 3).wait_recv()
    inner_rows(far + HELD, range(3))

    z_copy(2).wait_send()
    for way in range(2):
        @pl.when(y_links[way][1])
        def _(way=way):
            y_copy(2, way).wait_send()

        @pl.when(x_links[way][1])
        def _(way=way):
            x_copy(way).wait_send()

    for group in whole_groups:
        group.wait_send()
    inner_copy(slice(1, 9), slice(0, 64), 0).wait_send()


def body(velocity, geometry, element_place):
    vmem = pltpu.VMEM
    dma = pltpu.SemaphoreType.DMA
    f32 = jnp.float32
    out = pl.pallas_call(
        kernel,
        out_shape=pltpu.VMEM((NODES * NODES * NODES * TILES, LANES), f32),
        in_specs=[
            pl.BlockSpec(memory_space=pl.ANY),
            pl.BlockSpec(memory_space=pl.ANY),
            pl.BlockSpec(memory_space=pl.ANY),
        ],
        out_specs=pl.BlockSpec(memory_space=pltpu.VMEM),
        scratch_shapes=[
            vmem((3, HALF, NODES, NODES, 2, ELEMS), f32),
            vmem((3, 3, HALF, NODES, NODES, 2, ELEMS), f32),
            pltpu.SMEM((2 * HALF * HALF,), f32),
            vmem((HALF, NODES, NODES, 2, ELEMS), f32),
            vmem((HALF, NODES, NODES, 2, ELEMS), f32),
            vmem((NODES, NODES, 2, ELEMS), f32),
            vmem((2, 2 * ELEMS, ELEMS), jnp.bfloat16),
            vmem((2 * ELEMS, ELEMS), jnp.bfloat16),
            vmem((1, ELEMS), jnp.int32),
            vmem((1, ELEMS), jnp.int32),
            vmem((2, NODES, ROWS, ELEMS), f32),
            vmem((2, NODES, ROWS, ELEMS), f32),
            vmem((NODES, ROWS, ELEMS), f32),
            vmem((2, NODES, 16, LANES), f32),
            vmem((2, NODES, 16, LANES), f32),
            vmem((2, ROWS, LANES), f32),
            vmem((2, ROWS, LANES), f32),
            vmem((2, ROWS, LANES), f32),
            vmem((2, ROWS, LANES), f32),
            vmem((NODES - 1, 16, LANES), f32),
            vmem((NODES - 1, 16, LANES), f32),
            vmem((56, LANES), f32),
            vmem((56, LANES), f32),
            dma((2, HALF)), dma((HALF,)), dma((3,)), dma((3,)), dma((3, 2)), dma((2, 2)),
            dma((4,)), dma((4,)), dma((3,)),
        ],
        compiler_params=pltpu.CompilerParams(
            collective_id=0, has_side_effects=True, vmem_limit_bytes=60 * 1024 * 1024
        ),
    )(velocity, geometry, element_place)
    return out.reshape(NODES, NODES, NODES, 1, ELEMS)


def solution(mesh):
    placed = (
        P(None, "comp", None, None, None, ("elem", "rep")),
        P(None, None, "comp", None, None, None, ("elem", "rep")),
        P("comp", ("elem", "rep")),
    )
    return jax.shard_map(
        body,
        mesh=mesh,
        in_specs=placed,
        out_specs=P(None, None, None, "comp", ("elem", "rep")),
        check_vma=False,
    )
```

```python
import jax
import jax.numpy as jnp
import numpy as np
from jax import lax
from jax.experimental import pallas as pl
from jax.experimental.pallas import tpu as pltpu
from jax.sharding import PartitionSpec as P

BLOCK_X = 6
BLOCK_Y = 8
BLOCK_Z = 8
GRID_Y = 4
RING_Y = 4
HELD = 3
PART_ROWS = ((1, 2, 3), (4, 5, 6, 7, 8, 9, 0))
PART_INNER = (slice(0, 24), slice(24, 64))
NODES = 10
HALF = 5
ELEMS = 384
LANES = 128
TILES = 3
ROWS = 104
MESH = pl.DeviceIdType.MESH


def legendre_columns(points, degree):
    columns = [points * 0.0 + 1.0, points]
    for order in range(2, degree + 1):
        columns.append(
            ((2 * order - 1) * points * columns[order - 1] - (order - 1) * columns[order - 2])
            / order
        )
    return columns


def derivative_table(node_count):
    degree = node_count - 1
    points = np.cos(np.pi * np.arange(node_count) / degree)
    for sweep in range(100):
        columns = legendre_columns(points, degree)
        points = points - (points * columns[degree] - columns[degree - 1]) / (
            node_count * columns[degree]
        )
    points = np.sort(points)
    values = legendre_columns(points, degree)[degree]
    identity = np.eye(node_count)
    spacing = points[:, None] - points[None, :] + identity
    matrix = values[:, None] / (values[None, :] * spacing)
    matrix = np.where(identity > 0.5, 0.0, matrix)
    matrix[0, 0] = -degree * (degree + 1) / 4.0
    matrix[degree, degree] = degree * (degree + 1) / 4.0
    return matrix


TABLE = derivative_table(NODES)
EVEN = [[float(0.5 * (TABLE[i, m] + TABLE[i, 9 - m])) for m in range(HALF)] for i in range(HALF)]
ODD = [[float(0.5 * (TABLE[i, m] - TABLE[i, 9 - m])) for m in range(HALF)] for i in range(HALF)]


def weighted(terms, weights):
    total = terms[0] * weights[0]
    for term, weight in zip(terms[1:], weights[1:]):
        total = total + term * weight
    return total


def along(values):
    minus = [values[i] - values[9 - i] for i in range(HALF)]
    plus = [values[i] + values[9 - i] for i in range(HALF)]
    out = [None] * NODES
    for m in range(HALF):
        even = weighted(minus, [EVEN[i][m] for i in range(HALF)])
        odd = weighted(plus, [ODD[i][m] for i in range(HALF)])
        out[m] = even + odd
        out[9 - m] = even - odd
    return out


def tile(t):
    return slice(t * LANES, (t + 1) * LANES)


def roll_lanes(x, shift):
    return pltpu.roll(x, shift % LANES, 1)


def roll_rows(x, shift):
    return pltpu.roll(x, shift % 8, 0)


def two_parts(x):
    high = x.astype(jnp.bfloat16)
    low = (x - high.astype(jnp.float32)).astype(jnp.bfloat16)
    return jnp.concatenate([high, low], axis=1)


def steps(start, count, per, fn):
    if per == count:
        for k in range(count):
            fn(start + k, 0)
        return

    def several(step, carry):
        for k in range(per):
            fn(start + step * per + k, 0)
        return carry

    lax.fori_loop(0, count // per, several, 0)


def kernel(
    v_hbm, g_hbm, place_hbm, out_ref,
    v, g, coef, f0, fl, fn, perm, back, place_own, place_in, raw, canon, got,
    zs, zr, ys, yr, xs, xr, tops, tops_in, ends, ends_in,
    first_sem, place_sem, z_sem, y_sem, x_sem, send_sem, inner_sem, edge_sem,
):
    elem = lax.axis_index("elem")
    c = lax.axis_index("comp")
    r = lax.axis_index("rep")
    o = 1 - c
    elem_count = lax.axis_size("elem")
    grid_x = elem_count // GRID_Y
    sx = elem // GRID_Y
    sy = elem % GRID_Y
    y_links = (((elem + 1, c, r), sy < GRID_Y - 1), ((elem - 1, c, r), sy > 0))
    up_comp = jnp.where(sx % RING_Y == RING_Y - 1, o, c)
    down_comp = jnp.where(sx % RING_Y == 0, o, c)
    x_links = (((elem + GRID_Y, up_comp, r), sx < grid_x - 1), ((elem - GRID_Y, down_comp, r), sx > 0))

    barrier = pltpu.get_barrier_semaphore()
    expected = 2
    for neighbour, exists in x_links + y_links:
        expected = expected + exists.astype(jnp.int32)

        @pl.when(exists)
        def _(neighbour=neighbour):
            pl.semaphore_signal(barrier, inc=1, device_id=neighbour, device_id_type=MESH)

    for other in ((elem, o, r), (elem, c, 1 - r)):
        pl.semaphore_signal(barrier, inc=1, device_id=other, device_id_type=MESH)

    own_copy = pltpu.make_async_copy(place_hbm, place_own, place_sem.at[2])
    own_copy.start()

    def first_copies(i, part):
        copies = []
        for here in (slice(1, 4),) if part == 0 else (slice(4, 10), slice(0, 1)):
            copies.append(pltpu.make_async_copy(v_hbm.at[:, i, here], v.at[:, i, here], first_sem.at[part, i]))
            copies.append(
                pltpu.make_async_copy(g_hbm.at[:, 0, i, here], g.at[:, 0, i, here], first_sem.at[part, i])
            )
        return copies

    def first_arrived(i, part):
        here = slice(0, len(PART_ROWS[part]))
        pltpu.make_async_copy(g_hbm.at[:, 0:2, i, here], g.at[:, 0:2, i, here], first_sem.at[part, i]).wait()

    def later_copy(i):
        return pltpu.make_async_copy(g_hbm.at[:, 1:3, i], g.at[:, 1:3, i], first_sem.at[0, i])

    for i in range(HALF):
        for copy in first_copies(i, 0):
            copy.start()

    for links, target in ((y_links, yr), (x_links, xr)):
        for way in range(2):
            @pl.when(jnp.logical_not(links[1 - way][1]))
            def _(target=target, way=way):
                target[way] = jnp.zeros(target.shape[1:], jnp.float32)

    for kind in range(2):
        for m in range(HALF):
            for i in range(HALF):
                first = float(TABLE[i, (5 + m) if kind == 0 else m])
                second = float(TABLE[5 + i, m if kind == 0 else (5 + m)])
                coef[(kind * HALF + m) * HALF + i] = jnp.where(c == 0, first, second).astype(jnp.float32)


    rows_iota = lax.broadcasted_iota(jnp.int32, (ELEMS, ELEMS), 0)
    lanes_iota = lax.broadcasted_iota(jnp.int32, (LANES, ELEMS), 1).astype(jnp.float32)

    def fill_perm(q, places):
        for t in range(TILES):
            place = jnp.broadcast_to(places[:, tile(t)].astype(jnp.float32), (LANES, LANES)).T
            place = jnp.concatenate([place] * TILES, axis=1)
            part = jnp.where(lanes_iota == place, 1.0, 0.0).astype(jnp.bfloat16)
            for copy in range(2):
                perm[q, copy * ELEMS + t * LANES : copy * ELEMS + (t + 1) * LANES, :] = part

    raw[:, :, 96:104] = jnp.zeros((2, NODES, 8, ELEMS), jnp.float32)

    far = HALF * o
    near = HALF * c

    def inner_copy(a, rows, group):
        return pltpu.make_async_remote_copy(
            src_ref=raw.at[o, a, rows], dst_ref=got.at[a, rows], send_sem=send_sem.at[0], recv_sem=inner_sem.at[group],
            device_id=(elem, o, r), device_id_type=MESH,
        )

    def is_inner(a):
        return jnp.logical_and(a > 0, a < NODES - 1)

    def send_inner(a, halves, group):
        @pl.when(is_inner(a))
        def _():
            for half in halves:
                inner_copy(a, PART_INNER[half], group).start()

    def first_flux(half):
        def at_plane(i, carry):
            first_arrived(i, half)
            for copy in first_copies(i, 1) if half == 0 else (later_copy(i),):
                copy.start()

            def at_b(b, carry):
                for k in range(NODES):
                    f0[i, b, k] = (
                        g[0, 0, i, b, k] * v[0, i, b, k]
                        + g[1, 0, i, b, k] * v[1, i, b, k]
                        + g[2, 0, i, b, k] * v[2, i, b, k]
                    )

            for b in PART_ROWS[half]:
                at_b(b, 0)
            return carry

        return at_plane

    def mix_planes(m, half):
        weights = [coef[m * HALF + i] for i in range(HALF)]
        for b in PART_ROWS[half]:
            for k in range(NODES):
                fl[m, b, k] = weighted([f0[i, b, k] for i in range(HALF)], weights)

    def gather_inner(m, a, half):
        for q in range(2):
            for t in range(TILES):
                for b in range(PART_INNER[half].start // 8, PART_INNER[half].stop // 8):
                    raw[q, a, b * 8 : b * 8 + 8, tile(t)] = fl[m, b + 1, 1:9, q, tile(t)]

    def gather_edges(m, a):
        for q in range(2):
            for t in range(TILES):
                raw[q, a, 64:72, tile(t)] = fl[m, 1:9, 0, q, tile(t)]
                raw[q, a, 72:80, tile(t)] = fl[m, 0, 1:9, q, tile(t)]
                raw[q, a, 80:88, tile(t)] = fl[m, 1:9, 9, q, tile(t)]
                raw[q, a, 88:96, tile(t)] = fl[m, 9, 1:9, q, tile(t)]
            raw[q, a, 96:97, :] = fl[m, 0, 0, q : q + 1, :]
            raw[q, a, 97:98, :] = fl[m, 0, 9, q : q + 1, :]
            raw[q, a, 98:99, :] = fl[m, 9, 0, q : q + 1, :]
            raw[q, a, 99:100, :] = fl[m, 9, 9, q : q + 1, :]

    def permuted(x, matrix):
        return jnp.dot(two_parts(x), matrix, preferred_element_type=jnp.float32)

    def to_canon(a, between=None):
        parts = [two_parts(raw[q, a, 64:104]) for q in range(2)]
        if between is not None:
            between()
        for q in range(2):
            canon[q, a, 64:104] = jnp.dot(parts[q], perm[q], preferred_element_type=jnp.float32)

    def far_rows(step):
        m = (step + c) % HALF
        mix_planes(m, 0)
        gather_inner(m, far + m, 0)

    def far_first(step, carry):
        far_rows(step)
        send_inner(far + (step + c) % HALF, (0,), 0)
        return carry

    def far_second(step, carry):
        m = (step + c) % HALF
        mix_planes(m, 1)
        gather_inner(m, far + m, 1)
        send_inner(far + m, (1,), 0)
        gather_edges(m, far + m)
        return carry

    fl[0] = jnp.zeros(fl.shape[1:], jnp.float32)
    gather_inner(0, 0, 0)
    gather_inner(0, 0, 1)
    gather_edges(0, 0)
    lax.fori_loop(0, HALF, first_flux(0), 0)
    far_rows(0)
    own_copy.wait()
    pl.semaphore_wait(barrier, expected)
    send_inner(far + c, (0,), 0)
    place_copy = pltpu.make_async_remote_copy(
        src_ref=place_own, dst_ref=place_in, send_sem=place_sem.at[0], recv_sem=place_sem.at[1],
        device_id=(elem, o, r), device_id_type=MESH,
    )
    place_copy.start()
    lax.fori_loop(1, HALF, far_first, 0)
    lax.fori_loop(0, HALF, first_flux(1), 0)
    lax.fori_loop(0, HALF, far_second, 0)

    def near_plane(m):
        later_copy(m).wait()

        def flux(j, b, k):
            return (
                g[0, j, m, b, k] * v[0, m, b, k]
                + g[1, j, m, b, k] * v[1, m, b, k]
                + g[2, j, m, b, k] * v[2, m, b, k]
            )

        def at_b(b, carry):
            base = (HALF + m) * HALF
            weights = [coef[base + i] for i in range(HALF)]
            out = along([flux(2, b, k) for k in range(NODES)])
            for k in range(NODES):
                fn[b, k] = out[k] + weighted([f0[i, b, k] for i in range(HALF)], weights)
            return carry

        steps(0, NODES, 2, at_b)

        def at_k(k, carry):
            out = along([flux(1, b, k) for b in range(NODES)])
            for b in range(NODES):
                fl[m, b, k] = fn[b, k] + out[b]
            return carry

        steps(0, NODES, 2, at_k)

    def near_gather(m):
        gather_inner(m, near + m, 0)
        gather_inner(m, near + m, 1)
        gather_edges(m, near + m)

    def near_step(m, carry):
        near_plane(m)
        to_canon(far + m - c, lambda: near_gather(m))

        @pl.when(m != HELD)
        def _():
            send_inner(near + m, (0, 1), 1)

        @pl.when(m == HELD)
        def _():
            send_inner(near + m, (1,), 2)

        return carry

    near_plane(0)
    near_gather(0)
    send_inner(near, (0, 1), 1)
    place_copy.wait()
    back_half = jnp.where(rows_iota == place_own[...], 1.0, 0.0).astype(jnp.bfloat16)
    back[0:ELEMS, :] = back_half
    back[ELEMS : 2 * ELEMS, :] = back_half
    fill_perm(c, place_own[...])
    fill_perm(o, place_in[...])
    lax.fori_loop(1, HALF, near_step, 0)
    six_planes = pl.ds(near - c, HALF + 1)
    for q in range(2):
        canon[q, six_planes, 64:104] = permuted(
            raw[q, six_planes, 64:104].reshape((HALF + 1) * 40, ELEMS), perm[q]
        ).reshape(HALF + 1, 40, ELEMS)

    lane = lax.broadcasted_iota(jnp.int32, (8, LANES), 1)
    row = lax.broadcasted_iota(jnp.int32, (8, LANES), 0)
    zi = lane % 8
    yi = (lane // 8) % 8
    low_half = lane < 64
    zero = jnp.zeros((8, LANES), jnp.float32)
    c_lo = jnp.logical_or(row == 0, row == 2)
    c_hi = jnp.logical_or(row == 1, row == 3)
    b_lo = row < 2
    b_hi = jnp.logical_or(row == 2, row == 3)

    def line_pass(lo_row, index, shift, corner_lo, corner_hi, corner_step):
        def two_planes(planes):
            spots = [(q, a, tile(t)) for a in planes for q in range(2) for t in range(TILES)]
            corners = [canon[q, a, 96:104, lanes] for q, a, lanes in spots]
            lows = [canon[q, a, lo_row : lo_row + 8, lanes] for q, a, lanes in spots]
            highs = [canon[q, a, lo_row + 16 : lo_row + 24, lanes] for q, a, lanes in spots]
            for (q, a, lanes), k, lo, hi in zip(spots, corners, lows, highs):
                canon[q, a, lo_row : lo_row + 8, lanes] = lo + jnp.where(index > 0, roll_lanes(hi, shift), zero)
                canon[q, a, lo_row + 16 : lo_row + 24, lanes] = hi + jnp.where(
                    index < 7, roll_lanes(lo, -shift), zero
                )
                canon[q, a, 96:104, lanes] = (
                    k
                    + jnp.where(
                        jnp.logical_and(corner_lo, index > 0), roll_lanes(roll_rows(k, -corner_step), shift), zero
                    )
                    + jnp.where(
                        jnp.logical_and(corner_hi, index < 7), roll_lanes(roll_rows(k, corner_step), -shift), zero
                    )
                )

        return two_planes

    def over_middle(pass_over):
        def at_step(step, carry):
            pass_over([1 + 2 * step, 2 + 2 * step])
            return carry

        lax.fori_loop(0, 4, at_step, 0)

    z_pass = line_pass(64, zi, 1, c_lo, c_hi, 1)
    y_pass = line_pass(72, yi, 8, b_lo, b_hi, 2)

    def x_pass(block, carry):
        here = pl.ds(block * 8, 8)
        for q in range(2):
            lo = [canon[q, 0, here, tile(t)] for t in range(TILES)]
            hi = [canon[q, 9, here, tile(t)] for t in range(TILES)]
            lo_rolled = [roll_lanes(x, 64) for x in lo] + [zero]
            hi_rolled = [roll_lanes(x, 64) for x in hi] + [zero]
            for t in range(TILES):
                canon[q, 0, here, tile(t)] = lo[t] + jnp.where(low_half, hi_rolled[t - 1], hi_rolled[t])
                canon[q, 9, here, tile(t)] = hi[t] + jnp.where(low_half, lo_rolled[t], lo_rolled[t + 1])
        return carry

    def pack_top(parts, index, step):
        total = parts[0]
        for u in range(1, len(parts)):
            total = jnp.where(index == 7 - u, roll_lanes(parts[u], -step * u), total)
        return total

    def pack_low(parts, index, step):
        total = parts[0]
        for u in range(1, len(parts)):
            total = jnp.where(index == u, roll_lanes(parts[u], step * u), total)
        return total

    def six(a, rows):
        return [canon[q, a, rows, tile(t)] for q in range(2) for t in range(TILES)]

    def on(flag):
        return jnp.where(flag, 1.0, 0.0).astype(jnp.float32)

    middle, ends_planes = tuple(range(1, 9)), (0, 9)
    slots = {a: (a - 1 if 0 < a < 9 else 8 + a // 9) for a in range(NODES)}

    def z_pack(planes):
        for a in planes:
            corner = six(a, slice(96, 104))
            zs[0, slots[a], 0:8] = pack_top(six(a, slice(80, 88)), zi, 1)
            zs[0, slots[a], 8:16] = pack_top(corner, zi, 1)
            zs[1, slots[a], 0:8] = pack_low(six(a, slice(64, 72)), zi, 1)
            zs[1, slots[a], 8:16] = pack_low(corner, zi, 1)

    def z_copy(part):
        here = (slice(0, 8), slice(8, 10), slice(0, 10))[part]
        return pltpu.make_async_remote_copy(
            src_ref=zs.at[:, here], dst_ref=zr.at[:, here], send_sem=first_sem.at[1, 4], recv_sem=z_sem.at[part % 2],
            device_id=(elem, c, 1 - r), device_id_type=MESH,
        )

    r0, r1 = on(r == 0), on(r == 1)

    def x_pack(block, carry):
        here = pl.ds(block * 8, 8)
        xs[0, here] = jnp.where(low_half, roll_lanes(canon[0, 9, here, tile(2)], 64), canon[1, 9, here, tile(2)])
        xs[1, here] = jnp.where(low_half, canon[0, 0, here, tile(0)], roll_lanes(canon[1, 0, here, tile(0)], 64))
        return carry

    def x_copy(way):
        return pltpu.make_async_remote_copy(
            src_ref=xs.at[way], dst_ref=xr.at[way], send_sem=first_sem.at[1, way], recv_sem=x_sem.at[way],
            device_id=x_links[way][0], device_id_type=MESH,
        )

    def y_copy(part, way):
        here = (slice(0, 80), slice(80, ROWS), slice(0, ROWS))[part]
        return pltpu.make_async_remote_copy(
            src_ref=ys.at[way, here], dst_ref=yr.at[way, here],
            send_sem=first_sem.at[1, 2 + way], recv_sem=y_sem.at[part % 2, way],
            device_id=y_links[way][0], device_id_type=MESH,
        )

    def send_both(links, copies):
        for way in range(2):
            @pl.when(links[way][1])
            def _(copy=copies[way]):
                copy.start()

    def wait_both(links, copies):
        for way in range(2):
            @pl.when(links[1 - way][1])
            def _(copy=copies[way]):
                copy.wait_recv()

    def x_unpack(block, carry):
        here = pl.ds(block * 8, 8)
        below = xr[0, here]
        above = xr[1, here]
        low = (jnp.where(low_half, below, zero), jnp.where(low_half, roll_lanes(below, 64), zero))
        top = (jnp.where(low_half, zero, roll_lanes(above, 64)), jnp.where(low_half, zero, above))
        for q in range(2):
            canon[q, 0, here, tile(0)] = canon[q, 0, here, tile(0)] + low[q]
            canon[q, 9, here, tile(2)] = canon[q, 9, here, tile(2)] + top[q]
        return carry

    def put(a, b_row, value, t, first):
        start = ((a * 10 + b_row) * 10 + 1) * 3 + t
        out_ref[pl.ds(start, 8, stride=3), :] = value[first : first + 8, tile(t)]

    def put_column(a, k_row, value, t, first):
        start = ((a * 10 + 1) * 10 + k_row) * 3 + t
        out_ref[pl.ds(start, 8, stride=30), :] = value[first : first + 8, tile(t)]

    def put_edges(a, value, first):
        for t in range(TILES):
            put_column(a, 0, value, t, first)
            put(a, 0, value, t, first + 8)
            put_column(a, 9, value, t, first + 16)
            put(a, 9, value, t, first + 24)
            for number, (b, k) in enumerate(((0, 0), (0, 9), (9, 0), (9, 9))):
                start = ((a * 10 + b) * 10 + k) * 3 + t
                out_ref[pl.ds(start, 1), :] = value[first + 32 + number : first + 33 + number, tile(t)]

    def inner_wait(group):
        inner_copy(slice(1, 5 - group), slice(0, 64), group).wait_recv()

    def inner_rows(a, blocks):
        for t in range(TILES):
            for b in blocks:
                rows = slice(b * 8, b * 8 + 8)
                start = ((a * 10 + b + 1) * 10 + 1) * 3 + t
                out_ref[pl.ds(start, 8, stride=3), :] = got[a, rows, tile(t)] + raw[c, a, rows, tile(t)]

    def inner_done(a, carry):
        @pl.when(jnp.logical_and(is_inner(a), a != far + HELD))
        def _():
            inner_rows(a, range(8))

        return carry

    for q in range(2):
        both = jnp.concatenate([raw[q, 0, 0:64], raw[q, 9, 0:64]], axis=0)
        both = permuted(both, perm[q])
        canon[q, 0, 0:64] = both[0:64]
        canon[q, 9, 0:64] = both[64:128]
    steps(0, ROWS // 8, 13, x_pack)
    send_both(x_links, [x_copy(way) for way in range(2)])

    z_pack(middle)
    z_copy(0).start()
    over_middle(z_pass)
    steps(0, ROWS // 8, 13, x_pass)

    def edge_copy(group, source, target):
        return pltpu.make_async_remote_copy(
            src_ref=source, dst_ref=target, send_sem=send_sem.at[group + 1], recv_sem=edge_sem.at[group],
            device_id=(elem, o, r), device_id_type=MESH,
        )

    z_rows = edge_copy(0, canon.at[o, 1:9, 64:72], got.at[1:9, 64:72])
    y_rows = edge_copy(0, canon.at[o, 1:9, 72:80], got.at[1:9, 72:80])
    most_tops = edge_copy(0, tops.at[1:9], tops_in.at[1:9])
    x_inner = edge_copy(2, canon.at[o, 0, 0:64], got.at[0, 0:64])
    x_edges = edge_copy(1, canon.at[o, 0, 64:80], got.at[0, 64:80])
    x_tops = edge_copy(1, tops.at[0], tops_in.at[0])
    x_ends_inner = edge_copy(2, ends.at[0:32], ends_in.at[0:32])
    x_ends = edge_copy(1, ends.at[32:56], ends_in.at[32:56])
    whole_groups = (
        edge_copy(0, canon.at[o, 1:9, 0:64, 0:LANES], got.at[1:9, 0:64, 0:LANES]),
        edge_copy(1, canon.at[o, 0, 0:88, 0:LANES], got.at[0, 0:88, 0:LANES]),
        edge_copy(2, canon.at[o, 1:5, 0:56, 0:LANES], got.at[1:5, 0:56, 0:LANES]),
    )

    def z_unpack(a, carry):
        slot = slots[a]
        tops_here = [zr[0, slot, 0:8], roll_rows(zr[0, slot, 8:16], -1)]
        lows_here = [zr[1, slot, 0:8], roll_rows(zr[1, slot, 8:16], 1)]
        for t in range(TILES):
            for kind in range(2):
                top_rows = slice(80, 88) if kind == 0 else slice(96, 104)
                low_rows = slice(64, 72) if kind == 0 else slice(96, 104)
                top_mask = zi == 7 if kind == 0 else jnp.logical_and(c_hi, zi == 7)
                low_mask = zi == 0 if kind == 0 else jnp.logical_and(c_lo, zi == 0)
                from_above = [roll_lanes(lows_here[kind], 7 - (3 * q + t)) for q in range(2)]
                from_below = [roll_lanes(tops_here[kind], 3 * q + t - 7) for q in range(2)]
                adds = (
                    (0, top_rows, top_mask, from_above[0] * r0 + from_above[1] * r1),
                    (1, top_rows, top_mask, from_above[1] * r0),
                    (0, low_rows, low_mask, from_below[0] * r1),
                    (1, low_rows, low_mask, from_below[0] * r0 + from_below[1] * r1),
                )
                for q, rows, mask, value in adds:
                    canon[q, a, rows, tile(t)] = canon[q, a, rows, tile(t)] + jnp.where(mask, value, zero)
        return carry

    def y_pack(planes, first):
        for k, a in enumerate(planes):
            here = slice(first + k * 8, first + k * 8 + 8)
            ys[0, here] = pack_top(six(a, slice(88, 96)), yi, 8)
            ys[1, here] = pack_low(six(a, slice(72, 80)), yi, 8)
        for group in range(0, len(planes), 4):
            top_total, low_total = zero, zero
            for k, a in enumerate(planes[group : group + 4]):
                corner = six(a, slice(96, 104))
                mine = row // 2 == k
                top_total = jnp.where(mine, roll_rows(pack_top(corner, yi, 8), 2 * k - 2), top_total)
                low_total = jnp.where(mine, roll_rows(pack_low(corner, yi, 8), 2 * k), low_total)
            here = slice(first + len(planes) * 8 + group * 2, first + len(planes) * 8 + group * 2 + 8)
            ys[0, here] = top_total
            ys[1, here] = low_total

    def y_unpack(a, carry):
        place, first, count = (a - 1, 0, 8) if 0 < a < 9 else (a // 9, 80, 2)
        here = slice(first + place * 8, first + place * 8 + 8)
        group, k = first + count * 8 + place // 4 * 8, place % 4
        below = [yr[0, here], roll_rows(yr[0, group : group + 8], -2 * k)]
        above = [yr[1, here], roll_rows(yr[1, group : group + 8], 2 - 2 * k)]
        for q in range(2):
            for t in range(TILES):
                u = 3 * q + t
                for kind in range(2):
                    top_rows = slice(88, 96) if kind == 0 else slice(96, 104)
                    low_rows = slice(72, 80) if kind == 0 else slice(96, 104)
                    top_mask = yi == 7 if kind == 0 else jnp.logical_and(b_hi, yi == 7)
                    low_mask = yi == 0 if kind == 0 else jnp.logical_and(b_lo, yi == 0)
                    up = jnp.where(top_mask, roll_lanes(above[kind], 8 * (7 - u)), zero)
                    down = jnp.where(low_mask, roll_lanes(below[kind], 8 * (u - 7)), zero)
                    canon[q, a, top_rows, tile(t)] = canon[q, a, top_rows, tile(t)] + up
                    canon[q, a, low_rows, tile(t)] = canon[q, a, low_rows, tile(t)] + down
        return carry


    def fill_tops(a, carry):
        z_top = pack_top([canon[o, a, 80:88, tile(t)] for t in range(TILES)], zi, 1)
        y_top = pack_top([canon[o, a, 88:96, tile(t)] for t in range(TILES)], yi, 8)
        tops[a, 0:8] = jnp.where(yi > 4, y_top, jnp.where(zi > 4, z_top, roll_lanes(z_top, -27)))
        corner = [canon[o, a, 96:104, tile(t)] for t in range(TILES)]
        packed = jnp.where(row < 2, pack_top(corner, zi, 1), pack_top(corner, yi, 8))
        for t in range(TILES):
            packed = jnp.where(row == 4 + t, roll_rows(corner[t], 4 + t), packed)
        tops[a, 8:16] = packed
        return carry

    def fill_ends(block, pairs, first):
        for k in range(pairs):
            low = canon[o, 9, (block + k) * 8 : (block + k) * 8 + 8, tile(2)]
            high_block = block + k + pairs
            high = canon[o, 9, high_block * 8 : high_block * 8 + 8, tile(2)] if high_block < ROWS // 8 else zero
            ends[first + k * 8 : first + k * 8 + 8] = jnp.where(low_half, roll_lanes(low, 64), high)

    z_copy(0).wait_recv()
    for a in middle:
        z_unpack(a, 0)
    z_rows.start()
    y_pack(middle, 0)
    send_both(y_links, [y_copy(0, way) for way in range(2)])
    over_middle(y_pass)
    inner_wait(0)
    lax.fori_loop(near, near + 2, inner_done, 0)
    wait_both(y_links, [y_copy(0, way) for way in range(2)])
    for a in middle:
        y_unpack(a, 0)
    y_rows.start()
    steps(1, NODES - 2, NODES - 2, fill_tops)
    most_tops.start()

    wait_both(x_links, [x_copy(way) for way in range(2)])
    steps(0, ROWS // 8, 13, x_unpack)
    x_inner.start()
    fill_ends(0, 4, 0)
    x_ends_inner.start()
    z_pack(ends_planes)
    z_copy(1).start()
    z_pass(ends_planes)
    lax.fori_loop(near + 2, near + 4, inner_done, 0)
    z_copy(1).wait_recv()
    for a in ends_planes:
        z_unpack(a, 0)
    y_pack(ends_planes, 80)
    send_both(y_links, [y_copy(1, way) for way in range(2)])
    y_pass(ends_planes)
    lax.fori_loop(near + 4, near + HALF, inner_done, 0)
    wait_both(y_links, [y_copy(1, way) for way in range(2)])
    for a in ends_planes:
        y_unpack(a, 0)
    x_edges.start()
    fill_tops(0, 0)
    fill_ends(8, 3, 32)
    x_tops.start()
    x_ends.start()
    inner_copy(near + HELD, PART_INNER[0], 3).start()
    inner_wait(1)
    lax.fori_loop(far, far + HALF, inner_done, 0)
    inner_copy(far + HELD, PART_INNER[1], 2).wait_recv()
    inner_rows(far + HELD, range(3, 8))

    def complete(a, carry):
        for t in range(TILES):
            top = tops_in[a, 0:8]
            lo = got[a, 64:72, tile(t)]
            z_top = jnp.where(yi < 5, roll_lanes(top, t), roll_lanes(top, 27 + t))
            got[a, 80:88, tile(t)] = jnp.where(zi < 7, roll_lanes(lo, -1), z_top)
            lo = got[a, 72:80, tile(t)]
            got[a, 88:96, tile(t)] = jnp.where(yi < 7, roll_lanes(lo, -8), roll_lanes(top, 8 * t))
            top = tops_in[a, 8:16]
            full = roll_rows(top, -4 - t)
            after = jnp.where(zi < 7, roll_rows(roll_lanes(full, -1), 1), roll_lanes(top, t))
            full = jnp.where(row == 0, full, after)
            after = jnp.where(yi < 7, roll_rows(roll_lanes(full, -8), 2), roll_lanes(top, 8 * t))
            got[a, 96:104, tile(t)] = jnp.where(row < 2, full, jnp.where(row < 4, after, zero))
        return carry

    whole_groups[0].wait_recv()
    steps(1, NODES - 2, NODES - 2, complete)

    def pair_done(pair, carry):
        start = 1 + pair * 4
        total = canon[c, pl.ds(start, 4), 64:104] + got[pl.ds(start, 4), 64:104]
        value = permuted(total.reshape(160, ELEMS), back[...])
        for k in range(4):
            put_edges(start + k, value, k * 40)
        return carry

    lax.fori_loop(0, 2, pair_done, 0)

    def last_plane(block, pairs, first):
        for k in range(block, min(block + 2 * pairs, ROWS // 8)):
            here = slice(k * 8, k * 8 + 8)
            start = first + (k - block) % pairs * 8
            end = ends_in[start : start + 8]
            lo = [roll_lanes(got[0, here, tile(t)], 64) for t in range(TILES)]
            lo.append(roll_lanes(end, 64) if k < block + pairs else end)
            for t in range(TILES):
                got[9, here, tile(t)] = jnp.where(low_half, lo[t], lo[t + 1])

    whole_groups[2].wait_recv()
    last_plane(0, 4, 0)
    total = jnp.concatenate([canon[c, a, 0:64] + got[a, 0:64] for a in (0, 9)], axis=0)
    value = permuted(total, back[...])
    for k, a in enumerate((0, 9)):
        for t in range(TILES):
            for b in range(8):
                put(a, b + 1, value, t, k * 64 + b * 8)

    whole_groups[1].wait_recv()
    complete(0, 0)
    last_plane(8, 3, 32)
    total = jnp.concatenate([canon[c, a, 64:104] + got[a, 64:104] for a in (0, 9)], axis=0)
    value = permuted(total, back[...])
    for k, a in enumerate((0, 9)):
        put_edges(a, value, k * 40)

    inner_copy(far + HELD, PART_INNER[0], 3).wait_recv()
    inner_rows(far + HELD, range(3))

    z_copy(2).wait_send()
    for way in range(2):
        @pl.when(y_links[way][1])
        def _(way=way):
            y_copy(2, way).wait_send()

        @pl.when(x_links[way][1])
        def _(way=way):
            x_copy(way).wait_send()

    for group in whole_groups:
        group.wait_send()
    inner_copy(slice(1, 9), slice(0, 64), 0).wait_send()


def body(velocity, geometry, element_place):
    vmem = pltpu.VMEM
    dma = pltpu.SemaphoreType.DMA
    f32 = jnp.float32
    out = pl.pallas_call(
        kernel,
        out_shape=pltpu.VMEM((NODES * NODES * NODES * TILES, LANES), f32),
        in_specs=[
            pl.BlockSpec(memory_space=pl.ANY),
            pl.BlockSpec(memory_space=pl.ANY),
            pl.BlockSpec(memory_space=pl.ANY),
        ],
        out_specs=pl.BlockSpec(memory_space=pltpu.VMEM),
        scratch_shapes=[
            vmem((3, HALF, NODES, NODES, 2, ELEMS), f32),
            vmem((3, 3, HALF, NODES, NODES, 2, ELEMS), f32),
            pltpu.SMEM((2 * HALF * HALF,), f32),
            vmem((HALF, NODES, NODES, 2, ELEMS), f32),
            vmem((HALF, NODES, NODES, 2, ELEMS), f32),
            vmem((NODES, NODES, 2, ELEMS), f32),
            vmem((2, 2 * ELEMS, ELEMS), jnp.bfloat16),
            vmem((2 * ELEMS, ELEMS), jnp.bfloat16),
            vmem((1, ELEMS), jnp.int32),
            vmem((1, ELEMS), jnp.int32),
            vmem((2, NODES, ROWS, ELEMS), f32),
            vmem((2, NODES, ROWS, ELEMS), f32),
            vmem((NODES, ROWS, ELEMS), f32),
            vmem((2, NODES, 16, LANES), f32),
            vmem((2, NODES, 16, LANES), f32),
            vmem((2, ROWS, LANES), f32),
            vmem((2, ROWS, LANES), f32),
            vmem((2, ROWS, LANES), f32),
            vmem((2, ROWS, LANES), f32),
            vmem((NODES - 1, 16, LANES), f32),
            vmem((NODES - 1, 16, LANES), f32),
            vmem((56, LANES), f32),
            vmem((56, LANES), f32),
            dma((2, HALF)), dma((3,)), dma((2,)), dma((2, 2)), dma((2,)),
            dma((4,)), dma((4,)), dma((3,)),
        ],
        compiler_params=pltpu.CompilerParams(
            collective_id=0, has_side_effects=True, vmem_limit_bytes=60 * 1024 * 1024
        ),
    )(velocity, geometry, element_place)
    return out.reshape(NODES, NODES, NODES, 1, ELEMS)


def solution(mesh):
    placed = (
        P(None, "comp", None, None, None, ("elem", "rep")),
        P(None, None, "comp", None, None, None, ("elem", "rep")),
        P("comp", ("elem", "rep")),
    )
    return jax.shard_map(
        body,
        mesh=mesh,
        in_specs=placed,
        out_specs=P(None, None, None, "comp", ("elem", "rep")),
        check_vma=False,
    )
```
